512 devices in a mesh: dp: 64 (over z, x, core), rows: 8 (over y).
Axes of the slice: x: 4, y: 8, z: 8, core: 2. Of those that a mesh axis runs over, the one named last changes fastest.
Arguments:
- fine_level: bfloat16 [64, 128, 64, 256], P('dp', 'rows'), may hold values from -6 to 6
- out_grad: bfloat16 [64, 128, 64, 256], P('dp', 'rows'), may hold values from -6 to 6
- fine_input: bfloat16 [64, 128, 64, 256], P('dp', 'rows'), may hold values from -6 to 6
- mid_input: bfloat16 [64, 64, 32, 512], P('dp', None, None, 'rows'), may hold values from -6 to 6
- top_input: bfloat16 [64, 32, 16, 1024], P('dp', None, None, 'rows'), may hold values from -6 to 6
- smooth_weight: bfloat16 [3, 3, 256, 256], replicated, may hold values from -0.125 to 0.125
- fine_lateral: bfloat16 [256, 256], replicated, may hold values from -0.375 to 0.375
- mid_lateral: bfloat16 [512, 256], P('rows'), may hold values from -0.375 to 0.375
- top_lateral: bfloat16 [1024, 256], P('rows'), may hold values from -0.375 to 0.375
Outputs:
- grad_fine: bfloat16 [64, 128, 64, 256], P('dp', 'rows')
- grad_mid: bfloat16 [64, 64, 32, 512], P('dp', None, None, 'rows')
- grad_top: bfloat16 [64, 32, 16, 1024], P('dp', None, None, 'rows')
- kernel_grads: float32 [2560, 256], P('dp')
- midlat_grad: float32 [512, 256], P('rows')
- toplat_grad: float32 [1024, 256], P('rows')
The draws below stay inside these ranges and needn't reach their ends.
All inputs are finite; a program needn't handle non-finite values.
Results may differ from the reference program's by a relative error of at most 0.0062.
Values may be sent and summed in bfloat16 or wider, within the bound.
A program may use at most 64 MiB of HBM per device.

```python
import jax
import jax.numpy as jnp
from jax import lax

FPN = 256
C2 = 256
C3 = 512
C4 = 1024
W2 = 64
BATCH = 64
H2 = 128
H3 = 64
W3 = 32
H4 = 32
W4 = 16


def block_levels(rng, extent, split, smallest, top_value):
    def one(axis_at, shards_of):
        draws = jax.random.uniform(jax.random.fold_in(jax.random.fold_in(rng, 6), axis_at), (shards_of,), jnp.float32, smallest / len(split), top_value / len(split))
        return jnp.repeat(jnp.exp(draws), extent[axis_at] // shards_of).reshape((-1,) + (1,) * (len(extent) - axis_at - 1))

    loudness = one(*split[0])
    for cut in split[1:]:
        loudness = loudness * one(*cut)
    return loudness


def scatter_about(stream_key, shape, spread, bound, cuts=(), held_as=jnp.bfloat16):
    level = block_levels(stream_key, shape, cuts, -0.22, 0.18) if cuts else 1.0
    result = jax.random.normal(stream_key, shape, jnp.float32) * spread * level
    return jnp.minimum(jnp.maximum(result, -bound), bound).astype(held_as)


def setup_inputs(seed: int = 0) -> dict:
    streams_of = jax.random.split(jax.random.key(seed), 10)
    fine_level = scatter_about(streams_of[0], (BATCH, H2, W2, FPN), 1.0, 6.0, ((0, 64), (1, 8)))
    out_grad = scatter_about(streams_of[1], (BATCH, H2, W2, FPN), 1.0, 6.0, ((0, 64), (1, 8)))
    fine_input = scatter_about(streams_of[2], (BATCH, H2, W2, C2), 1.0, 6.0, ((0, 64), (1, 8)))
    mid_input = scatter_about(streams_of[3], (BATCH, H3, W3, C3), 1.0, 6.0, ((0, 64), (3, 8)))
    top_input = scatter_about(streams_of[4], (BATCH, H4, W4, C4), 1.0, 6.0, ((0, 64), (3, 8)))
    smooth_weight = scatter_about(streams_of[5], (3, 3, FPN, FPN), (9 * FPN) ** -0.5, 0.125)
    fine_lateral = scatter_about(streams_of[6], (C2, FPN), FPN ** -0.5, 0.375)
    mid_lateral = scatter_about(streams_of[7], (C3, FPN), FPN ** -0.5, 0.375, ((0, 8),))
    top_lateral = scatter_about(streams_of[8], (C4, FPN), FPN ** -0.5, 0.375, ((0, 8),))
    return dict(fine_level=fine_level, out_grad=out_grad, fine_input=fine_input, mid_input=mid_input, top_input=top_input, smooth_weight=smooth_weight, fine_lateral=fine_lateral, mid_lateral=mid_lateral, top_lateral=top_lateral)


def pool_two(field):
    rows_n, cols_n, chans = field.shape
    return field.reshape(rows_n // 2, 2, cols_n // 2, 2, chans).sum(axis=(1, 3))


def contract_last(left, right):
    return lax.dot_general(left, right, (((1,), (1,)), ((), ())), preferred_element_type=jnp.float32)


def contract_first(left, right):
    return lax.dot_general(left, right, (((0,), (0,)), ((), ())), preferred_element_type=jnp.float32)


def one_image(fine_map, grad_map, fine_in, mid_in, top_in, smooth_weight, fine_lateral, mid_lateral, top_lateral):
    height, width, chans = grad_map.shape
    cells = height * width
    padded = jnp.pad(grad_map, ((1, 1), (1, 1), (0, 0)))
    fine_flat = fine_map.reshape(cells, chans)
    level_grad = jnp.zeros((cells, chans), jnp.float32)
    pieces = []
    for tap_a in range(3):
        for tap_b in range(3):
            shifted = padded[2 - tap_a:2 - tap_a + height, 2 - tap_b:2 - tap_b + width, :].reshape(cells, chans)
            level_grad = level_grad + contract_last(shifted, smooth_weight[tap_a, tap_b])
            pieces.append(contract_first(fine_flat, shifted))
    fine_grad = level_grad.astype(jnp.bfloat16)
    grad_fine = contract_last(fine_grad, fine_lateral).astype(jnp.bfloat16).reshape(height, width, -1)
    pieces.append(contract_first(fine_in.reshape(cells, -1), fine_grad))
    kernel_term = jnp.concatenate(pieces, axis=0)
    mid_grad = pool_two(level_grad.reshape(height, width, chans)).astype(jnp.bfloat16)
    top_grad = pool_two(mid_grad.astype(jnp.float32)).astype(jnp.bfloat16)
    mid_flat = mid_grad.reshape(-1, chans)
    top_flat = top_grad.reshape(-1, chans)
    grad_mid = contract_last(mid_flat, mid_lateral).astype(jnp.bfloat16).reshape(mid_in.shape)
    grad_top = contract_last(top_flat, top_lateral).astype(jnp.bfloat16).reshape(top_in.shape)
    mid_term = contract_first(mid_in.reshape(mid_flat.shape[0], -1), mid_flat)
    top_term = contract_first(top_in.reshape(top_flat.shape[0], -1), top_flat)
    return grad_fine, grad_mid, grad_top, kernel_term, mid_term, top_term


def reference(fine_level, out_grad, fine_input, mid_input, top_input, smooth_weight, fine_lateral, mid_lateral, top_lateral):
    def step(carry, items):
        outs = one_image(items[0], items[1], items[2], items[3], items[4], smooth_weight, fine_lateral, mid_lateral, top_lateral)
        carry = (carry[0] + outs[3], carry[1] + outs[4], carry[2] + outs[5])
        return carry, (outs[0], outs[1], outs[2])

    start = (jnp.zeros((9 * FPN + C2, FPN), jnp.float32), jnp.zeros((C3, FPN), jnp.float32), jnp.zeros((C4, FPN), jnp.float32))
    sums, grads = lax.scan(step, start, (fine_level, out_grad, fine_input, mid_input, top_input))
    return grads[0], grads[1], grads[2], sums[0], sums[1], sums[2]
```

```python
import jax
import jax.numpy as jnp
from jax import lax
from jax.experimental import pallas as pl
from jax.experimental.pallas import tpu as pltpu
from jax.sharding import Mesh
from jax.sharding import PartitionSpec as P

DP = ("dp_0", "dp_1", "dp_2")
MESH = pl.DeviceIdType.MESH
F32 = jnp.float32
BF16 = jnp.bfloat16
NZ, NX, NC, NY = 8, 4, 2, 8
STRIP, WIDTH, CH = 16, 64, 256
CELLS = STRIP * WIDTH
PIECES = 4
PIECE = CELLS // 4 // PIECES


def nt(left, right):
    return lax.dot_general(left, right, (((1,), (1,)), ((), ())), preferred_element_type=F32)


def tn(left, right):
    return lax.dot_general(left, right, (((0,), (0,)), ((), ())), preferred_element_type=F32)


def nn(left, right):
    return lax.dot_general(left, right, (((1,), (0,)), ((), ())), preferred_element_type=F32)


def kernel(
    fl, og, fi, mi, ti, sw, fw, mw, tw,
    gf_o, gm_o, gt_o, kg_o, ml_o, tl_o,
    fl_v, g_v, fi_v, mi_v, ti_v, sw_v, fw_v, mw_v, tw_v,
    big, wt, flt, lvl, tmp, fg, gf_v, gath, top, gm_v, gt_v, macc,
    term, crecv, csum, xrecv, zsend, zrecv, yex, kown, kswap, kg_v,
    bterm, brecv, bsum, bxrecv, bz, bfin, bout,
    in_sem, out_sem, halo_s, halo_r, r_s, r_r, l_s, l_r,
    core_s, core_r, x_s, x_r, z_s, z_r, y_s, y_r, k_s, k_r,
    bc_s, bc_r, bx_s, bx_r, bz_s, bz_r, bf_s, bf_r,
):
    z = lax.axis_index("dp_0")
    x = lax.axis_index("dp_1")
    c = lax.axis_index("dp_2")
    y = lax.axis_index("rows")

    def remote(src, dst, send, recv, **where):
        return pltpu.make_async_remote_copy(
            src_ref=src, dst_ref=dst, send_sem=send, recv_sem=recv,
            device_id=where, device_id_type=MESH,
        )

    loads = [
        pltpu.make_async_copy(og, g_v.at[pl.ds(64, CELLS)], in_sem.at[0]),
        pltpu.make_async_copy(sw, sw_v, in_sem.at[1]),
        pltpu.make_async_copy(fl, fl_v, in_sem.at[2]),
        pltpu.make_async_copy(fi, fi_v, in_sem.at[3]),
        pltpu.make_async_copy(fw, fw_v, in_sem.at[4]),
        pltpu.make_async_copy(mi, mi_v, in_sem.at[5]),
        pltpu.make_async_copy(ti, ti_v, in_sem.at[6]),
        pltpu.make_async_copy(mw, mw_v, in_sem.at[7]),
        pltpu.make_async_copy(tw, tw_v, in_sem.at[8]),
    ]
    for load in loads:
        load.start()

    barrier = pltpu.get_barrier_semaphore()

    def greet(**where):
        pl.semaphore_signal(barrier, inc=1, device_id=where, device_id_type=MESH)

    greet(dp_2=1 - c)
    for d in range(1, NX):
        greet(dp_1=lax.rem(x + d, NX))
        greet(dp_1=lax.rem(x + d, NX), dp_2=1 - c)
    for d in range(1, NZ):
        greet(dp_0=lax.rem(z + d, NZ))
    for d in range(1, NY):
        greet(rows=lax.rem(y + d, NY))

    def widen(first, rows):
        value = g_v[pl.ds(first, rows), :].astype(F32)
        column = lax.rem(lax.broadcasted_iota(jnp.int32, (rows, CH), 0), WIDTH)
        after = jnp.where(column == WIDTH - 1, 0.0, pltpu.roll(value, rows - 1, 0))
        before = jnp.where(column == 0, 0.0, pltpu.roll(value, 1, 0))
        big[pl.ds(first, rows), 0:CH] = after.astype(BF16)
        big[pl.ds(first, rows), CH : 2 * CH] = value.astype(BF16)
        big[pl.ds(first, rows), 2 * CH : 3 * CH] = before.astype(BF16)

    loads[0].wait()

    @pl.loop(0, 4)
    def _(t):
        widen(pl.multiple_of(64 + t * 256, 64), 256)

    loads[1].wait()

    @pl.loop(0, 9)
    def _(k):
        wt[pl.ds(pl.multiple_of(k * CH, CH), CH), :] = sw_v[k].T

    pl.semaphore_wait(barrier, 1 + 2 * (NX - 1) + NZ - 1 + NY - 1)

    down = lax.rem(y + 1, NY)
    up = lax.rem(y + NY - 1, NY)
    halo_down = remote(
        g_v.at[pl.ds(CELLS, 64)], g_v.at[pl.ds(0, 64)], halo_s.at[0], halo_r.at[0], rows=down
    )
    halo_up = remote(
        g_v.at[pl.ds(64, 64)], g_v.at[pl.ds(CELLS + 64, 64)], halo_s.at[1], halo_r.at[1], rows=up
    )
    halo_down.start()
    halo_up.start()

    def ring(h, p, to_down):
        origin = lax.rem(y + NY - (h - 1), NY) if to_down else lax.rem(y + (h - 1), NY)
        block = gath.at[origin, pl.ds(pl.multiple_of(p * PIECE, PIECE), PIECE)]
        send, recv = (r_s, r_r) if to_down else (l_s, l_r)
        return remote(
            block, block, send.at[h - 1, p], recv.at[h - 1, p], rows=down if to_down else up
        )

    def arrived(h, p, from_up):
        origin = lax.rem(y + NY - h, NY) if from_up else lax.rem(y + h, NY)
        block = gath.at[origin, pl.ds(pl.multiple_of(p * PIECE, PIECE), PIECE)]
        send, recv = (r_s, r_r) if from_up else (l_s, l_r)
        return remote(
            block, block, send.at[h - 1, p], recv.at[h - 1, p], rows=down if from_up else up
        )

    def conv(t):
        first = pl.multiple_of(t * 256, 256)
        total = nn(big[pl.ds(first + 128, 256), :], wt[0:768, :])
        total = total + nn(big[pl.ds(first + 64, 256), :], wt[768:1536, :])
        total = total + nn(big[pl.ds(first, 256), :], wt[1536:2304, :])
        fg[pl.ds(first, 256), :] = total.astype(BF16)
        for j in range(2):
            half = total[:, 128 * j : 128 * j + 128]
            lvl[j, 0:64, :] = half[0:64] + half[64:128]
            lvl[j, 64:128, :] = half[128:192] + half[192:256]
            gath[y, pl.ds(pl.multiple_of(t * PIECE, PIECE), PIECE), 128 * j : 128 * j + 128] = (
                lvl[j, pl.ds(0, 64, stride=2), :] + lvl[j, pl.ds(1, 64, stride=2), :]
            ).astype(BF16)

    @pl.loop(1, 3)
    def _(t):
        conv(t)
        ring(1, t, True).start()
        ring(1, t, False).start()

    halo_down.wait_recv()
    halo_up.wait_recv()

    @pl.when(y == 0)
    def _():
        g_v[0:64, :] = jnp.zeros((64, CH), BF16)

    @pl.when(y == NY - 1)
    def _():
        g_v[CELLS + 64 : CELLS + 128, :] = jnp.zeros((64, CH), BF16)

    widen(0, 64)
    widen(CELLS + 64, 64)

    @pl.loop(0, 2)
    def _(i):
        conv(3 * i)
        ring(1, 3 * i, True).start()
        ring(1, 3 * i, False).start()

    def swap_core(k):
        rows = pl.ds(pl.multiple_of(k * CH, CH), CH)
        return remote(
            term.at[1 - c, rows], crecv.at[rows], core_s.at[k], core_r.at[k], dp_2=1 - c
        )

    def put_term(k, value):
        rows = pl.ds(pl.multiple_of(k * CH, CH), CH)
        value = value.astype(BF16)
        term[0, rows, :] = value[:, 0:128]
        term[1, rows, :] = value[:, 128:256]
        swap_core(k).start()

    def tap(k):
        row = pl.multiple_of((2 - k // 3) * 64, 64)
        col = pl.multiple_of(lax.rem(k, 3) * CH, CH)
        put_term(k, nn(flt[...], big[pl.ds(row, CELLS), pl.ds(col, CH)]))

    def step(h):
        for p in range(PIECES):
            arrived(h, p, True).wait_recv()
            if h < 3 or p < 2:
                ring(h + 1, p, True).start()
            arrived(h, p, False).wait_recv()
            if h < 3 or p >= 2:
                ring(h + 1, p, False).start()

    def coarse(s):
        mid = gath[s]
        cells = pl.ds(pl.multiple_of(s * CH, CH), CH)
        gm_v[cells, :] = nt(mid, mw_v[...]).astype(BF16)
        macc[0:64, :] += tn(mi_v[cells, :], mid)
        wide = mid.astype(F32)
        for j in range(2):
            half = wide[:, 128 * j : 128 * j + 128]
            for i in range(4):
                tmp[j, 32 * i : 32 * i + 32, :] = (
                    half[64 * i : 64 * i + 32] + half[64 * i + 32 : 64 * i + 64]
                )
            top[:, 128 * j : 128 * j + 128] = (
                tmp[j, pl.ds(0, 64, stride=2), :] + tmp[j, pl.ds(1, 64, stride=2), :]
            ).astype(BF16)
        small = top[...]
        cells = pl.ds(pl.multiple_of(s * 64, 64), 64)
        gt_v[cells, :] = nt(small, tw_v[...]).astype(BF16)
        macc[64:192, :] += tn(ti_v[cells, :], small)

    loads[2].wait()

    @pl.loop(0, 4)
    def _(t):
        rows = pl.ds(pl.multiple_of(t * 256, 256), 256)
        flt[:, rows] = fl_v[rows, :].T

    @pl.loop(0, 5)
    def _(k):
        tap(k)

    step(1)

    @pl.loop(5, 9)
    def _(k):
        tap(k)

    loads[3].wait()
    put_term(9, tn(fi_v[...], fg[...]))

    for load in loads[4:]:
        load.wait()
    macc[...] = jnp.zeros_like(macc)
    coarse(y)
    step(2)

    @pl.loop(0, 10)
    def _(k):
        swap_core(k).wait_recv()
        rows = pl.ds(pl.multiple_of(k * CH, CH), CH)
        csum[rows, :] = (term[c, rows, :].astype(F32) + crecv[rows, :].astype(F32)).astype(BF16)

    def x_copy(s, d):
        z_to = lax.rem(z + s + 1, NZ)
        x_to = lax.rem(x + d, NX)
        rows = pl.ds(pl.multiple_of((z_to * NX + x_to) * 80, 80), 80)
        return remote(
            csum.at[rows], xrecv.at[s, d - 1], x_s.at[s, d - 1], x_r.at[s, d - 1], dp_1=x_to
        )

    @pl.loop(0, NZ)
    def _(s):
        for d in range(1, NX):
            x_copy(s, d).start()

    coarse(lax.rem(y + 1, NY))
    coarse(lax.rem(y + NY - 1, NY))
    step(3)

    def z_copy(s):
        return remote(
            zsend.at[s], zrecv.at[s], z_s.at[s], z_r.at[s], dp_0=lax.rem(z + s + 1, NZ)
        )

    def x_reduce(s):
        for d in range(1, NX):
            x_copy(s, d).wait_recv()
        z_to = lax.rem(z + s + 1, NZ)
        rows = pl.ds(pl.multiple_of((z_to * NX + x) * 80, 80), 80)
        total = csum[rows, :].astype(F32)
        for d in range(1, NX):
            total = total + xrecv[s, d - 1].astype(F32)
        zsend[s] = total.astype(BF16)

    @pl.loop(0, NZ - 1)
    def _(s):
        x_reduce(s)
        z_copy(s).start()

    x_reduce(NZ - 1)

    for k in range(4):
        rows = slice(256 * k, 256 * k + 256)
        gf_v[rows, :] = nt(fg[rows, :], fw_v[...]).astype(BF16)
    stores = [pltpu.make_async_copy(gf_v, gf_o, out_sem.at[0])]
    stores[0].start()

    coarse(lax.rem(y + 2, NY))
    coarse(lax.rem(y + NY - 2, NY))
    coarse(lax.rem(y + 3, NY))
    coarse(lax.rem(y + NY - 3, NY))

    for p in range(2):
        arrived(4, p, True).wait_recv()
        arrived(4, p + 2, False).wait_recv()
    coarse(lax.rem(y + 4, NY))

    stores.append(pltpu.make_async_copy(gm_v, gm_o, out_sem.at[1]))
    stores.append(pltpu.make_async_copy(gt_v, gt_o, out_sem.at[2]))
    stores[1].start()
    stores[2].start()

    bterm[0] = macc[:, 0:128].astype(BF16)
    bterm[1] = macc[:, 128:256].astype(BF16)
    b_core = remote(bterm.at[1 - c], brecv, bc_s.at[0], bc_r.at[0], dp_2=1 - c)
    b_core.start()

    @pl.loop(0, NZ - 1)
    def _(s):
        z_copy(s).wait_recv()

    total = zsend[NZ - 1].astype(F32)
    for s in range(NZ - 1):
        total = total + zrecv[s].astype(F32)
    yex[y] = total.astype(BF16)

    def y_copy(d):
        return remote(
            yex.at[y], yex.at[y], y_s.at[d - 1], y_r.at[d - 1], rows=lax.rem(y + d, NY)
        )

    def y_arrived(d):
        block = yex.at[lax.rem(y + NY - d, NY)]
        return remote(
            block, block, y_s.at[d - 1], y_r.at[d - 1], rows=lax.rem(y + d, NY)
        )

    for d in range(1, NY):
        y_copy(d).start()

    b_core.wait_recv()
    bsum[...] = (bterm[c].astype(F32) + brecv[...].astype(F32)).astype(BF16)

    def bx_copy(d):
        x_to = lax.rem(x + d, NX)
        rows = pl.ds(pl.multiple_of(x_to * 48, 48), 48)
        return remote(bsum.at[rows], bxrecv.at[d - 1], bx_s.at[d - 1], bx_r.at[d - 1], dp_1=x_to)

    for d in range(1, NX):
        bx_copy(d).start()
    for d in range(1, NX):
        bx_copy(d).wait_recv()
    total = bsum[pl.ds(pl.multiple_of(x * 48, 48), 48), :].astype(F32)
    for d in range(1, NX):
        total = total + bxrecv[d - 1].astype(F32)
    bz[z] = total.astype(BF16)

    def bz_copy(d):
        return remote(bz.at[z], bz.at[z], bz_s.at[d - 1], bz_r.at[d - 1], dp_0=lax.rem(z + d, NZ))

    def bz_arrived(d):
        block = bz.at[lax.rem(z + NZ - d, NZ)]
        return remote(block, block, bz_s.at[d - 1], bz_r.at[d - 1], dp_0=lax.rem(z + d, NZ))

    for d in range(1, NZ):
        bz_copy(d).start()

    for d in range(1, NY):
        y_arrived(d).wait_recv()
    total = yex[0].astype(F32)
    for i in range(1, NY):
        total = total + yex[i].astype(F32)
    kown[...] = total
    k_copy = remote(
        kown.at[pl.ds(pl.multiple_of((1 - c) * 40, 8), 40)], kswap, k_s.at[0], k_r.at[0], dp_2=1 - c
    )
    k_copy.start()

    for d in range(1, NZ):
        bz_arrived(d).wait_recv()
    total = bz[0].astype(F32)
    for i in range(1, NZ):
        total = total + bz[i].astype(F32)
    bfin[x, c] = total.astype(BF16)

    def bf_copy(d, e):
        return remote(
            bfin.at[x, c], bfin.at[x, c], bf_s.at[d, e], bf_r.at[d, e],
            dp_1=lax.rem(x + d, NX), dp_2=lax.rem(c + e, NC),
        )

    def bf_arrived(d, e):
        block = bfin.at[lax.rem(x + NX - d, NX), lax.rem(c + e, NC)]
        return remote(
            block, block, bf_s.at[d, e], bf_r.at[d, e],
            dp_1=lax.rem(x + d, NX), dp_2=lax.rem(c + e, NC),
        )

    others = [(d, e) for d in range(NX) for e in range(NC) if d or e]
    for d, e in others:
        bf_copy(d, e).start()

    k_copy.wait_recv()
    kg_v[:, pl.ds(pl.multiple_of(c * 128, 128), 128)] = kown[
        pl.ds(pl.multiple_of(c * 40, 8), 40), :
    ]
    kg_v[:, pl.ds(pl.multiple_of((1 - c) * 128, 128), 128)] = kswap[...]
    stores.append(pltpu.make_async_copy(kg_v, kg_o, out_sem.at[3]))
    stores[3].start()

    for d, e in others:
        bf_arrived(d, e).wait_recv()
    for i in range(NX):
        for j in range(NC):
            bout[48 * i : 48 * i + 48, 128 * j : 128 * j + 128] = bfin[i, j].astype(F32)
    stores.append(pltpu.make_async_copy(bout.at[0:64], ml_o, out_sem.at[4]))
    stores.append(pltpu.make_async_copy(bout.at[64:192], tl_o, out_sem.at[5]))
    stores[4].start()
    stores[5].start()

    halo_down.wait_send()
    halo_up.wait_send()
    for h in range(1, 5):
        for p in range(PIECES):
            if h < 4 or p < 2:
                ring(h, p, True).wait_send()
            if h < 4 or p >= 2:
                ring(h, p, False).wait_send()

    @pl.loop(0, 10)
    def _(k):
        swap_core(k).wait_send()

    @pl.loop(0, NZ)
    def _(s):
        for d in range(1, NX):
            x_copy(s, d).wait_send()

    @pl.loop(0, NZ - 1)
    def _(s):
        z_copy(s).wait_send()

    for d in range(1, NY):
        y_copy(d).wait_send()
    b_core.wait_send()
    for d in range(1, NX):
        bx_copy(d).wait_send()
    for d in range(1, NZ):
        bz_copy(d).wait_send()
    k_copy.wait_send()
    for d, e in others:
        bf_copy(d, e).wait_send()
    for store in stores:
        store.wait()


def body(
    fine_level, out_grad, fine_input, mid_input, top_input,
    smooth_weight, fine_lateral, mid_lateral, top_lateral,
):
    sem = pltpu.SemaphoreType.DMA
    sizes = [
        ((CELLS, CH), BF16), ((CELLS + 128, CH), BF16), ((CELLS, CH), BF16), ((2048, 64), BF16),
        ((512, 128), BF16), ((9, CH, CH), BF16), ((CH, CH), BF16), ((64, CH), BF16), ((128, CH), BF16),
        ((CELLS + 128, 3 * CH), BF16), ((9 * CH, CH), BF16), ((CH, CELLS), BF16),
        ((2, 128, 128), F32), ((2, 128, 128), F32), ((CELLS, CH), BF16), ((CELLS, CH), BF16),
        ((NY, CH, CH), BF16), ((64, CH), BF16), ((2048, 64), BF16), ((512, 128), BF16), ((192, CH), F32),
        ((2, 2560, 128), BF16), ((2560, 128), BF16), ((2560, 128), BF16), ((NZ, NX - 1, 80, 128), BF16),
        ((NZ, 80, 128), BF16), ((NZ - 1, 80, 128), BF16), ((NY, 80, 128), BF16), ((80, 128), F32),
        ((40, 128), F32), ((40, CH), F32),
        ((2, 192, 128), BF16), ((192, 128), BF16), ((192, 128), BF16), ((NX - 1, 48, 128), BF16),
        ((NZ, 48, 128), BF16), ((NX, NC, 48, 128), BF16), ((192, CH), F32),
    ]
    sems = [
        (9,), (6,), (2,), (2,), (4, PIECES), (4, PIECES), (4, PIECES), (4, PIECES),
        (10,), (10,), (NZ, NX - 1), (NZ, NX - 1), (NZ - 1,), (NZ - 1,), (NY - 1,), (NY - 1,), (1,), (1,),
        (1,), (1,), (NX - 1,), (NX - 1,), (NZ - 1,), (NZ - 1,), (NX, NC), (NX, NC),
    ]
    hbm = pl.BlockSpec(memory_space=pl.ANY)
    grads = pl.pallas_call(
        kernel,
        out_shape=[
            jax.ShapeDtypeStruct((CELLS, CH), BF16),
            jax.ShapeDtypeStruct((2048, 64), BF16),
            jax.ShapeDtypeStruct((512, 128), BF16),
            jax.ShapeDtypeStruct((40, CH), F32),
            jax.ShapeDtypeStruct((64, CH), F32),
            jax.ShapeDtypeStruct((128, CH), F32),
        ],
        in_specs=[hbm] * 9,
        out_specs=[hbm] * 6,
        scratch_shapes=[pltpu.VMEM(*size) for size in sizes] + [sem(size) for size in sems],
        compiler_params=pltpu.CompilerParams(
            collective_id=0, has_side_effects=True, vmem_limit_bytes=40 * 1024 * 1024
        ),
    )(
        fine_level.reshape(CELLS, CH), out_grad.reshape(CELLS, CH), fine_input.reshape(CELLS, CH),
        mid_input.reshape(2048, 64), top_input.reshape(512, 128), smooth_weight.reshape(9, CH, CH),
        fine_lateral, mid_lateral, top_lateral,
    )
    return (
        grads[0].reshape(out_grad.shape), grads[1].reshape(mid_input.shape),
        grads[2].reshape(top_input.shape), grads[3], grads[4], grads[5],
    )


def solution(mesh):
    torus = Mesh(
        mesh.devices.reshape(NZ, NX, NC, NY), ("dp_0", "dp_1", "dp_2", "rows")
    )
    return jax.shard_map(
        body,
        mesh=torus,
        in_specs=(
            P(DP, "rows", None, None), P(DP, "rows", None, None), P(DP, "rows", None, None),
            P(DP, None, None, "rows"), P(DP, None, None, "rows"),
            P(), P(), P("rows", None), P("rows", None),
        ),
        out_specs=(
            P(DP, "rows", None, None), P(DP, None, None, "rows"), P(DP, None, None, "rows"),
            P(DP, None), P("rows", None), P("rows", None),
        ),
        check_vma=False,
    )
```

```python
import jax
import jax.numpy as jnp
from jax import lax
from jax.experimental import pallas as pl
from jax.experimental.pallas import tpu as pltpu
from jax.sharding import Mesh
from jax.sharding import PartitionSpec as P

DP = ("dp_0", "dp_1", "dp_2")
MESH = pl.DeviceIdType.MESH
F32 = jnp.float32
BF16 = jnp.bfloat16
NZ, NX, NC, NY = 8, 4, 2, 8
STRIP, WIDTH, CH = 16, 64, 256
CELLS = STRIP * WIDTH
PIECES = ((32, 64), (96, 64), (160, 64), (0, 32), (224, 32))
INNER, EDGES = (0, 1, 2), (3, 4)
LAST_DOWN, LAST_UP = (0, 1), (2, 3, 4)


def nt(left, right):
    return lax.dot_general(left, right, (((1,), (1,)), ((), ())), preferred_element_type=F32)


def tn(left, right):
    return lax.dot_general(left, right, (((0,), (0,)), ((), ())), preferred_element_type=F32)


def nn(left, right):
    return lax.dot_general(left, right, (((1,), (0,)), ((), ())), preferred_element_type=F32)


def kernel(
    fl, og, fi, mi, ti, sw, fw, mw, tw,
    gf_o, gm_o, gt_o, kg_o, ml_o, tl_o,
    fl_v, g_v, fi_v, mi_v, ti_v, sw_v, fw_v, mw_v, tw_v,
    big, wt, flt, lvl, tmp, fg, gf_v, gath, top, gm_v, gt_v, macc,
    term, crecv, csum, xrecv, zsend, zrecv, yex, kown, kswap, kg_v,
    bterm, bxrecv, bz, bfin, bout,
    in_sem, out_sem, halo_s, halo_r, r_s, r_r, l_s, l_r,
    core_s, core_r, x_s, x_r, z_s, z_r, y_s, y_r, k_s, k_r,
    bx_s, bx_r, bz_s, bz_r, bf_s, bf_r,
):
    z = lax.axis_index("dp_0")
    x = lax.axis_index("dp_1")
    c = lax.axis_index("dp_2")
    y = lax.axis_index("rows")

    def remote(src, dst, send, recv, **where):
        return pltpu.make_async_remote_copy(
            src_ref=src, dst_ref=dst, send_sem=send, recv_sem=recv,
            device_id=where, device_id_type=MESH,
        )

    loads = [
        pltpu.make_async_copy(og, g_v.at[pl.ds(64, CELLS)], in_sem.at[0]),
        pltpu.make_async_copy(sw, sw_v, in_sem.at[1]),
        pltpu.make_async_copy(fl, fl_v, in_sem.at[2]),
        pltpu.make_async_copy(fi, fi_v, in_sem.at[3]),
        pltpu.make_async_copy(fw, fw_v, in_sem.at[4]),
        pltpu.make_async_copy(mi, mi_v, in_sem.at[5]),
        pltpu.make_async_copy(ti, ti_v, in_sem.at[6]),
        pltpu.make_async_copy(mw, mw_v, in_sem.at[7]),
        pltpu.make_async_copy(tw, tw_v, in_sem.at[8]),
    ]
    for load in loads[:3]:
        load.start()

    barrier = pltpu.get_barrier_semaphore()

    def greet(**where):
        pl.semaphore_signal(barrier, inc=1, device_id=where, device_id_type=MESH)

    greet(dp_2=1 - c)
    for d in range(1, NX):
        greet(dp_1=lax.rem(x + d, NX))
        greet(dp_1=lax.rem(x + d, NX), dp_2=1 - c)
    for d in range(1, NZ):
        greet(dp_0=lax.rem(z + d, NZ))
    for d in range(1, NY):
        greet(rows=lax.rem(y + d, NY))

    def widen(first, rows):
        value = g_v[pl.ds(first, rows), :].astype(F32)
        column = lax.rem(lax.broadcasted_iota(jnp.int32, (rows, CH), 0), WIDTH)
        after = jnp.where(column == WIDTH - 1, 0.0, pltpu.roll(value, rows - 1, 0))
        before = jnp.where(column == 0, 0.0, pltpu.roll(value, 1, 0))
        big[pl.ds(first, rows), 0:CH] = after.astype(BF16)
        big[pl.ds(first, rows), CH : 2 * CH] = value.astype(BF16)
        big[pl.ds(first, rows), 2 * CH : 3 * CH] = before.astype(BF16)

    loads[0].wait()

    @pl.loop(0, 4)
    def _(t):
        widen(pl.multiple_of(64 + t * 256, 64), 256)

    loads[1].wait()

    @pl.loop(0, 9)
    def _(k):
        wt[pl.ds(pl.multiple_of(k * CH, CH), CH), :] = sw_v[k].T

    for load in loads[3:]:
        load.start()

    pl.semaphore_wait(barrier, 1 + 2 * (NX - 1) + NZ - 1 + NY - 1)

    down = lax.rem(y + 1, NY)
    up = lax.rem(y + NY - 1, NY)
    halo_down = remote(
        g_v.at[pl.ds(CELLS, 64)], g_v.at[pl.ds(0, 64)], halo_s.at[0], halo_r.at[0], rows=down
    )
    halo_up = remote(
        g_v.at[pl.ds(64, 64)], g_v.at[pl.ds(CELLS + 64, 64)], halo_s.at[1], halo_r.at[1], rows=up
    )
    halo_down.start()
    halo_up.start()

    def hop(h, p, to_down, sent):
        away = h - 1 if sent else h
        origin = lax.rem(y + NY - away, NY) if to_down else lax.rem(y + away, NY)
        first, count = PIECES[p] if isinstance(p, int) else (pl.multiple_of(32 + 64 * p, 32), 64)
        block = gath.at[origin, pl.ds(first, count)]
        send, recv = (r_s, r_r) if to_down else (l_s, l_r)
        return remote(
            block, block, send.at[h - 1, p], recv.at[h - 1, p], rows=down if to_down else up
        )

    def start_own(p):
        hop(1, p, True, True).start()
        hop(1, p, False, True).start()

    def goes(h, p, to_down):
        return h < 4 or p in (LAST_DOWN if to_down else LAST_UP)

    def forward(h, pieces):
        for p in pieces:
            for to_down in (True, False):
                if goes(h, p, to_down):
                    hop(h, p, to_down, False).wait_recv()
                if h < 4 and goes(h + 1, p, to_down):
                    hop(h + 1, p, to_down, True).start()

    def conv(first, cells, out):
        total = nn(big[pl.ds(first + 128, cells), :], wt[0:768, :])
        total = total + nn(big[pl.ds(first + 64, cells), :], wt[768:1536, :])
        total = total + nn(big[pl.ds(first, cells), :], wt[1536:2304, :])
        fg[pl.ds(first, cells), :] = total.astype(BF16)
        for j in range(2):
            half = total[:, 128 * j : 128 * j + 128]
            for i in range(cells // 128):
                lvl[j, 64 * i : 64 * i + 64, :] = (
                    half[128 * i : 128 * i + 64] + half[128 * i + 64 : 128 * i + 128]
                )
            gath[y, pl.ds(out, cells // 4), 128 * j : 128 * j + 128] = (
                lvl[j, pl.ds(0, cells // 4, stride=2), :] + lvl[j, pl.ds(1, cells // 4, stride=2), :]
            ).astype(BF16)

    @pl.loop(0, 3)
    def _(t):
        conv(pl.multiple_of(128 + 256 * t, 128), 256, pl.multiple_of(32 + 64 * t, 32))
        start_own(t)

    def swap_core(k):
        rows = pl.ds(pl.multiple_of(k * CH, CH), CH)
        return remote(
            term.at[1 - c, rows], crecv.at[rows], core_s.at[k], core_r.at[k], dp_2=1 - c
        )

    def put_term(k, value):
        rows = pl.ds(pl.multiple_of(k * CH, CH), CH)
        value = value.astype(BF16)
        term[0, rows, :] = value[:, 0:128]
        term[1, rows, :] = value[:, 128:256]
        swap_core(k).start()

    def tap(k):
        row = pl.multiple_of((2 - k // 3) * 64, 64)
        col = pl.multiple_of(lax.rem(k, 3) * CH, CH)
        put_term(k, nn(flt[...], big[pl.ds(row, CELLS), pl.ds(col, CH)]))

    loads[2].wait()

    @pl.loop(0, 4)
    def _(t):
        rows = pl.ds(pl.multiple_of(t * 256, 256), 256)
        flt[:, rows] = fl_v[rows, :].T

    @pl.loop(3, 6)
    def _(k):
        tap(k)

    halo_down.wait_recv()
    halo_up.wait_recv()

    @pl.when(y == 0)
    def _():
        g_v[0:64, :] = jnp.zeros((64, CH), BF16)

    @pl.when(y == NY - 1)
    def _():
        g_v[CELLS + 64 : CELLS + 128, :] = jnp.zeros((64, CH), BF16)

    widen(0, 64)
    widen(CELLS + 64, 64)

    for p in EDGES:
        first, count = PIECES[p]
        conv(4 * first, 4 * count, first)
        start_own(p)

    forward(1, INNER)

    @pl.loop(0, 3)
    def _(k):
        tap(k)

    forward(1, EDGES)

    @pl.loop(6, 9)
    def _(k):
        tap(k)

    def coarse(s):
        mid = gath[s]
        cells = pl.ds(pl.multiple_of(s * CH, CH), CH)
        gm_v[cells, :] = nt(mid, mw_v[...]).astype(BF16)
        macc[0:64, :] += tn(mi_v[cells, :], mid)
        wide = mid.astype(F32)
        for j in range(2):
            half = wide[:, 128 * j : 128 * j + 128]
            for i in range(4):
                tmp[j, 32 * i : 32 * i + 32, :] = (
                    half[64 * i : 64 * i + 32] + half[64 * i + 32 : 64 * i + 64]
                )
            top[:, 128 * j : 128 * j + 128] = (
                tmp[j, pl.ds(0, 64, stride=2), :] + tmp[j, pl.ds(1, 64, stride=2), :]
            ).astype(BF16)
        small = top[...]
        cells = pl.ds(pl.multiple_of(s * 64, 64), 64)
        gt_v[cells, :] = nt(small, tw_v[...]).astype(BF16)
        macc[64:192, :] += tn(ti_v[cells, :], small)

    loads[3].wait()
    put_term(9, tn(fi_v[...], fg[...]))

    for load in loads[4:]:
        load.wait()
    macc[...] = jnp.zeros_like(macc)
    coarse(y)
    forward(2, INNER)

    @pl.loop(0, 10)
    def _(k):
        swap_core(k).wait_recv()
        rows = pl.ds(pl.multiple_of(k * CH, CH), CH)
        csum[rows, :] = (term[c, rows, :].astype(F32) + crecv[rows, :].astype(F32)).astype(BF16)

    def x_copy(s, d):
        z_to = lax.rem(z + s + 1, NZ)
        x_to = lax.rem(x + d, NX)
        rows = pl.ds(pl.multiple_of((z_to * NX + x_to) * 80, 80), 80)
        return remote(
            csum.at[rows], xrecv.at[s, d - 1], x_s.at[s, d - 1], x_r.at[s, d - 1], dp_1=x_to
        )

    @pl.loop(0, NZ)
    def _(s):
        for d in range(1, NX):
            x_copy(s, d).start()

    coarse(lax.rem(y + 1, NY))
    coarse(lax.rem(y + NY - 1, NY))
    forward(2, EDGES)
    coarse(lax.rem(y + 2, NY))
    coarse(lax.rem(y + NY - 2, NY))
    forward(3, INNER)
    forward(3, EDGES)

    def z_copy(s):
        return remote(
            zsend.at[s], zrecv.at[s], z_s.at[s], z_r.at[s], dp_0=lax.rem(z + s + 1, NZ)
        )

    def x_reduce(s):
        for d in range(1, NX):
            x_copy(s, d).wait_recv()
        z_to = lax.rem(z + s + 1, NZ)
        rows = pl.ds(pl.multiple_of((z_to * NX + x) * 80, 80), 80)
        total = csum[rows, :].astype(F32)
        for d in range(1, NX):
            total = total + xrecv[s, d - 1].astype(F32)
        zsend[s] = total.astype(BF16)

    @pl.loop(0, NZ - 1)
    def _(s):
        x_reduce(s)
        z_copy(s).start()

    x_reduce(NZ - 1)

    for k in range(4):
        rows = slice(256 * k, 256 * k + 256)
        gf_v[rows, :] = nt(fg[rows, :], fw_v[...]).astype(BF16)
    stores = [pltpu.make_async_copy(gf_v, gf_o, out_sem.at[0])]
    stores[0].start()

    coarse(lax.rem(y + 3, NY))
    coarse(lax.rem(y + NY - 3, NY))

    forward(4, INNER + EDGES)
    coarse(lax.rem(y + 4, NY))

    stores.append(pltpu.make_async_copy(gm_v, gm_o, out_sem.at[1]))
    stores.append(pltpu.make_async_copy(gt_v, gt_o, out_sem.at[2]))
    stores[1].start()
    stores[2].start()

    others = [(d, e) for d in range(NX) for e in range(NC) if d or e]
    for i in range(NX):
        for j in range(NC):
            bterm[i, j] = macc[48 * i : 48 * i + 48, 128 * j : 128 * j + 128].astype(BF16)

    def bx_copy(d, e):
        x_to, c_to = lax.rem(x + d, NX), lax.rem(c + e, NC)
        return remote(
            bterm.at[x_to, c_to], bxrecv.at[d, e], bx_s.at[d, e], bx_r.at[d, e],
            dp_1=x_to, dp_2=c_to,
        )

    for d, e in others:
        bx_copy(d, e).start()

    for d, e in others:
        bx_copy(d, e).wait_recv()
    total = bterm[x, c].astype(F32)
    for d, e in others:
        total = total + bxrecv[d, e].astype(F32)
    bz[z] = total.astype(BF16)

    def bz_copy(d):
        return remote(bz.at[z], bz.at[z], bz_s.at[d - 1], bz_r.at[d - 1], dp_0=lax.rem(z + d, NZ))

    def bz_arrived(d):
        block = bz.at[lax.rem(z + NZ - d, NZ)]
        return remote(block, block, bz_s.at[d - 1], bz_r.at[d - 1], dp_0=lax.rem(z + d, NZ))

    for d in range(1, NZ):
        bz_copy(d).start()

    @pl.loop(0, NZ - 1)
    def _(s):
        z_copy(s).wait_recv()

    total = zsend[NZ - 1].astype(F32)
    for s in range(NZ - 1):
        total = total + zrecv[s].astype(F32)
    yex[y] = total.astype(BF16)

    def y_copy(d):
        return remote(
            yex.at[y], yex.at[y], y_s.at[d - 1], y_r.at[d - 1], rows=lax.rem(y + d, NY)
        )

    def y_arrived(d):
        block = yex.at[lax.rem(y + NY - d, NY)]
        return remote(
            block, block, y_s.at[d - 1], y_r.at[d - 1], rows=lax.rem(y + d, NY)
        )

    for d in range(1, NY):
        y_copy(d).start()

    for d in range(1, NY):
        y_arrived(d).wait_recv()
    total = yex[0].astype(F32)
    for i in range(1, NY):
        total = total + yex[i].astype(F32)
    kown[...] = total
    k_copy = remote(
        kown.at[pl.ds(pl.multiple_of((1 - c) * 40, 8), 40)], kswap, k_s.at[0], k_r.at[0], dp_2=1 - c
    )
    k_copy.start()

    for d in range(1, NZ):
        bz_arrived(d).wait_recv()
    total = bz[0].astype(F32)
    for i in range(1, NZ):
        total = total + bz[i].astype(F32)
    bfin[x, c] = total.astype(BF16)

    def bf_copy(d, e):
        return remote(
            bfin.at[x, c], bfin.at[x, c], bf_s.at[d, e], bf_r.at[d, e],
            dp_1=lax.rem(x + d, NX), dp_2=lax.rem(c + e, NC),
        )

    def bf_arrived(d, e):
        block = bfin.at[lax.rem(x + NX - d, NX), lax.rem(c + e, NC)]
        return remote(
            block, block, bf_s.at[d, e], bf_r.at[d, e],
            dp_1=lax.rem(x + d, NX), dp_2=lax.rem(c + e, NC),
        )

    for d, e in others:
        bf_copy(d, e).start()

    k_copy.wait_recv()
    kg_v[:, pl.ds(pl.multiple_of(c * 128, 128), 128)] = kown[
        pl.ds(pl.multiple_of(c * 40, 8), 40), :
    ]
    kg_v[:, pl.ds(pl.multiple_of((1 - c) * 128, 128), 128)] = kswap[...]
    stores.append(pltpu.make_async_copy(kg_v, kg_o, out_sem.at[3]))
    stores[3].start()

    for d, e in others:
        bf_arrived(d, e).wait_recv()
    for i in range(NX):
        for j in range(NC):
            bout[48 * i : 48 * i + 48, 128 * j : 128 * j + 128] = bfin[i, j].astype(F32)
    stores.append(pltpu.make_async_copy(bout.at[0:64], ml_o, out_sem.at[4]))
    stores.append(pltpu.make_async_copy(bout.at[64:192], tl_o, out_sem.at[5]))
    stores[4].start()
    stores[5].start()

    halo_down.wait_send()
    halo_up.wait_send()
    for h in range(1, 5):
        for p in range(len(PIECES)):
            for to_down in (True, False):
                if goes(h, p, to_down):
                    hop(h, p, to_down, True).wait_send()

    @pl.loop(0, 10)
    def _(k):
        swap_core(k).wait_send()

    @pl.loop(0, NZ)
    def _(s):
        for d in range(1, NX):
            x_copy(s, d).wait_send()

    @pl.loop(0, NZ - 1)
    def _(s):
        z_copy(s).wait_send()

    for d in range(1, NY):
        y_copy(d).wait_send()
    for d, e in others:
        bx_copy(d, e).wait_send()
    for d in range(1, NZ):
        bz_copy(d).wait_send()
    k_copy.wait_send()
    for d, e in others:
        bf_copy(d, e).wait_send()
    for store in stores:
        store.wait()


def store(*refs):
    copies = [pltpu.make_async_copy(refs[i], refs[6 + i], refs[12].at[i]) for i in range(6)]
    for copy in copies:
        copy.start()
    for copy in copies:
        copy.wait()


def body(
    fine_level, out_grad, fine_input, mid_input, top_input,
    smooth_weight, fine_lateral, mid_lateral, top_lateral,
):
    sem = pltpu.SemaphoreType.DMA
    sizes = [
        ((CELLS, CH), BF16), ((CELLS + 128, CH), BF16), ((CELLS, CH), BF16), ((2048, 64), BF16),
        ((512, 128), BF16), ((9, CH, CH), BF16), ((CH, CH), BF16), ((64, CH), BF16), ((128, CH), BF16),
        ((CELLS + 128, 3 * CH), BF16), ((9 * CH, CH), BF16), ((CH, CELLS), BF16),
        ((2, 128, 128), F32), ((2, 128, 128), F32), ((CELLS, CH), BF16), ((CELLS, CH), BF16),
        ((NY, CH, CH), BF16), ((64, CH), BF16), ((2048, 64), BF16), ((512, 128), BF16), ((192, CH), F32),
        ((2, 2560, 128), BF16), ((2560, 128), BF16), ((2560, 128), BF16), ((NZ, NX - 1, 80, 128), BF16),
        ((NZ, 80, 128), BF16), ((NZ - 1, 80, 128), BF16), ((NY, 80, 128), BF16), ((80, 128), F32),
        ((40, 128), F32), ((40, CH), F32),
        ((NX, NC, 48, 128), BF16), ((NX, NC, 48, 128), BF16),
        ((NZ, 48, 128), BF16), ((NX, NC, 48, 128), BF16), ((192, CH), F32),
    ]
    sems = [
        (9,), (6,), (2,), (2,), (4, 5), (4, 5), (4, 5), (4, 5),
        (10,), (10,), (NZ, NX - 1), (NZ, NX - 1), (NZ - 1,), (NZ - 1,), (NY - 1,), (NY - 1,), (1,), (1,),
        (NX, NC), (NX, NC), (NZ - 1,), (NZ - 1,), (NX, NC), (NX, NC),
    ]
    shapes = [
        ((CELLS, CH), BF16), ((2048, 64), BF16), ((512, 128), BF16),
        ((40, CH), F32), ((64, CH), F32), ((128, CH), F32),
    ]
    hbm = pl.BlockSpec(memory_space=pltpu.HBM)
    anywhere = pl.BlockSpec(memory_space=pl.ANY)
    grads = pl.pallas_call(
        kernel,
        out_shape=[pltpu.VMEM(*shape) for shape in shapes],
        in_specs=[hbm] * 9,
        out_specs=[anywhere] * 6,
        scratch_shapes=[pltpu.VMEM(*size) for size in sizes] + [sem(size) for size in sems],
        compiler_params=pltpu.CompilerParams(
            collective_id=0, has_side_effects=True, vmem_limit_bytes=48 * 1024 * 1024
        ),
    )(*(pltpu.with_memory_space_constraint(value, pltpu.HBM) for value in (
        fine_level.reshape(CELLS, CH), out_grad.reshape(CELLS, CH), fine_input.reshape(CELLS, CH),
        mid_input.reshape(2048, 64), top_input.reshape(512, 128), smooth_weight.reshape(9, CH, CH),
        fine_lateral, mid_lateral, top_lateral,
    )))
    grads = pl.pallas_call(
        store,
        out_shape=[pltpu.HBM(*shape) for shape in shapes],
        in_specs=[anywhere] * 6,
        out_specs=[hbm] * 6,
        scratch_shapes=[sem((6,))],
    )(*(pltpu.with_memory_space_constraint(grad, pltpu.VMEM) for grad in grads))
    return (
        grads[0].reshape(out_grad.shape), grads[1].reshape(mid_input.shape),
        grads[2].reshape(top_input.shape), grads[3], grads[4], grads[5],
    )


def solution(mesh):
    torus = Mesh(
        mesh.devices.reshape(NZ, NX, NC, NY), ("dp_0", "dp_1", "dp_2", "rows")
    )
    return jax.shard_map(
        body,
        mesh=torus,
        in_specs=(
            P(DP, "rows", None, None), P(DP, "rows", None, None), P(DP, "rows", None, None),
            P(DP, None, None, "rows"), P(DP, None, None, "rows"),
            P(), P(), P("rows", None), P("rows", None),
        ),
        out_specs=(
            P(DP, "rows", None, None), P(DP, None, None, "rows"), P(DP, None, None, "rows"),
            P(DP, None), P("rows", None), P("rows", None),
        ),
        check_vma=False,
    )
```

```python
import jax
import jax.numpy as jnp
from jax import lax
from jax.experimental import pallas as pl
from jax.experimental.pallas import tpu as pltpu
from jax.sharding import Mesh
from jax.sharding import PartitionSpec as P

DP = ("dp_0", "dp_1", "dp_2")
MESH = pl.DeviceIdType.MESH
F32 = jnp.float32
BF16 = jnp.bfloat16
NZ, NX, NC, NY = 8, 4, 2, 8
STRIP, WIDTH, CH = 16, 64, 256
CELLS = STRIP * WIDTH
PIECES = ((32, 64), (96, 64), (160, 64), (0, 32), (224, 32))
INNER, EDGES = (0, 1, 2), (3, 4)
LAST_DOWN, LAST_UP = (0, 1), (2, 3, 4)


def nt(left, right):
    return lax.dot_general(left, right, (((1,), (1,)), ((), ())), preferred_element_type=F32)


def tn(left, right):
    return lax.dot_general(left, right, (((0,), (0,)), ((), ())), preferred_element_type=F32)


def nn(left, right):
    return lax.dot_general(left, right, (((1,), (0,)), ((), ())), preferred_element_type=F32)


def kernel(
    fl, og, fi, mi, ti, sw, fw, mw, tw,
    gf_o, gm_o, gt_o, kg_o, ml_o, tl_o,
    fl_v, g_v, fi_v, mi_v, ti_v, sw_v, fw_v, mw_v, tw_v,
    big, wt, flt, lvl, tmp, fg, gf_v, gath, top, gm_v, gt_v, macc,
    term, crecv, csum, xrecv, zsend, zrecv, yex, kown, kswap, kg_v,
    bterm, bxrecv, bz, bfin, bout,
    in_sem, out_sem, halo_s, halo_r, r_s, r_r, l_s, l_r,
    core_s, core_r, x_s, x_r, z_s, z_r, y_s, y_r, k_s, k_r,
    bx_s, bx_r, bz_s, bz_r, bf_s, bf_r,
    seen_y, seen_z, seen_x, seen_c,
):
    z = lax.axis_index("dp_0")
    x = lax.axis_index("dp_1")
    c = lax.axis_index("dp_2")
    y = lax.axis_index("rows")

    def remote(src, dst, send, recv, **where):
        return pltpu.make_async_remote_copy(
            src_ref=src, dst_ref=dst, send_sem=send, recv_sem=recv,
            device_id=where, device_id_type=MESH,
        )

    loads = [
        pltpu.make_async_copy(og, g_v.at[pl.ds(64, CELLS)], in_sem.at[0]),
        pltpu.make_async_copy(sw, sw_v, in_sem.at[1]),
        pltpu.make_async_copy(fl, fl_v, in_sem.at[2]),
        pltpu.make_async_copy(fi, fi_v, in_sem.at[3]),
        pltpu.make_async_copy(fw, fw_v, in_sem.at[4]),
        pltpu.make_async_copy(mi, mi_v, in_sem.at[5]),
        pltpu.make_async_copy(ti, ti_v, in_sem.at[6]),
        pltpu.make_async_copy(mw, mw_v, in_sem.at[7]),
        pltpu.make_async_copy(tw, tw_v, in_sem.at[8]),
    ]
    for load in loads[:3]:
        load.start()

    barrier = pltpu.get_barrier_semaphore()

    def greet(**where):
        pl.semaphore_signal(barrier, inc=1, device_id=where, device_id_type=MESH)

    down, up = lax.rem(y + 1, NY), lax.rem(y + NY - 1, NY)
    x_next, x_last = lax.rem(x + 1, NX), lax.rem(x + NX - 1, NX)
    z_next, z_last = lax.rem(z + 1, NZ), lax.rem(z + NZ - 1, NZ)
    for where in (
        dict(rows=down), dict(rows=up), dict(dp_1=x_next), dict(dp_1=x_last),
        dict(dp_0=z_next), dict(dp_0=z_last), dict(dp_2=1 - c),
    ):
        greet(**where)

    def tell(r):
        def pair(sem, nexts, lasts):
            pl.semaphore_signal(sem.at[0], inc=1, device_id=nexts, device_id_type=MESH)
            pl.semaphore_signal(sem.at[1], inc=1, device_id=lasts, device_id_type=MESH)

        pair(seen_y, dict(rows=down), dict(rows=up))
        pair(seen_z, dict(dp_0=z_next), dict(dp_0=z_last))
        if r == 1:
            pair(seen_x, dict(dp_1=x_next), dict(dp_1=x_last))
        if r == 2:
            pl.semaphore_signal(seen_c.at[0], inc=1, device_id=dict(dp_2=1 - c), device_id_type=MESH)

    def hear(r):
        for sem in (seen_y, seen_z) + ((seen_x,) if r == 1 else ()):
            pl.semaphore_wait(sem.at[0], 1)
            pl.semaphore_wait(sem.at[1], 1)
        if r == 2:
            pl.semaphore_wait(seen_c.at[0], 1)

    def widen(first, rows):
        value = g_v[pl.ds(first, rows), :].astype(F32)
        column = lax.rem(lax.broadcasted_iota(jnp.int32, (rows, CH), 0), WIDTH)
        after = jnp.where(column == WIDTH - 1, 0.0, pltpu.roll(value, rows - 1, 0))
        before = jnp.where(column == 0, 0.0, pltpu.roll(value, 1, 0))
        big[pl.ds(first, rows), 0:CH] = after.astype(BF16)
        big[pl.ds(first, rows), CH : 2 * CH] = value.astype(BF16)
        big[pl.ds(first, rows), 2 * CH : 3 * CH] = before.astype(BF16)

    loads[0].wait()

    @pl.loop(0, 4)
    def _(t):
        widen(pl.multiple_of(64 + t * 256, 64), 256)

    pl.semaphore_wait(barrier, 7)

    halo_down = remote(
        g_v.at[pl.ds(CELLS, 64)], g_v.at[pl.ds(0, 64)], halo_s.at[0], halo_r.at[0], rows=down
    )
    halo_up = remote(
        g_v.at[pl.ds(64, 64)], g_v.at[pl.ds(CELLS + 64, 64)], halo_s.at[1], halo_r.at[1], rows=up
    )
    halo_down.start()
    halo_up.start()

    tell(1)

    loads[1].wait()

    @pl.loop(0, 9)
    def _(k):
        wt[pl.ds(pl.multiple_of(k * CH, CH), CH), :] = sw_v[k].T

    def hop(h, p, to_down, sent):
        away = h - 1 if sent else h
        origin = lax.rem(y + NY - away, NY) if to_down else lax.rem(y + away, NY)
        first, count = PIECES[p] if isinstance(p, int) else (pl.multiple_of(32 + 64 * p, 32), 64)
        block = gath.at[origin, pl.ds(first, count)]
        send, recv = (r_s, r_r) if to_down else (l_s, l_r)
        return remote(
            block, block, send.at[h - 1, p], recv.at[h - 1, p], rows=down if to_down else up
        )

    def start_own(p):
        hop(1, p, True, True).start()
        hop(1, p, False, True).start()

    def goes(h, p, to_down):
        return h < 4 or p in (LAST_DOWN if to_down else LAST_UP)

    def forward(h, pieces):
        for p in pieces:
            for to_down in (True, False):
                if goes(h, p, to_down):
                    hop(h, p, to_down, False).wait_recv()
                if h < 4 and goes(h + 1, p, to_down):
                    hop(h + 1, p, to_down, True).start()

    def conv(rows):
        total = nn(rows(128), wt[0:768, :])
        total = total + nn(rows(64), wt[768:1536, :])
        return total + nn(rows(0), wt[1536:2304, :])

    def pool(total, put):
        for j in range(2):
            half = total[:, 128 * j : 128 * j + 128]
            for i in range(2):
                lvl[j, 64 * i : 64 * i + 64, :] = (
                    half[128 * i : 128 * i + 64] + half[128 * i + 64 : 128 * i + 128]
                )
            put(
                j,
                (lvl[j, pl.ds(0, 64, stride=2), :] + lvl[j, pl.ds(1, 64, stride=2), :]).astype(BF16),
            )

    def conv_inner(t):
        first = pl.multiple_of(128 + 256 * t, 128)
        out = pl.multiple_of(32 + 64 * t, 32)
        total = conv(lambda shift: big[pl.ds(first + shift, 256), :])
        fg[pl.ds(first, 256), :] = total.astype(BF16)

        def put(j, pooled):
            gath[y, pl.ds(out, 64), 128 * j : 128 * j + 128] = pooled

        pool(total, put)

    def conv_edges():
        low = CELLS - 128
        total = conv(
            lambda shift: jnp.concatenate(
                [big[shift : shift + 128, :], big[low + shift : low + shift + 128, :]]
            )
        )
        fg[0:128, :] = total[0:128].astype(BF16)
        fg[low:CELLS, :] = total[128:256].astype(BF16)

        def put(j, pooled):
            gath[y, 0:32, 128 * j : 128 * j + 128] = pooled[0:32]
            gath[y, 224:256, 128 * j : 128 * j + 128] = pooled[32:64]

        pool(total, put)

    for load in loads[3:]:
        load.start()

    @pl.loop(0, 3)
    def _(t):
        conv_inner(t)
        start_own(t)

    def swap_core(k):
        rows = pl.ds(pl.multiple_of(k * CH, CH), CH)
        return remote(
            term.at[1 - c, rows], crecv.at[rows], core_s.at[k], core_r.at[k], dp_2=1 - c
        )

    def put_term(k, value):
        rows = pl.ds(pl.multiple_of(k * CH, CH), CH)
        value = value.astype(BF16)
        term[0, rows, :] = value[:, 0:128]
        term[1, rows, :] = value[:, 128:256]
        swap_core(k).start()

    def tap(k):
        row = pl.multiple_of((2 - k // 3) * 64, 64)
        col = pl.multiple_of(lax.rem(k, 3) * CH, CH)
        put_term(k, nn(flt[...], big[pl.ds(row, CELLS), pl.ds(col, CH)]))

    loads[2].wait()

    @pl.loop(0, 4)
    def _(t):
        rows = pl.ds(pl.multiple_of(t * 256, 256), 256)
        flt[:, rows] = fl_v[rows, :].T

    @pl.loop(3, 6)
    def _(k):
        tap(k)

    halo_down.wait_recv()
    halo_up.wait_recv()

    @pl.when(y == 0)
    def _():
        g_v[0:64, :] = jnp.zeros((64, CH), BF16)

    @pl.when(y == NY - 1)
    def _():
        g_v[CELLS + 64 : CELLS + 128, :] = jnp.zeros((64, CH), BF16)

    widen(0, 64)
    widen(CELLS + 64, 64)

    conv_edges()
    for p in EDGES:
        start_own(p)

    forward(1, INNER)

    @pl.loop(0, 3)
    def _(k):
        tap(k)

    hear(1)
    tell(2)

    @pl.loop(6, 9)
    def _(k):
        tap(k)

    forward(1, EDGES)

    def coarse(s):
        mid = gath[s]
        cells = pl.ds(pl.multiple_of(s * CH, CH), CH)
        gm_v[cells, :] = nt(mid, mw_v[...]).astype(BF16)
        macc[0:64, :] += tn(mi_v[cells, :], mid)
        wide = mid.astype(F32)
        for j in range(2):
            half = wide[:, 128 * j : 128 * j + 128]
            for i in range(4):
                tmp[j, 32 * i : 32 * i + 32, :] = (
                    half[64 * i : 64 * i + 32] + half[64 * i + 32 : 64 * i + 64]
                )
            top[:, 128 * j : 128 * j + 128] = (
                tmp[j, pl.ds(0, 64, stride=2), :] + tmp[j, pl.ds(1, 64, stride=2), :]
            ).astype(BF16)
        small = top[...]
        cells = pl.ds(pl.multiple_of(s * 64, 64), 64)
        gt_v[cells, :] = nt(small, tw_v[...]).astype(BF16)
        macc[64:192, :] += tn(ti_v[cells, :], small)

    def core_sum(k):
        swap_core(k).wait_recv()
        rows = pl.ds(pl.multiple_of(k * CH, CH), CH)
        csum[rows, :] = (term[c, rows, :].astype(F32) + crecv[rows, :].astype(F32)).astype(BF16)

    def owner(s):
        return 4 * (s // 4) + lax.rem(z + s + 1, 4)

    def x_copy(s, d):
        x_to = lax.rem(x + d, NX)
        rows = pl.ds(pl.multiple_of((owner(s) * NX + x_to) * 80, 80), 80)
        return remote(
            csum.at[rows], xrecv.at[s, d - 1], x_s.at[s, d - 1], x_r.at[s, d - 1], dp_1=x_to
        )

    def x_send(batch):
        @pl.loop(5 * batch, 5 * batch + 5)
        def _(k):
            core_sum(k)

        @pl.loop(4 * batch, 4 * batch + 4)
        def _(s):
            for d in range(1, NX):
                x_copy(s, d).start()

    def z_copy(z_to):
        slot = lax.rem(z_to - z + NZ, NZ) - 1
        return remote(zsend.at[z_to], zrecv.at[slot], z_s.at[slot], z_r.at[slot], dp_0=z_to)

    def x_reduce(batch):
        @pl.loop(4 * batch, 4 * batch + 4)
        def _(s):
            for d in range(1, NX):
                x_copy(s, d).wait_recv()
            z_to = owner(s)
            rows = pl.ds(pl.multiple_of((z_to * NX + x) * 80, 80), 80)
            total = csum[rows, :].astype(F32)
            for d in range(1, NX):
                total = total + xrecv[s, d - 1].astype(F32)
            zsend[z_to] = total.astype(BF16)

            @pl.when(z_to != z)
            def _():
                z_copy(z_to).start()

    def z_arrived(d):
        block = zrecv.at[d - 1]
        return remote(block, block, z_s.at[d - 1], z_r.at[d - 1], dp_0=lax.rem(z + d, NZ))

    x_send(0)

    loads[3].wait()
    put_term(9, tn(fi_v[...], fg[...]))

    forward(2, INNER)

    for load in loads[4:]:
        load.wait()
    macc[...] = jnp.zeros_like(macc)
    coarse(y)
    coarse(lax.rem(y + 1, NY))
    coarse(lax.rem(y + NY - 1, NY))

    x_send(1)

    hear(2)
    tell(3)
    forward(2, EDGES)

    forward(3, INNER)

    coarse(lax.rem(y + 2, NY))
    coarse(lax.rem(y + NY - 2, NY))

    for k in range(4):
        rows = slice(256 * k, 256 * k + 256)
        gf_v[rows, :] = nt(fg[rows, :], fw_v[...]).astype(BF16)
    stores = [pltpu.make_async_copy(gf_v, gf_o, out_sem.at[0])]
    stores[0].start()

    forward(3, EDGES)

    coarse(lax.rem(y + 3, NY))
    coarse(lax.rem(y + NY - 3, NY))

    hear(3)
    x_reduce(0)

    forward(4, INNER + EDGES)

    coarse(lax.rem(y + 4, NY))

    others = [(d, e) for d in range(NX) for e in range(NC) if d or e]
    for i in range(NX):
        for j in range(NC):
            bterm[i, j] = macc[48 * i : 48 * i + 48, 128 * j : 128 * j + 128].astype(BF16)

    def bx_copy(d, e):
        x_to, c_to = lax.rem(x + d, NX), lax.rem(c + e, NC)
        return remote(
            bterm.at[x_to, c_to], bxrecv.at[d, e], bx_s.at[d, e], bx_r.at[d, e],
            dp_1=x_to, dp_2=c_to,
        )

    for d, e in others:
        bx_copy(d, e).start()

    stores.append(pltpu.make_async_copy(gm_v, gm_o, out_sem.at[1]))
    stores.append(pltpu.make_async_copy(gt_v, gt_o, out_sem.at[2]))
    stores[1].start()
    stores[2].start()

    x_reduce(1)

    for d, e in others:
        bx_copy(d, e).wait_recv()
    total = bterm[x, c].astype(F32)
    for d, e in others:
        total = total + bxrecv[d, e].astype(F32)
    bz[z] = total.astype(BF16)

    def bz_copy(d):
        return remote(bz.at[z], bz.at[z], bz_s.at[d - 1], bz_r.at[d - 1], dp_0=lax.rem(z + d, NZ))

    def bz_arrived(d):
        block = bz.at[lax.rem(z + NZ - d, NZ)]
        return remote(block, block, bz_s.at[d - 1], bz_r.at[d - 1], dp_0=lax.rem(z + d, NZ))

    for d in range(1, NZ):
        bz_copy(d).start()

    for d in range(1, NZ):
        z_arrived(d).wait_recv()
    total = zsend[z].astype(F32)
    for i in range(NZ - 1):
        total = total + zrecv[i].astype(F32)
    yex[y] = total.astype(BF16)

    def y_copy(d):
        return remote(
            yex.at[y], yex.at[y], y_s.at[d - 1], y_r.at[d - 1], rows=lax.rem(y + d, NY)
        )

    def y_arrived(d):
        block = yex.at[lax.rem(y + NY - d, NY)]
        return remote(block, block, y_s.at[d - 1], y_r.at[d - 1], rows=lax.rem(y + d, NY))

    for d in range(1, NY):
        y_copy(d).start()

    for d in range(1, NZ):
        bz_arrived(d).wait_recv()
    total = bz[0].astype(F32)
    for i in range(1, NZ):
        total = total + bz[i].astype(F32)
    bfin[x, c] = total.astype(BF16)

    def bf_copy(d, e):
        return remote(
            bfin.at[x, c], bfin.at[x, c], bf_s.at[d, e], bf_r.at[d, e],
            dp_1=lax.rem(x + d, NX), dp_2=lax.rem(c + e, NC),
        )

    def bf_arrived(d, e):
        block = bfin.at[lax.rem(x + NX - d, NX), lax.rem(c + e, NC)]
        return remote(
            block, block, bf_s.at[d, e], bf_r.at[d, e],
            dp_1=lax.rem(x + d, NX), dp_2=lax.rem(c + e, NC),
        )

    for d, e in others:
        bf_copy(d, e).start()

    for d in range(1, NY):
        y_arrived(d).wait_recv()
    total = yex[0].astype(F32)
    for i in range(1, NY):
        total = total + yex[i].astype(F32)
    kown[...] = total
    k_copy = remote(
        kown.at[pl.ds(pl.multiple_of((1 - c) * 40, 8), 40)], kswap, k_s.at[0], k_r.at[0], dp_2=1 - c
    )
    k_copy.start()

    k_copy.wait_recv()
    kg_v[:, pl.ds(pl.multiple_of(c * 128, 128), 128)] = kown[
        pl.ds(pl.multiple_of(c * 40, 8), 40), :
    ]
    kg_v[:, pl.ds(pl.multiple_of((1 - c) * 128, 128), 128)] = kswap[...]
    stores.append(pltpu.make_async_copy(kg_v, kg_o, out_sem.at[3]))
    stores[3].start()

    for d, e in others:
        bf_arrived(d, e).wait_recv()
    for i in range(NX):
        for j in range(NC):
            bout[48 * i : 48 * i + 48, 128 * j : 128 * j + 128] = bfin[i, j].astype(F32)
    stores.append(pltpu.make_async_copy(bout.at[0:64], ml_o, out_sem.at[4]))
    stores.append(pltpu.make_async_copy(bout.at[64:192], tl_o, out_sem.at[5]))
    stores[4].start()
    stores[5].start()

    halo_down.wait_send()
    halo_up.wait_send()
    for h in range(1, 5):
        for p in range(len(PIECES)):
            for to_down in (True, False):
                if goes(h, p, to_down):
                    hop(h, p, to_down, True).wait_send()

    @pl.loop(0, 10)
    def _(k):
        swap_core(k).wait_send()

    @pl.loop(0, NZ)
    def _(s):
        for d in range(1, NX):
            x_copy(s, d).wait_send()

    for d in range(1, NZ):
        z_copy(lax.rem(z + d, NZ)).wait_send()

    for d in range(1, NY):
        y_copy(d).wait_send()
    for d, e in others:
        bx_copy(d, e).wait_send()
    for d in range(1, NZ):
        bz_copy(d).wait_send()
    k_copy.wait_send()
    for d, e in others:
        bf_copy(d, e).wait_send()
    for store in stores:
        store.wait()


def store(*refs):
    copies = [pltpu.make_async_copy(refs[i], refs[6 + i], refs[12].at[i]) for i in range(6)]
    for copy in copies:
        copy.start()
    for copy in copies:
        copy.wait()


def body(
    fine_level, out_grad, fine_input, mid_input, top_input,
    smooth_weight, fine_lateral, mid_lateral, top_lateral,
):
    sem = pltpu.SemaphoreType.DMA
    sizes = [
        ((CELLS, CH), BF16), ((CELLS + 128, CH), BF16), ((CELLS, CH), BF16), ((2048, 64), BF16),
        ((512, 128), BF16), ((9, CH, CH), BF16), ((CH, CH), BF16), ((64, CH), BF16), ((128, CH), BF16),
        ((CELLS + 128, 3 * CH), BF16), ((9 * CH, CH), BF16), ((CH, CELLS), BF16),
        ((2, 128, 128), F32), ((2, 128, 128), F32), ((CELLS, CH), BF16), ((CELLS, CH), BF16),
        ((NY, CH, CH), BF16), ((64, CH), BF16), ((2048, 64), BF16), ((512, 128), BF16), ((192, CH), F32),
        ((2, 2560, 128), BF16), ((2560, 128), BF16), ((2560, 128), BF16), ((NZ, NX - 1, 80, 128), BF16),
        ((NZ, 80, 128), BF16), ((NZ - 1, 80, 128), BF16), ((NY, 80, 128), BF16), ((80, 128), F32),
        ((40, 128), F32), ((40, CH), F32),
        ((NX, NC, 48, 128), BF16), ((NX, NC, 48, 128), BF16),
        ((NZ, 48, 128), BF16), ((NX, NC, 48, 128), BF16), ((192, CH), F32),
    ]
    sems = [
        (9,), (6,), (2,), (2,), (4, 5), (4, 5), (4, 5), (4, 5),
        (10,), (10,), (NZ, NX - 1), (NZ, NX - 1), (NZ - 1,), (NZ - 1,), (NY - 1,), (NY - 1,), (1,), (1,),
        (NX, NC), (NX, NC), (NZ - 1,), (NZ - 1,), (NX, NC), (NX, NC),
    ]
    shapes = [
        ((CELLS, CH), BF16), ((2048, 64), BF16), ((512, 128), BF16),
        ((40, CH), F32), ((64, CH), F32), ((128, CH), F32),
    ]
    hbm = pl.BlockSpec(memory_space=pltpu.HBM)
    anywhere = pl.BlockSpec(memory_space=pl.ANY)
    grads = pl.pallas_call(
        kernel,
        out_shape=[pltpu.VMEM(*shape) for shape in shapes],
        in_specs=[hbm] * 9,
        out_specs=[anywhere] * 6,
        scratch_shapes=[pltpu.VMEM(*size) for size in sizes] + [sem(size) for size in sems]
        + [pltpu.SemaphoreType.REGULAR((count,)) for count in (2, 2, 2, 1)],
        compiler_params=pltpu.CompilerParams(
            collective_id=0, has_side_effects=True, vmem_limit_bytes=48 * 1024 * 1024
        ),
    )(*(pltpu.with_memory_space_constraint(value, pltpu.HBM) for value in (
        fine_level.reshape(CELLS, CH), out_grad.reshape(CELLS, CH), fine_input.reshape(CELLS, CH),
        mid_input.reshape(2048, 64), top_input.reshape(512, 128), smooth_weight.reshape(9, CH, CH),
        fine_lateral, mid_lateral, top_lateral,
    )))
    grads = pl.pallas_call(
        store,
        out_shape=[pltpu.HBM(*shape) for shape in shapes],
        in_specs=[anywhere] * 6,
        out_specs=[hbm] * 6,
        scratch_shapes=[sem((6,))],
    )(*(pltpu.with_memory_space_constraint(grad, pltpu.VMEM) for grad in grads))
    return (
        grads[0].reshape(out_grad.shape), grads[1].reshape(mid_input.shape),
        grads[2].reshape(top_input.shape), grads[3], grads[4], grads[5],
    )


def solution(mesh):
    torus = Mesh(
        mesh.devices.reshape(NZ, NX, NC, NY), ("dp_0", "dp_1", "dp_2", "rows")
    )
    return jax.shard_map(
        body,
        mesh=torus,
        in_specs=(
            P(DP, "rows", None, None), P(DP, "rows", None, None), P(DP, "rows", None, None),
            P(DP, None, None, "rows"), P(DP, None, None, "rows"),
            P(), P(), P("rows", None), P("rows", None),
        ),
        out_specs=(
            P(DP, "rows", None, None), P(DP, None, None, "rows"), P(DP, None, None, "rows"),
            P(DP, None), P("rows", None), P("rows", None),
        ),
        check_vma=False,
    )
```

```python
import jax
import jax.numpy as jnp
from jax import lax
from jax.experimental import pallas as pl
from jax.experimental.pallas import tpu as pltpu
from jax.sharding import Mesh
from jax.sharding import PartitionSpec as P

DP = ("dp_0", "dp_1", "dp_2")
MESH = pl.DeviceIdType.MESH
F32 = jnp.float32
BF16 = jnp.bfloat16
NZ, NX, NC, NY = 8, 4, 2, 8
STRIP, WIDTH, CH = 16, 64, 256
CELLS = STRIP * WIDTH
PIECES = ((32, 64), (96, 64), (160, 64), (0, 32), (224, 32))
INNER, EDGES = (0, 1, 2), (3, 4)
LAST_DOWN, LAST_UP = (0, 1), (2, 3, 4)


def nt(left, right):
    return lax.dot_general(left, right, (((1,), (1,)), ((), ())), preferred_element_type=F32)


def tn(left, right):
    return lax.dot_general(left, right, (((0,), (0,)), ((), ())), preferred_element_type=F32)


def nn(left, right):
    return lax.dot_general(left, right, (((1,), (0,)), ((), ())), preferred_element_type=F32)


def kernel(
    fl, og, fi, mi, ti, sw, fw, mw, tw,
    gf_o, gm_o, gt_o, kg_o, ml_o, tl_o,
    fl_v, g_v, fi_v, mi_v, ti_v, sw_v, fw_v, mw_v, tw_v,
    big, wt, flt, lvl, tmp, fg, gath, top, macc,
    term, crecv, csum, xrecv, zsend, zrecv, yown, yex,
    bterm, bxrecv, bz, bfin,
    in_sem, halo_s, halo_r, ring_s, edge_s, ring_r, last_r,
    core_s, core_r, x_s, x_r, z_s, z_r, y_s, y_r,
    bx_s, bx_r, bz_s, bz_r, bf_s, bf_r,
    seen_y, seen_z, seen_x, seen_c,
):
    z = lax.axis_index("dp_0")
    x = lax.axis_index("dp_1")
    c = lax.axis_index("dp_2")
    y = lax.axis_index("rows")

    def remote(src, dst, send, recv, **where):
        return pltpu.make_async_remote_copy(
            src_ref=src, dst_ref=dst, send_sem=send, recv_sem=recv,
            device_id=where, device_id_type=MESH,
        )

    def wait_bytes(ref, sem):
        remote(ref, ref, sem, sem, dp_2=1 - c).wait_recv()

    loads = [
        pltpu.make_async_copy(og, g_v.at[pl.ds(64, CELLS)], in_sem.at[0]),
        pltpu.make_async_copy(sw, sw_v, in_sem.at[1]),
        pltpu.make_async_copy(fl, fl_v, in_sem.at[2]),
        pltpu.make_async_copy(fi, fi_v, in_sem.at[3]),
        pltpu.make_async_copy(fw, fw_v, in_sem.at[4]),
        pltpu.make_async_copy(mi, mi_v, in_sem.at[5]),
        pltpu.make_async_copy(ti, ti_v, in_sem.at[6]),
        pltpu.make_async_copy(mw, mw_v, in_sem.at[7]),
        pltpu.make_async_copy(tw, tw_v, in_sem.at[8]),
    ]
    for load in loads[:3]:
        load.start()

    barrier = pltpu.get_barrier_semaphore()

    def greet(**where):
        pl.semaphore_signal(barrier, inc=1, device_id=where, device_id_type=MESH)

    down, up = lax.rem(y + 1, NY), lax.rem(y + NY - 1, NY)
    x_next, x_last = lax.rem(x + 1, NX), lax.rem(x + NX - 1, NX)
    z_next, z_last = lax.rem(z + 1, NZ), lax.rem(z + NZ - 1, NZ)
    for where in (
        dict(rows=down), dict(rows=up), dict(dp_1=x_next), dict(dp_1=x_last),
        dict(dp_0=z_next), dict(dp_0=z_last), dict(dp_2=1 - c),
    ):
        greet(**where)

    def tell(sem, *others):
        for i, where in enumerate(others):
            pl.semaphore_signal(sem.at[i], inc=1, device_id=where, device_id_type=MESH)

    def hear(sem, count=2):
        for i in range(count):
            pl.semaphore_wait(sem.at[i], 1)

    def tell_y():
        tell(seen_y, dict(rows=down), dict(rows=up))

    def tell_z():
        tell(seen_z, dict(dp_0=z_next), dict(dp_0=z_last))

    def widen(first, rows):
        value = g_v[pl.ds(first, rows), :].astype(F32)
        column = lax.rem(lax.broadcasted_iota(jnp.int32, (rows, CH), 0), WIDTH)
        after = jnp.where(column == WIDTH - 1, 0.0, pltpu.roll(value, rows - 1, 0))
        before = jnp.where(column == 0, 0.0, pltpu.roll(value, 1, 0))
        big[pl.ds(first, rows), 0:CH] = after.astype(BF16)
        big[pl.ds(first, rows), CH : 2 * CH] = value.astype(BF16)
        big[pl.ds(first, rows), 2 * CH : 3 * CH] = before.astype(BF16)

    loads[0].wait()
    pl.semaphore_wait(barrier, 7)

    halo_down = remote(
        g_v.at[pl.ds(CELLS, 64)], g_v.at[pl.ds(0, 64)], halo_s.at[0], halo_r.at[0], rows=down
    )
    halo_up = remote(
        g_v.at[pl.ds(64, 64)], g_v.at[pl.ds(CELLS + 64, 64)], halo_s.at[0], halo_r.at[0], rows=up
    )
    halo_down.start()
    halo_up.start()


    @pl.loop(0, 4)
    def _(t):
        widen(pl.multiple_of(64 + t * 256, 64), 256)

    tell_y()
    tell_z()
    tell(seen_x, dict(dp_1=x_next), dict(dp_1=x_last))

    loads[1].wait()

    @pl.loop(0, 9)
    def _(k):
        wt[pl.ds(pl.multiple_of(k * CH, CH), CH), :] = sw_v[k].T

    def send_piece(p, away, stride, to_down):
        origin = lax.rem(y + NY - away, NY) if to_down else lax.rem(y + away, NY)
        target = lax.rem(y + stride, NY) if to_down else lax.rem(y + NY - stride, NY)
        first, count = PIECES[p] if isinstance(p, int) else (pl.multiple_of(32 + 64 * p, 32), 64)
        block = gath.at[origin, pl.ds(first, count)]
        h = away + stride
        group = 3 if isinstance(p, int) and p in EDGES else p
        recv = last_r.at[0] if h == 4 else ring_r.at[h - 1, group, 0 if to_down else 1]
        send = edge_s if isinstance(p, int) and p in EDGES else ring_s
        remote(block, block, send.at[0], recv, rows=target).start()

    def came(h, group, to_down):
        wait_bytes(gath.at[0, pl.ds(0, 64)], ring_r.at[h - 1, group, 0 if to_down else 1])

    def start_own(p):
        send_piece(p, 0, 1, True)
        send_piece(p, 0, 1, False)

    def forward(h, p):
        for to_down in (True, False):
            came(h, p, to_down)
            if h < 3 or p in (LAST_DOWN if to_down else LAST_UP):
                send_piece(p, h, 1, to_down)

    def edges_from_home():
        for stride in (1, 2):
            for p in EDGES:
                send_piece(p, 0, stride, True)
                send_piece(p, 0, stride, False)

    def edges_on():
        for to_down in (True, False):
            came(2, 3, to_down)
            for p in EDGES:
                send_piece(p, 2, 1, to_down)
                if p in (LAST_DOWN if to_down else LAST_UP):
                    send_piece(p, 2, 2, to_down)

    def conv(rows):
        total = nn(rows(128), wt[0:768, :])
        total = total + nn(rows(64), wt[768:1536, :])
        return total + nn(rows(0), wt[1536:2304, :])

    def pool(total, put):
        for j in range(2):
            half = total[:, 128 * j : 128 * j + 128]
            for i in range(2):
                lvl[j, 64 * i : 64 * i + 64, :] = (
                    half[128 * i : 128 * i + 64] + half[128 * i + 64 : 128 * i + 128]
                )
            put(
                j,
                (lvl[j, pl.ds(0, 64, stride=2), :] + lvl[j, pl.ds(1, 64, stride=2), :]).astype(BF16),
            )

    def conv_inner(t):
        first = pl.multiple_of(128 + 256 * t, 128)
        out = pl.multiple_of(32 + 64 * t, 32)
        total = conv(lambda shift: big[pl.ds(first + shift, 256), :])
        fg[pl.ds(first, 256), :] = total.astype(BF16)

        def put(j, pooled):
            gath[y, pl.ds(out, 64), 128 * j : 128 * j + 128] = pooled

        pool(total, put)

    def conv_edges():
        low = CELLS - 128
        total = conv(
            lambda shift: jnp.concatenate(
                [big[shift : shift + 128, :], big[low + shift : low + shift + 128, :]]
            )
        )
        fg[0:128, :] = total[0:128].astype(BF16)
        fg[low:CELLS, :] = total[128:256].astype(BF16)

        def put(j, pooled):
            gath[y, 0:32, 128 * j : 128 * j + 128] = pooled[0:32]
            gath[y, 224:256, 128 * j : 128 * j + 128] = pooled[32:64]

        pool(total, put)

    for load in loads[3:]:
        load.start()

    @pl.loop(0, 3)
    def _(t):
        conv_inner(t)
        start_own(t)

    def swap_core(k):
        rows = pl.ds(pl.multiple_of(k * CH, CH), CH)
        return remote(
            term.at[1 - c, rows], crecv.at[rows], core_s.at[0], core_r.at[k // 5], dp_2=1 - c
        )

    def put_term(k, value):
        rows = pl.ds(pl.multiple_of(k * CH, CH), CH)
        value = value.astype(BF16)
        term[0, rows, :] = value[:, 0:128]
        term[1, rows, :] = value[:, 128:256]
        swap_core(k).start()

    def tap(k):
        row = pl.multiple_of((2 - k // 3) * 64, 64)
        col = pl.multiple_of(lax.rem(k, 3) * CH, CH)
        put_term(k, nn(flt[...], big[pl.ds(row, CELLS), pl.ds(col, CH)]))

    loads[2].wait()

    @pl.loop(0, 4)
    def _(t):
        rows = pl.ds(pl.multiple_of(t * 256, 256), 256)
        flt[:, rows] = fl_v[rows, :].T

    @pl.loop(3, 6)
    def _(k):
        tap(k)

    wait_bytes(g_v.at[pl.ds(0, 128)], halo_r.at[0])

    @pl.when(y == 0)
    def _():
        g_v[0:64, :] = jnp.zeros((64, CH), BF16)

    @pl.when(y == NY - 1)
    def _():
        g_v[CELLS + 64 : CELLS + 128, :] = jnp.zeros((64, CH), BF16)

    widen(0, 64)
    widen(CELLS + 64, 64)

    conv_edges()
    hear(seen_y)
    edges_from_home()
    tell_y()

    @pl.loop(0, 3)
    def _(p):
        forward(1, p)
        tap(p)

    @pl.loop(6, 9)
    def _(k):
        tap(k)

    def coarse(s):
        mid = gath[s]
        cells = pl.ds(pl.multiple_of(s * CH, CH), CH)
        gm_o[cells, :] = nt(mid, mw_v[...]).astype(BF16)
        macc[0:64, :] += tn(mi_v[cells, :], mid)
        wide = mid.astype(F32)
        for j in range(2):
            half = wide[:, 128 * j : 128 * j + 128]
            for i in range(4):
                tmp[j, 32 * i : 32 * i + 32, :] = (
                    half[64 * i : 64 * i + 32] + half[64 * i + 32 : 64 * i + 64]
                )
            top[:, 128 * j : 128 * j + 128] = (
                tmp[j, pl.ds(0, 64, stride=2), :] + tmp[j, pl.ds(1, 64, stride=2), :]
            ).astype(BF16)
        small = top[...]
        cells = pl.ds(pl.multiple_of(s * 64, 64), 64)
        gt_o[cells, :] = nt(small, tw_v[...]).astype(BF16)
        macc[64:192, :] += tn(ti_v[cells, :], small)

    def core_sum(k):
        rows = pl.ds(pl.multiple_of(k * CH, CH), CH)
        csum[rows, :] = (term[c, rows, :].astype(F32) + crecv[rows, :].astype(F32)).astype(BF16)

    def owner(s):
        return 4 * (s // 4) + lax.rem(z + s + 1, 4)

    def x_copy(s, d):
        x_to = lax.rem(x + d, NX)
        rows = pl.ds(pl.multiple_of((owner(s) * NX + x_to) * 80, 80), 80)
        return remote(
            csum.at[rows], xrecv.at[s, d - 1], x_s.at[0], x_r.at[s], dp_1=x_to
        )

    def x_send(batch):
        wait_bytes(crecv.at[pl.ds(1280 * batch, 1280)], core_r.at[batch])

        @pl.loop(5 * batch, 5 * batch + 5)
        def _(k):
            core_sum(k)

        @pl.loop(4 * batch, 4 * batch + 4)
        def _(s):
            for d in range(1, NX):
                x_copy(s, d).start()

    def z_copy(z_to):
        slot = lax.rem(z_to - z + NZ, NZ) - 1
        return remote(zsend.at[z_to], zrecv.at[slot], z_s.at[0], z_r.at[0], dp_0=z_to)

    def x_reduce(batch):
        @pl.loop(4 * batch, 4 * batch + 4)
        def _(s):
            wait_bytes(xrecv.at[s], x_r.at[s])
            z_to = owner(s)
            rows = pl.ds(pl.multiple_of((z_to * NX + x) * 80, 80), 80)
            total = csum[rows, :].astype(F32)
            for d in range(1, NX):
                total = total + xrecv[s, d - 1].astype(F32)
            zsend[z_to] = total.astype(BF16)

            @pl.when(z_to != z)
            def _():
                z_copy(z_to).start()

    hear(seen_x)
    forward(2, 0)

    x_send(0)

    loads[3].wait()
    put_term(9, tn(fi_v[...], fg[...]))

    forward(2, 1)
    forward(2, 2)

    for load in loads[4:]:
        load.wait()
    macc[...] = jnp.zeros_like(macc)
    coarse(y)

    x_send(1)

    hear(seen_y)
    edges_on()
    tell_y()
    hear(seen_z)
    tell_z()

    came(1, 3, True)
    came(1, 3, False)
    coarse(lax.rem(y + 1, NY))
    coarse(lax.rem(y + NY - 1, NY))

    forward(3, 0)
    forward(3, 1)
    forward(3, 2)

    coarse(lax.rem(y + 2, NY))
    coarse(lax.rem(y + NY - 2, NY))

    for k in range(4):
        rows = slice(256 * k, 256 * k + 256)
        gf_o[rows, :] = nt(fg[rows, :], fw_v[...]).astype(BF16)

    hear(seen_y)
    hear(seen_z)
    tell_z()
    tell(seen_c, dict(dp_2=1 - c))

    came(3, 3, True)
    came(3, 3, False)

    coarse(lax.rem(y + 3, NY))
    coarse(lax.rem(y + NY - 3, NY))

    hear(seen_z)

    x_reduce(0)

    wait_bytes(gath.at[0], last_r.at[0])

    coarse(lax.rem(y + 4, NY))
    hear(seen_c, 1)

    others = [(d, e) for d in range(NX) for e in range(NC) if d or e]
    for i in range(NX):
        for j in range(NC):
            bterm[NC * i + j] = macc[48 * i : 48 * i + 48, 128 * j : 128 * j + 128].astype(BF16)

    def bx_copy(d, e):
        x_to, c_to = lax.rem(x + d, NX), lax.rem(c + e, NC)
        return remote(
            bterm.at[NC * x_to + c_to], bxrecv.at[NC * d + e - 1], bx_s.at[0], bx_r.at[0],
            dp_1=x_to, dp_2=c_to,
        )

    for d, e in others:
        bx_copy(d, e).start()

    x_reduce(1)

    wait_bytes(bxrecv, bx_r.at[0])
    total = bterm[NC * x + c].astype(F32)
    for i in range(NX * NC - 1):
        total = total + bxrecv[i].astype(F32)
    bz[z] = total.astype(BF16)

    def bz_copy(d):
        return remote(bz.at[z], bz.at[z], bz_s.at[0], bz_r.at[0], dp_0=lax.rem(z + d, NZ))

    for d in range(1, NZ):
        bz_copy(d).start()

    wait_bytes(zrecv, z_r.at[0])
    total = zsend[z].astype(F32)
    for i in range(NZ - 1):
        total = total + zrecv[i].astype(F32)
    for i in range(NC):
        yown[i] = total[40 * i : 40 * i + 40].astype(BF16)
    yex[NY * c + y] = yown[c]

    def y_copy(d, e):
        c_to = lax.rem(c + e, NC)
        return remote(
            yown.at[c_to], yex.at[NY * c + y], y_s.at[0], y_r.at[0],
            rows=lax.rem(y + d, NY), dp_2=c_to,
        )

    for d in range(NY):
        for e in range(NC):
            if d or e:
                y_copy(d, e).start()

    wait_bytes(bz.at[pl.ds(0, NZ - 1)], bz_r.at[0])
    total = bz[0].astype(F32)
    for i in range(1, NZ):
        total = total + bz[i].astype(F32)
    bfin[NC * x + c] = total.astype(BF16)

    def bf_copy(d, e):
        return remote(
            bfin.at[NC * x + c], bfin.at[NC * x + c], bf_s.at[0], bf_r.at[0],
            dp_1=lax.rem(x + d, NX), dp_2=lax.rem(c + e, NC),
        )

    for d, e in others:
        bf_copy(d, e).start()

    wait_bytes(yex.at[pl.ds(0, NC * NY - 1)], y_r.at[0])
    for i in range(NC):
        total = yex[NY * i].astype(F32)
        for j in range(1, NY):
            total = total + yex[NY * i + j].astype(F32)
        kg_o[:, 128 * i : 128 * i + 128] = total

    for ref, sem in (
        (g_v.at[pl.ds(0, 128)], halo_s), (gath.at[pl.ds(0, 7), pl.ds(0, 192)], ring_s),
        (gath.at[pl.ds(0, 7), pl.ds(0, 64)], edge_s), (crecv, core_s),
        (csum.at[pl.ds(0, NZ * (NX - 1) * 80)], x_s), (zrecv, z_s), (yex.at[pl.ds(0, NC * NY - 1)], y_s),
        (bxrecv, bx_s), (bz.at[pl.ds(0, NZ - 1)], bz_s),
    ):
        wait_bytes(ref, sem.at[0])

    wait_bytes(bfin.at[pl.ds(0, NX * NC - 1)], bf_r.at[0])
    for i in range(NX):
        for j in range(NC):
            block = bfin[NC * i + j].astype(F32)
            cols = slice(128 * j, 128 * j + 128)
            if i == 0:
                ml_o[0:48, cols] = block
            elif i == 1:
                ml_o[48:64, cols] = block[0:16]
                tl_o[0:32, cols] = block[16:48]
            else:
                tl_o[48 * i - 64 : 48 * i - 16, cols] = block
    wait_bytes(bfin.at[pl.ds(0, NX * NC - 1)], bf_s.at[0])


def store(*refs):
    copies = [pltpu.make_async_copy(refs[i], refs[6 + i], refs[12].at[i]) for i in range(6)]
    for copy in copies:
        copy.start()
    for copy in copies:
        copy.wait()


def body(
    fine_level, out_grad, fine_input, mid_input, top_input,
    smooth_weight, fine_lateral, mid_lateral, top_lateral,
):
    sem = pltpu.SemaphoreType.DMA
    sizes = [
        ((CELLS, CH), BF16), ((CELLS + 128, CH), BF16), ((CELLS, CH), BF16), ((2048, 64), BF16),
        ((512, 128), BF16), ((9, CH, CH), BF16), ((CH, CH), BF16), ((64, CH), BF16), ((128, CH), BF16),
        ((CELLS + 128, 3 * CH), BF16), ((9 * CH, CH), BF16), ((CH, CELLS), BF16),
        ((2, 128, 128), F32), ((2, 128, 128), F32), ((CELLS, CH), BF16),
        ((NY, CH, CH), BF16), ((64, CH), BF16), ((192, CH), F32),
        ((2, 2560, 128), BF16), ((2560, 128), BF16), ((2560, 128), BF16), ((NZ, NX - 1, 80, 128), BF16),
        ((NZ, 80, 128), BF16), ((NZ - 1, 80, 128), BF16), ((NC, 40, 128), BF16), ((NC * NY, 40, 128), BF16),
        ((NX * NC, 48, 128), BF16), ((NX * NC - 1, 48, 128), BF16),
        ((NZ, 48, 128), BF16), ((NX * NC, 48, 128), BF16),
    ]
    sems = [
        (9,), (1,), (1,), (1,), (1,), (3, 4, 2), (1,),
        (1,), (2,), (1,), (NZ,), (1,), (1,), (1,), (1,),
        (1,), (1,), (1,), (1,), (1,), (1,),
    ]
    shapes = [
        ((CELLS, CH), BF16), ((2048, 64), BF16), ((512, 128), BF16),
        ((40, CH), F32), ((64, CH), F32), ((128, CH), F32),
    ]
    hbm = pl.BlockSpec(memory_space=pltpu.HBM)
    anywhere = pl.BlockSpec(memory_space=pl.ANY)
    grads = pl.pallas_call(
        kernel,
        out_shape=[pltpu.VMEM(*shape) for shape in shapes],
        in_specs=[hbm] * 9,
        out_specs=[pl.BlockSpec(memory_space=pltpu.VMEM)] * 6,
        scratch_shapes=[pltpu.VMEM(*size) for size in sizes] + [sem(size) for size in sems]
        + [pltpu.SemaphoreType.REGULAR((count,)) for count in (2, 2, 2, 1)],
        compiler_params=pltpu.CompilerParams(
            collective_id=0, has_side_effects=True, vmem_limit_bytes=48 * 1024 * 1024
        ),
    )(*(pltpu.with_memory_space_constraint(value, pltpu.HBM) for value in (
        fine_level.reshape(CELLS, CH), out_grad.reshape(CELLS, CH), fine_input.reshape(CELLS, CH),
        mid_input.reshape(2048, 64), top_input.reshape(512, 128), smooth_weight.reshape(9, CH, CH),
        fine_lateral, mid_lateral, top_lateral,
    )))
    grads = pl.pallas_call(
        store,
        out_shape=[pltpu.HBM(*shape) for shape in shapes],
        in_specs=[anywhere] * 6,
        out_specs=[hbm] * 6,
        scratch_shapes=[sem((6,))],
    )(*(pltpu.with_memory_space_constraint(grad, pltpu.VMEM) for grad in grads))
    return (
        grads[0].reshape(out_grad.shape), grads[1].reshape(mid_input.shape),
        grads[2].reshape(top_input.shape), grads[3], grads[4], grads[5],
    )


def solution(mesh):
    torus = Mesh(
        mesh.devices.reshape(NZ, NX, NC, NY), ("dp_0", "dp_1", "dp_2", "rows")
    )
    return jax.shard_map(
        body,
        mesh=torus,
        in_specs=(
            P(DP, "rows", None, None), P(DP, "rows", None, None), P(DP, "rows", None, None),
            P(DP, None, None, "rows"), P(DP, None, None, "rows"),
            P(), P(), P("rows", None), P("rows", None),
        ),
        out_specs=(
            P(DP, "rows", None, None), P(DP, None, None, "rows"), P(DP, None, None, "rows"),
            P(DP, None), P("rows", None), P("rows", None),
        ),
        check_vma=False,
    )
```

```python
import jax
import jax.numpy as jnp
from jax import lax
from jax.experimental import pallas as pl
from jax.experimental.pallas import tpu as pltpu
from jax.sharding import Mesh
from jax.sharding import PartitionSpec as P

DP = ("dp_0", "dp_1", "dp_2")
MESH = pl.DeviceIdType.MESH
F32 = jnp.float32
BF16 = jnp.bfloat16
NZ, NX, NC, NY = 8, 4, 2, 8
STRIP, WIDTH, CH = 16, 64, 256
CELLS = STRIP * WIDTH
PIECES = ((32, 64), (96, 64), (160, 64), (0, 32), (224, 32))
INNER, EDGES = (0, 1, 2), (3, 4)
LAST_DOWN, LAST_UP = (0, 2), (1, 3, 4)


def nt(left, right):
    return lax.dot_general(left, right, (((1,), (1,)), ((), ())), preferred_element_type=F32)


def tn(left, right):
    return lax.dot_general(left, right, (((0,), (0,)), ((), ())), preferred_element_type=F32)


def nn(left, right):
    return lax.dot_general(left, right, (((1,), (0,)), ((), ())), preferred_element_type=F32)


def kernel(
    fl, og, fi, mi, ti, sw, fw, mw, tw,
    gf_o, gm_o, gt_o, kg_o, ml_o, tl_o,
    fl_v, g_v, fi_v, mi_v, ti_v, sw_v, fw_v, mw_v, tw_v,
    big, flt, lvl, tmp, fg, gath, top, macc,
    term, crecv, csum, xrecv, zsend, zrecv, yown, yex,
    bterm, bxrecv, bz, bfin,
    in_sem, halo_s, halo_r, ring_s, edge_s, ring_r, last_r,
    core_s, core_r, x_s, x_r, z_s, z_r, y_s, y_r,
    bx_s, bx_r, bz_s, bz_r, bf_s, bf_r,
    seen_y, seen_z, seen_x, seen_c,
):
    z = lax.axis_index("dp_0")
    x = lax.axis_index("dp_1")
    c = lax.axis_index("dp_2")
    y = lax.axis_index("rows")

    def remote(src, dst, send, recv, **where):
        return pltpu.make_async_remote_copy(
            src_ref=src, dst_ref=dst, send_sem=send, recv_sem=recv,
            device_id=where, device_id_type=MESH,
        )

    def wait_bytes(ref, sem):
        remote(ref, ref, sem, sem, dp_2=1 - c).wait_recv()

    loads = [
        pltpu.make_async_copy(og, g_v.at[pl.ds(64, CELLS)], in_sem.at[0]),
        pltpu.make_async_copy(sw, sw_v, in_sem.at[1]),
        pltpu.make_async_copy(fl, fl_v, in_sem.at[2]),
        pltpu.make_async_copy(fi, fi_v, in_sem.at[3]),
        pltpu.make_async_copy(fw, fw_v, in_sem.at[4]),
        pltpu.make_async_copy(mi, mi_v, in_sem.at[5]),
        pltpu.make_async_copy(ti, ti_v, in_sem.at[6]),
        pltpu.make_async_copy(mw, mw_v, in_sem.at[7]),
        pltpu.make_async_copy(tw, tw_v, in_sem.at[8]),
    ]
    for load in loads[:3]:
        load.start()

    barrier = pltpu.get_barrier_semaphore()

    def greet(**where):
        pl.semaphore_signal(barrier, inc=1, device_id=where, device_id_type=MESH)

    down, up = lax.rem(y + 1, NY), lax.rem(y + NY - 1, NY)
    x_next, x_last = lax.rem(x + 1, NX), lax.rem(x + NX - 1, NX)
    z_next, z_last = lax.rem(z + 1, NZ), lax.rem(z + NZ - 1, NZ)
    for where in (
        dict(rows=down), dict(rows=up), dict(dp_1=x_next), dict(dp_1=x_last),
        dict(dp_0=z_next), dict(dp_0=z_last), dict(dp_2=1 - c),
    ):
        greet(**where)

    def tell(sem, *others):
        for i, where in enumerate(others):
            pl.semaphore_signal(sem.at[i], inc=1, device_id=where, device_id_type=MESH)

    def hear(sem, count=2):
        for i in range(count):
            pl.semaphore_wait(sem.at[i], 1)

    def tell_y():
        tell(seen_y, dict(rows=down), dict(rows=up))

    def tell_z():
        tell(seen_z, dict(dp_0=z_next), dict(dp_0=z_last))

    def widen(first, rows):
        value = g_v[pl.ds(first, rows), :].astype(F32)
        column = lax.rem(lax.broadcasted_iota(jnp.int32, (rows, CH), 0), WIDTH)
        after = jnp.where(column == WIDTH - 1, 0.0, pltpu.roll(value, rows - 1, 0))
        before = jnp.where(column == 0, 0.0, pltpu.roll(value, 1, 0))
        big[pl.ds(first, rows), 0:CH] = after.astype(BF16)
        big[pl.ds(first, rows), CH : 2 * CH] = value.astype(BF16)
        big[pl.ds(first, rows), 2 * CH : 3 * CH] = before.astype(BF16)

    loads[0].wait()

    @pl.loop(0, 4)
    def _(t):
        widen(pl.multiple_of(64 + t * 256, 64), 256)

    def send_piece(p, away, stride, to_down):
        origin = lax.rem(y + NY - away, NY) if to_down else lax.rem(y + away, NY)
        target = lax.rem(y + stride, NY) if to_down else lax.rem(y + NY - stride, NY)
        first, count = PIECES[p] if isinstance(p, int) else (pl.multiple_of(32 + 64 * p, 32), 64)
        block = gath.at[origin, pl.ds(first, count)]
        h = away + stride
        group = 3 if isinstance(p, int) and p in EDGES else p
        recv = last_r.at[0] if h == 4 else ring_r.at[h - 1, group, 0 if to_down else 1]
        send = edge_s if isinstance(p, int) and p in EDGES else ring_s
        remote(block, block, send.at[0], recv, rows=target).start()

    def came(h, group, to_down):
        wait_bytes(gath.at[0, pl.ds(0, 64)], ring_r.at[h - 1, group, 0 if to_down else 1])

    def start_own(p):
        send_piece(p, 0, 1, True)
        send_piece(p, 0, 1, False)

    def forward(h, p):
        for to_down in (True, False):
            came(h, p, to_down)
            if h < 3 or p in (LAST_DOWN if to_down else LAST_UP):
                send_piece(p, h, 1, to_down)

    def edges_from_home():
        for stride in (1, 2):
            for p in EDGES:
                send_piece(p, 0, stride, True)
                send_piece(p, 0, stride, False)

    def edges_on():
        for to_down in (True, False):
            came(2, 3, to_down)
            for p in EDGES:
                send_piece(p, 2, 1, to_down)
                if p in (LAST_DOWN if to_down else LAST_UP):
                    send_piece(p, 2, 2, to_down)

    def conv(rows):
        total = None
        for a in range(3):
            value = rows(64 * (2 - a))
            for b in range(3):
                term_ab = nt(value[:, CH * b : CH * b + CH], sw_v[3 * a + b])
                total = term_ab if total is None else total + term_ab
        return total

    def pool(total, put):
        for j in range(2):
            half = total[:, 128 * j : 128 * j + 128]
            for i in range(2):
                lvl[j, 64 * i : 64 * i + 64, :] = (
                    half[128 * i : 128 * i + 64] + half[128 * i + 64 : 128 * i + 128]
                )
            put(
                j,
                (lvl[j, pl.ds(0, 64, stride=2), :] + lvl[j, pl.ds(1, 64, stride=2), :]).astype(BF16),
            )

    def conv_inner(t):
        first = pl.multiple_of(128 + 256 * t, 128)
        out = pl.multiple_of(32 + 64 * t, 32)
        total = conv(lambda shift: big[pl.ds(first + shift, 256), :])
        fg[pl.ds(first, 256), :] = total.astype(BF16)

        def put(j, pooled):
            gath[y, pl.ds(out, 64), 128 * j : 128 * j + 128] = pooled

        pool(total, put)

    def conv_edges():
        low = CELLS - 128
        total = conv(
            lambda shift: jnp.concatenate(
                [big[shift : shift + 128, :], big[low + shift : low + shift + 128, :]]
            )
        )
        fg[0:128, :] = total[0:128].astype(BF16)
        fg[low:CELLS, :] = total[128:256].astype(BF16)

        def put(j, pooled):
            gath[y, 0:32, 128 * j : 128 * j + 128] = pooled[0:32]
            gath[y, 224:256, 128 * j : 128 * j + 128] = pooled[32:64]

        pool(total, put)

    for load in loads[3:]:
        load.start()

    loads[1].wait()
    conv_inner(0)

    pl.semaphore_wait(barrier, 7)

    halo_down = remote(
        g_v.at[pl.ds(CELLS, 64)], g_v.at[pl.ds(0, 64)], halo_s.at[0], halo_r.at[0], rows=down
    )
    halo_up = remote(
        g_v.at[pl.ds(64, 64)], g_v.at[pl.ds(CELLS + 64, 64)], halo_s.at[0], halo_r.at[0], rows=up
    )
    halo_down.start()
    halo_up.start()

    tell_y()
    tell_z()
    tell(seen_x, dict(dp_1=x_next), dict(dp_1=x_last))

    start_own(0)

    @pl.loop(1, 3)
    def _(t):
        conv_inner(t)
        start_own(t)

    def swap_core(k):
        rows = pl.ds(pl.multiple_of(k * CH, CH), CH)
        return remote(
            term.at[1 - c, rows], crecv.at[rows], core_s.at[0], core_r.at[k // 5], dp_2=1 - c
        )

    def put_term(k, value):
        rows = pl.ds(pl.multiple_of(k * CH, CH), CH)
        value = value.astype(BF16)
        term[0, rows, :] = value[:, 0:128]
        term[1, rows, :] = value[:, 128:256]
        swap_core(k).start()

    def tap(k):
        row = pl.multiple_of((2 - k // 3) * 64, 64)
        col = pl.multiple_of(lax.rem(k, 3) * CH, CH)
        put_term(k, nn(flt[...], big[pl.ds(row, CELLS), pl.ds(col, CH)]))

    loads[2].wait()

    @pl.loop(0, 4)
    def _(t):
        rows = pl.ds(pl.multiple_of(t * 256, 256), 256)
        flt[:, rows] = fl_v[rows, :].T

    @pl.loop(3, 6)
    def _(k):
        tap(k)

    wait_bytes(g_v.at[pl.ds(0, 128)], halo_r.at[0])

    @pl.when(y == 0)
    def _():
        g_v[0:64, :] = jnp.zeros((64, CH), BF16)

    @pl.when(y == NY - 1)
    def _():
        g_v[CELLS + 64 : CELLS + 128, :] = jnp.zeros((64, CH), BF16)

    widen(0, 64)
    widen(CELLS + 64, 64)

    conv_edges()
    hear(seen_y)
    edges_from_home()
    tell_y()

    @pl.loop(0, 3)
    def _(p):
        forward(1, p)
        tap(p)

    @pl.loop(6, 9)
    def _(k):
        tap(k)

    def coarse(s):
        mid = gath[s]
        cells = pl.ds(pl.multiple_of(s * CH, CH), CH)
        gm_o[cells, :] = nt(mid, mw_v[...]).astype(BF16)
        macc[0:64, :] += tn(mi_v[cells, :], mid)
        wide = mid.astype(F32)
        for j in range(2):
            half = wide[:, 128 * j : 128 * j + 128]
            for i in range(4):
                tmp[j, 32 * i : 32 * i + 32, :] = (
                    half[64 * i : 64 * i + 32] + half[64 * i + 32 : 64 * i + 64]
                )
            top[:, 128 * j : 128 * j + 128] = (
                tmp[j, pl.ds(0, 64, stride=2), :] + tmp[j, pl.ds(1, 64, stride=2), :]
            ).astype(BF16)
        small = top[...]
        cells = pl.ds(pl.multiple_of(s * 64, 64), 64)
        gt_o[cells, :] = nt(small, tw_v[...]).astype(BF16)
        macc[64:192, :] += tn(ti_v[cells, :], small)

    def core_sum(k):
        rows = pl.ds(pl.multiple_of(k * CH, CH), CH)
        csum[rows, :] = (term[c, rows, :].astype(F32) + crecv[rows, :].astype(F32)).astype(BF16)

    def owner(s):
        return 4 * (s // 4) + lax.rem(z + s + 1, 4)

    def x_copy(s, d):
        x_to = lax.rem(x + d, NX)
        rows = pl.ds(pl.multiple_of((owner(s) * NX + x_to) * 80, 80), 80)
        return remote(
            csum.at[rows], xrecv.at[s, d - 1], x_s.at[0], x_r.at[s], dp_1=x_to
        )

    def x_send(batch):
        wait_bytes(crecv.at[pl.ds(1280 * batch, 1280)], core_r.at[batch])

        @pl.loop(5 * batch, 5 * batch + 5)
        def _(k):
            core_sum(k)

        @pl.loop(4 * batch, 4 * batch + 4)
        def _(s):
            for d in range(1, NX):
                x_copy(s, d).start()

    def z_copy(z_to):
        slot = lax.rem(z_to - z + NZ, NZ) - 1
        return remote(zsend.at[z_to], zrecv.at[slot], z_s.at[0], z_r.at[0], dp_0=z_to)

    def x_reduce(batch):
        @pl.loop(4 * batch, 4 * batch + 4)
        def _(s):
            wait_bytes(xrecv.at[s], x_r.at[s])
            z_to = owner(s)
            rows = pl.ds(pl.multiple_of((z_to * NX + x) * 80, 80), 80)
            total = csum[rows, :].astype(F32)
            for d in range(1, NX):
                total = total + xrecv[s, d - 1].astype(F32)
            zsend[z_to] = total.astype(BF16)

            @pl.when(z_to != z)
            def _():
                z_copy(z_to).start()

    hear(seen_x)
    hear(seen_z)
    tell_z()
    x_send(0)

    loads[3].wait()
    put_term(9, tn(fi_v[...], fg[...]))

    forward(2, 0)

    forward(2, 1)
    forward(2, 2)

    for load in loads[4:]:
        load.wait()
    macc[...] = jnp.zeros_like(macc)
    coarse(y)

    hear(seen_z)
    tell_z()

    x_send(1)

    hear(seen_y)
    edges_on()
    tell_y()

    came(1, 3, True)
    came(1, 3, False)
    coarse(lax.rem(y + 1, NY))
    coarse(lax.rem(y + NY - 1, NY))

    forward(3, 0)
    forward(3, 1)
    forward(3, 2)

    coarse(lax.rem(y + 2, NY))
    coarse(lax.rem(y + NY - 2, NY))

    for k in range(4):
        rows = slice(256 * k, 256 * k + 256)
        gf_o[rows, :] = nt(fg[rows, :], fw_v[...]).astype(BF16)

    hear(seen_y)
    tell(seen_c, dict(dp_2=1 - c))

    came(3, 3, True)
    came(3, 3, False)

    coarse(lax.rem(y + 3, NY))
    coarse(lax.rem(y + NY - 3, NY))

    hear(seen_z)

    x_reduce(0)

    wait_bytes(gath.at[0], last_r.at[0])

    coarse(lax.rem(y + 4, NY))
    hear(seen_c, 1)

    others = [(d, e) for d in range(NX) for e in range(NC) if d or e]
    for i in range(NX):
        for j in range(NC):
            bterm[NC * i + j] = macc[48 * i : 48 * i + 48, 128 * j : 128 * j + 128].astype(BF16)

    def bx_copy(d, e):
        x_to, c_to = lax.rem(x + d, NX), lax.rem(c + e, NC)
        return remote(
            bterm.at[NC * x_to + c_to], bxrecv.at[NC * d + e - 1], bx_s.at[0], bx_r.at[0],
            dp_1=x_to, dp_2=c_to,
        )

    for d, e in others:
        bx_copy(d, e).start()

    x_reduce(1)

    wait_bytes(bxrecv, bx_r.at[0])
    total = bterm[NC * x + c].astype(F32)
    for i in range(NX * NC - 1):
        total = total + bxrecv[i].astype(F32)
    bz[z] = total.astype(BF16)

    def bz_copy(d):
        return remote(bz.at[z], bz.at[z], bz_s.at[0], bz_r.at[0], dp_0=lax.rem(z + d, NZ))

    for d in range(1, NZ):
        bz_copy(d).start()

    wait_bytes(zrecv, z_r.at[0])
    total = zsend[z].astype(F32)
    for i in range(NZ - 1):
        total = total + zrecv[i].astype(F32)
    for i in range(NC):
        yown[i] = total[40 * i : 40 * i + 40].astype(BF16)
    yex[NY * c + y] = yown[c]

    def y_copy(d, e):
        c_to = lax.rem(c + e, NC)
        return remote(
            yown.at[c_to], yex.at[NY * c + y], y_s.at[0], y_r.at[0],
            rows=lax.rem(y + d, NY), dp_2=c_to,
        )

    for d in range(NY):
        for e in range(NC):
            if d or e:
                y_copy(d, e).start()

    wait_bytes(bz.at[pl.ds(0, NZ - 1)], bz_r.at[0])
    total = bz[0].astype(F32)
    for i in range(1, NZ):
        total = total + bz[i].astype(F32)
    bfin[NC * x + c] = total.astype(BF16)

    def bf_copy(d, e):
        return remote(
            bfin.at[NC * x + c], bfin.at[NC * x + c], bf_s.at[0], bf_r.at[0],
            dp_1=lax.rem(x + d, NX), dp_2=lax.rem(c + e, NC),
        )

    for d, e in others:
        bf_copy(d, e).start()

    wait_bytes(yex.at[pl.ds(0, NC * NY - 1)], y_r.at[0])
    for i in range(NC):
        total = yex[NY * i].astype(F32)
        for j in range(1, NY):
            total = total + yex[NY * i + j].astype(F32)
        kg_o[:, 128 * i : 128 * i + 128] = total

    for ref, sem in (
        (g_v.at[pl.ds(0, 128)], halo_s), (gath.at[pl.ds(0, 7), pl.ds(0, 192)], ring_s),
        (gath.at[pl.ds(0, 7), pl.ds(0, 64)], edge_s), (crecv, core_s),
        (csum.at[pl.ds(0, NZ * (NX - 1) * 80)], x_s), (zrecv, z_s), (yex.at[pl.ds(0, NC * NY - 1)], y_s),
        (bxrecv, bx_s), (bz.at[pl.ds(0, NZ - 1)], bz_s),
    ):
        wait_bytes(ref, sem.at[0])

    wait_bytes(bfin.at[pl.ds(0, NX * NC - 1)], bf_r.at[0])
    for i in range(NX):
        for j in range(NC):
            block = bfin[NC * i + j].astype(F32)
            cols = slice(128 * j, 128 * j + 128)
            if i == 0:
                ml_o[0:48, cols] = block
            elif i == 1:
                ml_o[48:64, cols] = block[0:16]
                tl_o[0:32, cols] = block[16:48]
            else:
                tl_o[48 * i - 64 : 48 * i - 16, cols] = block
    wait_bytes(bfin.at[pl.ds(0, NX * NC - 1)], bf_s.at[0])


def store(*refs):
    copies = [pltpu.make_async_copy(refs[i], refs[6 + i], refs[12].at[i]) for i in range(6)]
    for copy in copies:
        copy.start()
    for copy in copies:
        copy.wait()


def body(
    fine_level, out_grad, fine_input, mid_input, top_input,
    smooth_weight, fine_lateral, mid_lateral, top_lateral,
):
    sem = pltpu.SemaphoreType.DMA
    sizes = [
        ((CELLS, CH), BF16), ((CELLS + 128, CH), BF16), ((CELLS, CH), BF16), ((2048, 64), BF16),
        ((512, 128), BF16), ((9, CH, CH), BF16), ((CH, CH), BF16), ((64, CH), BF16), ((128, CH), BF16),
        ((CELLS + 128, 3 * CH), BF16), ((CH, CELLS), BF16),
        ((2, 128, 128), F32), ((2, 128, 128), F32), ((CELLS, CH), BF16),
        ((NY, CH, CH), BF16), ((64, CH), BF16), ((192, CH), F32),
        ((2, 2560, 128), BF16), ((2560, 128), BF16), ((2560, 128), BF16), ((NZ, NX - 1, 80, 128), BF16),
        ((NZ, 80, 128), BF16), ((NZ - 1, 80, 128), BF16), ((NC, 40, 128), BF16), ((NC * NY, 40, 128), BF16),
        ((NX * NC, 48, 128), BF16), ((NX * NC - 1, 48, 128), BF16),
        ((NZ, 48, 128), BF16), ((NX * NC, 48, 128), BF16),
    ]
    sems = [
        (9,), (1,), (1,), (1,), (1,), (3, 4, 2), (1,),
        (1,), (2,), (1,), (NZ,), (1,), (1,), (1,), (1,),
        (1,), (1,), (1,), (1,), (1,), (1,),
    ]
    shapes = [
        ((CELLS, CH), BF16), ((2048, 64), BF16), ((512, 128), BF16),
        ((40, CH), F32), ((64, CH), F32), ((128, CH), F32),
    ]
    hbm = pl.BlockSpec(memory_space=pltpu.HBM)
    anywhere = pl.BlockSpec(memory_space=pl.ANY)
    grads = pl.pallas_call(
        kernel,
        out_shape=[pltpu.VMEM(*shape) for shape in shapes],
        in_specs=[hbm] * 9,
        out_specs=[pl.BlockSpec(memory_space=pltpu.VMEM)] * 6,
        scratch_shapes=[pltpu.VMEM(*size) for size in sizes] + [sem(size) for size in sems]
        + [pltpu.SemaphoreType.REGULAR((count,)) for count in (2, 2, 2, 1)],
        compiler_params=pltpu.CompilerParams(
            collective_id=0, has_side_effects=True, vmem_limit_bytes=48 * 1024 * 1024
        ),
    )(*(pltpu.with_memory_space_constraint(value, pltpu.HBM) for value in (
        fine_level.reshape(CELLS, CH), out_grad.reshape(CELLS, CH), fine_input.reshape(CELLS, CH),
        mid_input.reshape(2048, 64), top_input.reshape(512, 128), smooth_weight.reshape(9, CH, CH),
        fine_lateral, mid_lateral, top_lateral,
    )))
    grads = pl.pallas_call(
        store,
        out_shape=[pltpu.HBM(*shape) for shape in shapes],
        in_specs=[anywhere] * 6,
        out_specs=[hbm] * 6,
        scratch_shapes=[sem((6,))],
    )(*(pltpu.with_memory_space_constraint(grad, pltpu.VMEM) for grad in grads))
    return (
        grads[0].reshape(out_grad.shape), grads[1].reshape(mid_input.shape),
        grads[2].reshape(top_input.shape), grads[3], grads[4], grads[5],
    )


def solution(mesh):
    torus = Mesh(
        mesh.devices.reshape(NZ, NX, NC, NY), ("dp_0", "dp_1", "dp_2", "rows")
    )
    return jax.shard_map(
        body,
        mesh=torus,
        in_specs=(
            P(DP, "rows", None, None), P(DP, "rows", None, None), P(DP, "rows", None, None),
            P(DP, None, None, "rows"), P(DP, None, None, "rows"),
            P(), P(), P("rows", None), P("rows", None),
        ),
        out_specs=(
            P(DP, "rows", None, None), P(DP, None, None, "rows"), P(DP, None, None, "rows"),
            P(DP, None), P("rows", None), P("rows", None),
        ),
        check_vma=False,
    )
```

```python
import jax
import jax.numpy as jnp
from jax import lax
from jax.experimental import pallas as pl
from jax.experimental.pallas import tpu as pltpu
from jax.sharding import Mesh
from jax.sharding import PartitionSpec as P

DP = ("dp_0", "dp_1", "dp_2")
MESH = pl.DeviceIdType.MESH
F32 = jnp.float32
BF16 = jnp.bfloat16
NZ, NX, NC, NY = 8, 4, 2, 8
STRIP, WIDTH, CH = 16, 64, 256
CELLS = STRIP * WIDTH
PIECES = ((64, 64), (128, 64), (192, 64), (0, 64))
INNER, EDGES = (0, 1, 2), (3,)
LAST_DOWN, LAST_UP = (0, 2), (1, 3)


def nt(left, right):
    return lax.dot_general(left, right, (((1,), (1,)), ((), ())), preferred_element_type=F32)


def tn(left, right):
    return lax.dot_general(left, right, (((0,), (0,)), ((), ())), preferred_element_type=F32)


def nn(left, right):
    return lax.dot_general(left, right, (((1,), (0,)), ((), ())), preferred_element_type=F32)


def kernel(
    fl, og, fi, mi, ti, sw, fw, mw, tw,
    gf_o, gm_o, gt_o, kg_o, ml_o, tl_o,
    fl_v, g_v, fi_v, mi_v, ti_v, sw_v, fw_v, mw_v, tw_v,
    big, flt, lvl, tmp, fg, gath, top, macc,
    term, crecv, csum, xrecv, zsend, zrecv, yown, yex,
    bterm, bxrecv, bz, bfin,
    in_sem, halo_s, halo_r, ring_s, edge_s, ring_r, last_r,
    core_s, core_r, x_s, x_r, z_s, z_r, y_s, y_r,
    bx_s, bx_r, bz_s, bz_r, bf_s, bf_r,
    seen_y, seen_z, seen_x, seen_c,
):
    z = lax.axis_index("dp_0")
    x = lax.axis_index("dp_1")
    c = lax.axis_index("dp_2")
    y = lax.axis_index("rows")

    def remote(src, dst, send, recv, **where):
        return pltpu.make_async_remote_copy(
            src_ref=src, dst_ref=dst, send_sem=send, recv_sem=recv,
            device_id=where, device_id_type=MESH,
        )

    def wait_bytes(ref, sem):
        remote(ref, ref, sem, sem, dp_2=1 - c).wait_recv()

    loads = [
        pltpu.make_async_copy(og, g_v.at[pl.ds(64, CELLS)], in_sem.at[0]),
        pltpu.make_async_copy(sw, sw_v, in_sem.at[1]),
        pltpu.make_async_copy(fl, fl_v, in_sem.at[2]),
        pltpu.make_async_copy(fi, fi_v, in_sem.at[3]),
        pltpu.make_async_copy(fw, fw_v, in_sem.at[4]),
        pltpu.make_async_copy(mi, mi_v, in_sem.at[5]),
        pltpu.make_async_copy(ti, ti_v, in_sem.at[6]),
        pltpu.make_async_copy(mw, mw_v, in_sem.at[7]),
        pltpu.make_async_copy(tw, tw_v, in_sem.at[8]),
    ]
    for load in loads[:3]:
        load.start()

    barrier = pltpu.get_barrier_semaphore()

    def greet(**where):
        pl.semaphore_signal(barrier, inc=1, device_id=where, device_id_type=MESH)

    down, up = lax.rem(y + 1, NY), lax.rem(y + NY - 1, NY)
    x_next, x_last = lax.rem(x + 1, NX), lax.rem(x + NX - 1, NX)
    z_next, z_last = lax.rem(z + 1, NZ), lax.rem(z + NZ - 1, NZ)
    for where in (
        dict(rows=down), dict(rows=up), dict(dp_1=x_next), dict(dp_1=x_last),
        dict(dp_0=z_next), dict(dp_0=z_last), dict(dp_2=1 - c),
    ):
        greet(**where)

    def tell(sem, *others):
        for i, where in enumerate(others):
            pl.semaphore_signal(sem.at[i], inc=1, device_id=where, device_id_type=MESH)

    def hear(sem, count=2):
        for i in range(count):
            pl.semaphore_wait(sem.at[i], 1)

    def tell_y():
        tell(seen_y, dict(rows=down), dict(rows=up))

    def tell_z():
        tell(seen_z, dict(dp_0=z_next), dict(dp_0=z_last))

    def widen(first, rows):
        value = g_v[pl.ds(first, rows), :].astype(F32)
        column = lax.rem(lax.broadcasted_iota(jnp.int32, (rows, CH), 0), WIDTH)
        after = jnp.where(column == WIDTH - 1, 0.0, pltpu.roll(value, rows - 1, 0))
        before = jnp.where(column == 0, 0.0, pltpu.roll(value, 1, 0))
        big[pl.ds(first, rows), 0:CH] = after.astype(BF16)
        big[pl.ds(first, rows), CH : 2 * CH] = value.astype(BF16)
        big[pl.ds(first, rows), 2 * CH : 3 * CH] = before.astype(BF16)

    loads[0].wait()

    @pl.loop(0, 4)
    def _(t):
        widen(pl.multiple_of(64 + t * 256, 64), 256)

    def send_piece(p, away, stride, to_down):
        origin = lax.rem(y + NY - away, NY) if to_down else lax.rem(y + away, NY)
        target = lax.rem(y + stride, NY) if to_down else lax.rem(y + NY - stride, NY)
        first, count = PIECES[p] if isinstance(p, int) else (pl.multiple_of(64 + 64 * p, 64), 64)
        block = gath.at[origin, pl.ds(first, count)]
        h = away + stride
        group = 3 if isinstance(p, int) and p in EDGES else p
        recv = last_r.at[0] if h == 4 else ring_r.at[h - 1, group, 0 if to_down else 1]
        send = edge_s if isinstance(p, int) and p in EDGES else ring_s
        remote(block, block, send.at[0], recv, rows=target).start()

    def came(h, group, to_down):
        wait_bytes(gath.at[0, pl.ds(0, 64)], ring_r.at[h - 1, group, 0 if to_down else 1])

    def start_own(p):
        send_piece(p, 0, 1, True)
        send_piece(p, 0, 1, False)

    def forward(h, p):
        for to_down in (True, False):
            came(h, p, to_down)
            if h < 3 or p in (LAST_DOWN if to_down else LAST_UP):
                send_piece(p, h, 1, to_down)

    def edges_from_home():
        for stride in (1, 2):
            for p in EDGES:
                send_piece(p, 0, stride, True)
                send_piece(p, 0, stride, False)

    def edges_on():
        for to_down in (True, False):
            came(2, 3, to_down)
            for p in EDGES:
                send_piece(p, 2, 1, to_down)
                if p in (LAST_DOWN if to_down else LAST_UP):
                    send_piece(p, 2, 2, to_down)

    def conv(rows):
        total = None
        for a in range(3):
            value = rows(64 * (2 - a))
            for b in range(3):
                term_ab = nt(value[:, CH * b : CH * b + CH], sw_v[3 * a + b])
                total = term_ab if total is None else total + term_ab
        return total

    def pool(total, put):
        for j in range(2):
            half = total[:, 128 * j : 128 * j + 128]
            for i in range(2):
                lvl[j, 64 * i : 64 * i + 64, :] = (
                    half[128 * i : 128 * i + 64] + half[128 * i + 64 : 128 * i + 128]
                )
            put(
                j,
                (lvl[j, pl.ds(0, 64, stride=2), :] + lvl[j, pl.ds(1, 64, stride=2), :]).astype(BF16),
            )

    def conv_inner(t):
        first = pl.multiple_of(128 + 256 * t, 128)
        out = pl.multiple_of(64 + 64 * t, 64)
        total = conv(lambda shift: big[pl.ds(first + shift, 256), :])
        fg[pl.ds(first, 256), :] = total.astype(BF16)

        def put(j, pooled):
            gath[y, pl.ds(out, 64), 128 * j : 128 * j + 128] = pooled

        pool(total, put)

    def conv_edges():
        low = CELLS - 128
        total = conv(
            lambda shift: jnp.concatenate(
                [big[shift : shift + 128, :], big[low + shift : low + shift + 128, :]]
            )
        )
        fg[0:128, :] = total[0:128].astype(BF16)
        fg[low:CELLS, :] = total[128:256].astype(BF16)

        def put(j, pooled):
            gath[y, 0:64, 128 * j : 128 * j + 128] = pooled

        pool(total, put)

    for load in loads[3:]:
        load.start()

    loads[1].wait()
    conv_inner(0)

    pl.semaphore_wait(barrier, 7)

    halo_down = remote(
        g_v.at[pl.ds(CELLS, 64)], g_v.at[pl.ds(0, 64)], halo_s.at[0], halo_r.at[0], rows=down
    )
    halo_up = remote(
        g_v.at[pl.ds(64, 64)], g_v.at[pl.ds(CELLS + 64, 64)], halo_s.at[0], halo_r.at[0], rows=up
    )
    halo_down.start()
    halo_up.start()

    tell_y()
    tell_z()
    tell(seen_x, dict(dp_1=x_next), dict(dp_1=x_last))

    start_own(0)

    @pl.loop(1, 3)
    def _(t):
        conv_inner(t)
        start_own(t)

    def swap_core(k):
        rows = pl.ds(pl.multiple_of(k * CH, CH), CH)
        return remote(
            term.at[1 - c, rows], crecv.at[rows], core_s.at[0], core_r.at[k // 5], dp_2=1 - c
        )

    def put_term(k, value):
        rows = pl.ds(pl.multiple_of(k * CH, CH), CH)
        value = value.astype(BF16)
        term[0, rows, :] = value[:, 0:128]
        term[1, rows, :] = value[:, 128:256]
        swap_core(k).start()

    def tap(k):
        row = pl.multiple_of((2 - k // 3) * 64, 64)
        col = pl.multiple_of(lax.rem(k, 3) * CH, CH)
        put_term(k, nn(flt[...], big[pl.ds(row, CELLS), pl.ds(col, CH)]))

    loads[2].wait()

    @pl.loop(0, 4)
    def _(t):
        rows = pl.ds(pl.multiple_of(t * 256, 256), 256)
        flt[:, rows] = fl_v[rows, :].T

    @pl.loop(3, 6)
    def _(k):
        tap(k)

    forward(1, 0)

    wait_bytes(g_v.at[pl.ds(0, 128)], halo_r.at[0])

    @pl.when(y == 0)
    def _():
        g_v[0:64, :] = jnp.zeros((64, CH), BF16)

    @pl.when(y == NY - 1)
    def _():
        g_v[CELLS + 64 : CELLS + 128, :] = jnp.zeros((64, CH), BF16)

    widen(0, 64)
    widen(CELLS + 64, 64)

    conv_edges()
    forward(1, 1)
    forward(1, 2)
    hear(seen_y)
    edges_from_home()
    tell_y()

    @pl.loop(0, 3)
    def _(k):
        tap(k)

    @pl.loop(6, 9)
    def _(k):
        tap(k)

    def coarse(s):
        mid = jnp.concatenate([gath[s, 0:32], gath[s, 64:256], gath[s, 32:64]])
        cells = pl.ds(pl.multiple_of(s * CH, CH), CH)
        gm_o[cells, :] = nt(mid, mw_v[...]).astype(BF16)
        macc[0:64, :] += tn(mi_v[cells, :], mid)
        wide = mid.astype(F32)
        for j in range(2):
            half = wide[:, 128 * j : 128 * j + 128]
            for i in range(4):
                tmp[j, 32 * i : 32 * i + 32, :] = (
                    half[64 * i : 64 * i + 32] + half[64 * i + 32 : 64 * i + 64]
                )
            top[:, 128 * j : 128 * j + 128] = (
                tmp[j, pl.ds(0, 64, stride=2), :] + tmp[j, pl.ds(1, 64, stride=2), :]
            ).astype(BF16)
        small = top[...]
        cells = pl.ds(pl.multiple_of(s * 64, 64), 64)
        gt_o[cells, :] = nt(small, tw_v[...]).astype(BF16)
        macc[64:192, :] += tn(ti_v[cells, :], small)

    def core_sum(k):
        rows = pl.ds(pl.multiple_of(k * CH, CH), CH)
        csum[rows, :] = (term[c, rows, :].astype(F32) + crecv[rows, :].astype(F32)).astype(BF16)

    def owner(s):
        return 4 * (s // 4) + lax.rem(z + s + 1, 4)

    def x_copy(s, d):
        x_to = lax.rem(x + d, NX)
        rows = pl.ds(pl.multiple_of((owner(s) * NX + x_to) * 80, 80), 80)
        return remote(
            csum.at[rows], xrecv.at[s, d - 1], x_s.at[0], x_r.at[s], dp_1=x_to
        )

    def x_send(batch):
        wait_bytes(crecv.at[pl.ds(1280 * batch, 1280)], core_r.at[batch])

        @pl.loop(5 * batch, 5 * batch + 5)
        def _(k):
            core_sum(k)

        @pl.loop(4 * batch, 4 * batch + 4)
        def _(s):
            for d in range(1, NX):
                x_copy(s, d).start()

    def z_copy(z_to):
        slot = lax.rem(z_to - z + NZ, NZ) - 1
        return remote(zsend.at[z_to], zrecv.at[slot], z_s.at[0], z_r.at[0], dp_0=z_to)

    def x_reduce(batch):
        @pl.loop(4 * batch, 4 * batch + 4)
        def _(s):
            wait_bytes(xrecv.at[s], x_r.at[s])
            z_to = owner(s)
            rows = pl.ds(pl.multiple_of((z_to * NX + x) * 80, 80), 80)
            total = csum[rows, :].astype(F32)
            for d in range(1, NX):
                total = total + xrecv[s, d - 1].astype(F32)
            zsend[z_to] = total.astype(BF16)

            @pl.when(z_to != z)
            def _():
                z_copy(z_to).start()

    hear(seen_x)
    hear(seen_z)
    tell_z()
    forward(2, 0)

    x_send(0)

    loads[3].wait()
    put_term(9, tn(fi_v[...], fg[...]))

    forward(2, 1)
    forward(2, 2)

    for load in loads[4:]:
        load.wait()
    macc[...] = jnp.zeros_like(macc)
    coarse(y)

    hear(seen_z)
    tell_z()

    x_send(1)

    hear(seen_y)
    edges_on()
    tell_y()

    came(1, 3, True)
    came(1, 3, False)
    coarse(lax.rem(y + 1, NY))
    coarse(lax.rem(y + NY - 1, NY))

    forward(3, 0)
    forward(3, 1)
    forward(3, 2)

    coarse(lax.rem(y + 2, NY))
    coarse(lax.rem(y + NY - 2, NY))

    for k in range(4):
        rows = slice(256 * k, 256 * k + 256)
        gf_o[rows, :] = nt(fg[rows, :], fw_v[...]).astype(BF16)

    hear(seen_y)
    tell(seen_c, dict(dp_2=1 - c))

    came(3, 3, True)
    came(3, 3, False)

    coarse(lax.rem(y + 3, NY))
    coarse(lax.rem(y + NY - 3, NY))

    hear(seen_z)

    x_reduce(0)

    wait_bytes(gath.at[0], last_r.at[0])

    coarse(lax.rem(y + 4, NY))
    hear(seen_c, 1)

    others = [(d, e) for d in range(NX) for e in range(NC) if d or e]
    for i in range(NX):
        for j in range(NC):
            bterm[NC * i + j] = macc[48 * i : 48 * i + 48, 128 * j : 128 * j + 128].astype(BF16)

    def bx_copy(d, e):
        x_to, c_to = lax.rem(x + d, NX), lax.rem(c + e, NC)
        return remote(
            bterm.at[NC * x_to + c_to], bxrecv.at[NC * d + e - 1], bx_s.at[0], bx_r.at[0],
            dp_1=x_to, dp_2=c_to,
        )

    for d, e in others:
        bx_copy(d, e).start()

    x_reduce(1)

    wait_bytes(bxrecv, bx_r.at[0])
    total = bterm[NC * x + c].astype(F32)
    for i in range(NX * NC - 1):
        total = total + bxrecv[i].astype(F32)
    bz[z] = total.astype(BF16)

    def bz_copy(d):
        return remote(bz.at[z], bz.at[z], bz_s.at[0], bz_r.at[0], dp_0=lax.rem(z + d, NZ))

    for d in range(1, NZ):
        bz_copy(d).start()

    wait_bytes(zrecv, z_r.at[0])
    total = zsend[z].astype(F32)
    for i in range(NZ - 1):
        total = total + zrecv[i].astype(F32)
    for i in range(NC):
        yown[i] = total[40 * i : 40 * i + 40].astype(BF16)
    yex[NY * c + y] = yown[c]

    def y_copy(d, e):
        c_to = lax.rem(c + e, NC)
        return remote(
            yown.at[c_to], yex.at[NY * c + y], y_s.at[0], y_r.at[0],
            rows=lax.rem(y + d, NY), dp_2=c_to,
        )

    for d in range(NY):
        for e in range(NC):
            if d or e:
                y_copy(d, e).start()

    wait_bytes(bz.at[pl.ds(0, NZ - 1)], bz_r.at[0])
    total = bz[0].astype(F32)
    for i in range(1, NZ):
        total = total + bz[i].astype(F32)
    bfin[NC * x + c] = total.astype(BF16)

    def bf_copy(d, e):
        return remote(
            bfin.at[NC * x + c], bfin.at[NC * x + c], bf_s.at[0], bf_r.at[0],
            dp_1=lax.rem(x + d, NX), dp_2=lax.rem(c + e, NC),
        )

    for d, e in others:
        bf_copy(d, e).start()

    wait_bytes(yex.at[pl.ds(0, NC * NY - 1)], y_r.at[0])
    for i in range(NC):
        total = yex[NY * i].astype(F32)
        for j in range(1, NY):
            total = total + yex[NY * i + j].astype(F32)
        kg_o[:, 128 * i : 128 * i + 128] = total

    for ref, sem in (
        (g_v.at[pl.ds(0, 128)], halo_s), (gath.at[pl.ds(0, 7), pl.ds(0, 192)], ring_s),
        (gath.at[pl.ds(0, 7), pl.ds(0, 64)], edge_s), (crecv, core_s),
        (csum.at[pl.ds(0, NZ * (NX - 1) * 80)], x_s), (zrecv, z_s), (yex.at[pl.ds(0, NC * NY - 1)], y_s),
        (bxrecv, bx_s), (bz.at[pl.ds(0, NZ - 1)], bz_s),
    ):
        wait_bytes(ref, sem.at[0])

    wait_bytes(bfin.at[pl.ds(0, NX * NC - 1)], bf_r.at[0])
    for i in range(NX):
        for j in range(NC):
            block = bfin[NC * i + j].astype(F32)
            cols = slice(128 * j, 128 * j + 128)
            if i == 0:
                ml_o[0:48, cols] = block
            elif i == 1:
                ml_o[48:64, cols] = block[0:16]
                tl_o[0:32, cols] = block[16:48]
            else:
                tl_o[48 * i - 64 : 48 * i - 16, cols] = block
    wait_bytes(bfin.at[pl.ds(0, NX * NC - 1)], bf_s.at[0])


def store(*refs):
    copies = [pltpu.make_async_copy(refs[i], refs[6 + i], refs[12].at[i]) for i in range(6)]
    for copy in copies:
        copy.start()
    for copy in copies:
        copy.wait()


def body(
    fine_level, out_grad, fine_input, mid_input, top_input,
    smooth_weight, fine_lateral, mid_lateral, top_lateral,
):
    sem = pltpu.SemaphoreType.DMA
    sizes = [
        ((CELLS, CH), BF16), ((CELLS + 128, CH), BF16), ((CELLS, CH), BF16), ((2048, 64), BF16),
        ((512, 128), BF16), ((9, CH, CH), BF16), ((CH, CH), BF16), ((64, CH), BF16), ((128, CH), BF16),
        ((CELLS + 128, 3 * CH), BF16), ((CH, CELLS), BF16),
        ((2, 128, 128), F32), ((2, 128, 128), F32), ((CELLS, CH), BF16),
        ((NY, CH, CH), BF16), ((64, CH), BF16), ((192, CH), F32),
        ((2, 2560, 128), BF16), ((2560, 128), BF16), ((2560, 128), BF16), ((NZ, NX - 1, 80, 128), BF16),
        ((NZ, 80, 128), BF16), ((NZ - 1, 80, 128), BF16), ((NC, 40, 128), BF16), ((NC * NY, 40, 128), BF16),
        ((NX * NC, 48, 128), BF16), ((NX * NC - 1, 48, 128), BF16),
        ((NZ, 48, 128), BF16), ((NX * NC, 48, 128), BF16),
    ]
    sems = [
        (9,), (1,), (1,), (1,), (1,), (3, 4, 2), (1,),
        (1,), (2,), (1,), (NZ,), (1,), (1,), (1,), (1,),
        (1,), (1,), (1,), (1,), (1,), (1,),
    ]
    shapes = [
        ((CELLS, CH), BF16), ((2048, 64), BF16), ((512, 128), BF16),
        ((40, CH), F32), ((64, CH), F32), ((128, CH), F32),
    ]
    hbm = pl.BlockSpec(memory_space=pltpu.HBM)
    anywhere = pl.BlockSpec(memory_space=pl.ANY)
    grads = pl.pallas_call(
        kernel,
        out_shape=[pltpu.VMEM(*shape) for shape in shapes],
        in_specs=[hbm] * 9,
        out_specs=[pl.BlockSpec(memory_space=pltpu.VMEM)] * 6,
        scratch_shapes=[pltpu.VMEM(*size) for size in sizes] + [sem(size) for size in sems]
        + [pltpu.SemaphoreType.REGULAR((count,)) for count in (2, 2, 2, 1)],
        compiler_params=pltpu.CompilerParams(
            collective_id=0, has_side_effects=True, vmem_limit_bytes=48 * 1024 * 1024
        ),
    )(*(pltpu.with_memory_space_constraint(value, pltpu.HBM) for value in (
        fine_level.reshape(CELLS, CH), out_grad.reshape(CELLS, CH), fine_input.reshape(CELLS, CH),
        mid_input.reshape(2048, 64), top_input.reshape(512, 128), smooth_weight.reshape(9, CH, CH),
        fine_lateral, mid_lateral, top_lateral,
    )))
    grads = pl.pallas_call(
        store,
        out_shape=[pltpu.HBM(*shape) for shape in shapes],
        in_specs=[anywhere] * 6,
        out_specs=[hbm] * 6,
        scratch_shapes=[sem((6,))],
    )(*(pltpu.with_memory_space_constraint(grad, pltpu.VMEM) for grad in grads))
    return (
        grads[0].reshape(out_grad.shape), grads[1].reshape(mid_input.shape),
        grads[2].reshape(top_input.shape), grads[3], grads[4], grads[5],
    )


def solution(mesh):
    torus = Mesh(
        mesh.devices.reshape(NZ, NX, NC, NY), ("dp_0", "dp_1", "dp_2", "rows")
    )
    return jax.shard_map(
        body,
        mesh=torus,
        in_specs=(
            P(DP, "rows", None, None), P(DP, "rows", None, None), P(DP, "rows", None, None),
            P(DP, None, None, "rows"), P(DP, None, None, "rows"),
            P(), P(), P("rows", None), P("rows", None),
        ),
        out_specs=(
            P(DP, "rows", None, None), P(DP, None, None, "rows"), P(DP, None, None, "rows"),
            P(DP, None), P("rows", None), P("rows", None),
        ),
        check_vma=False,
    )
```

```python
import jax
import jax.numpy as jnp
from jax import lax
from jax.experimental import pallas as pl
from jax.experimental.pallas import tpu as pltpu
from jax.sharding import Mesh
from jax.sharding import PartitionSpec as P

DP = ("dp_0", "dp_1", "dp_2")
MESH = pl.DeviceIdType.MESH
F32 = jnp.float32
BF16 = jnp.bfloat16
NZ, NX, NC, NY = 8, 4, 2, 8
STRIP, WIDTH, CH = 16, 64, 256
CELLS = STRIP * WIDTH
PIECES = ((64, 64), (128, 64), (192, 64), (0, 64))
INNER, EDGES = (0, 1, 2), (3,)
X_FAR, FAR = (2, 1, 3), (4, 3, 5, 2, 6, 1, 7)
LAST_DOWN, LAST_UP = (0, 2), (1, 3)


def nt(left, right):
    return lax.dot_general(left, right, (((1,), (1,)), ((), ())), preferred_element_type=F32)


def tn(left, right):
    return lax.dot_general(left, right, (((0,), (0,)), ((), ())), preferred_element_type=F32)


def nn(left, right):
    return lax.dot_general(left, right, (((1,), (0,)), ((), ())), preferred_element_type=F32)


def kernel(
    fl, og, fi, mi, ti, sw, fw, mw, tw,
    gf_o, gm_o, gt_o, kg_o, ml_o, tl_o,
    fl_v, g_v, fi_v, mi_v, ti_v, sw_v, fw_v, mw_v, tw_v,
    big, flt, lvl, tmp, fg, gath, top, macc,
    term, crecv, csum, xrecv, zsend, zrecv, yown, yex,
    bterm, bxrecv, bz, bfin,
    in_sem, halo_s, halo_r, ring_s, edge_s, ring_r, last_r,
    core_s, core_r, x_s, x_r, z_s, z_r, y_s, y_r,
    bx_s, bx_r, bz_s, bz_r, bf_s, bf_r,
    seen_y, seen_z, seen_x, seen_c,
):
    z = lax.axis_index("dp_0")
    x = lax.axis_index("dp_1")
    c = lax.axis_index("dp_2")
    y = lax.axis_index("rows")

    def remote(src, dst, send, recv, **where):
        return pltpu.make_async_remote_copy(
            src_ref=src, dst_ref=dst, send_sem=send, recv_sem=recv,
            device_id=where, device_id_type=MESH,
        )

    def wait_bytes(ref, sem):
        remote(ref, ref, sem, sem, dp_2=1 - c).wait_recv()

    loads = [
        pltpu.make_async_copy(og, g_v.at[pl.ds(64, CELLS)], in_sem.at[0]),
        pltpu.make_async_copy(sw, sw_v, in_sem.at[1]),
        pltpu.make_async_copy(fl, fl_v, in_sem.at[2]),
        pltpu.make_async_copy(fi, fi_v, in_sem.at[3]),
        pltpu.make_async_copy(fw, fw_v, in_sem.at[4]),
        pltpu.make_async_copy(mi, mi_v, in_sem.at[5]),
        pltpu.make_async_copy(ti, ti_v, in_sem.at[6]),
        pltpu.make_async_copy(mw, mw_v, in_sem.at[7]),
        pltpu.make_async_copy(tw, tw_v, in_sem.at[8]),
    ]
    for load in loads[:3]:
        load.start()

    barrier = pltpu.get_barrier_semaphore()

    def greet(**where):
        pl.semaphore_signal(barrier, inc=1, device_id=where, device_id_type=MESH)

    down, up = lax.rem(y + 1, NY), lax.rem(y + NY - 1, NY)
    x_next, x_last = lax.rem(x + 1, NX), lax.rem(x + NX - 1, NX)
    z_next, z_last = lax.rem(z + 1, NZ), lax.rem(z + NZ - 1, NZ)
    for where in (
        dict(rows=down), dict(rows=up), dict(dp_1=x_next), dict(dp_1=x_last),
        dict(dp_0=z_next), dict(dp_0=z_last), dict(dp_2=1 - c),
    ):
        greet(**where)

    def tell(sem, *others):
        for i, where in enumerate(others):
            pl.semaphore_signal(sem.at[i], inc=1, device_id=where, device_id_type=MESH)

    def hear(sem, count=2):
        for i in range(count):
            pl.semaphore_wait(sem.at[i], 1)

    def tell_y():
        tell(seen_y, dict(rows=down), dict(rows=up))

    def tell_z():
        tell(seen_z, dict(dp_0=z_next), dict(dp_0=z_last))

    def widen(first, rows):
        value = g_v[pl.ds(first, rows), :].astype(F32)
        column = lax.rem(lax.broadcasted_iota(jnp.int32, (rows, CH), 0), WIDTH)
        after = jnp.where(column == WIDTH - 1, 0.0, pltpu.roll(value, rows - 1, 0))
        before = jnp.where(column == 0, 0.0, pltpu.roll(value, 1, 0))
        big[pl.ds(first, rows), 0:CH] = after.astype(BF16)
        big[pl.ds(first, rows), CH : 2 * CH] = value.astype(BF16)
        big[pl.ds(first, rows), 2 * CH : 3 * CH] = before.astype(BF16)

    loads[0].wait()

    @pl.loop(0, 4)
    def _(t):
        widen(pl.multiple_of(64 + t * 256, 64), 256)

    def send_piece(p, away, stride, to_down):
        origin = lax.rem(y + NY - away, NY) if to_down else lax.rem(y + away, NY)
        target = lax.rem(y + stride, NY) if to_down else lax.rem(y + NY - stride, NY)
        first, count = PIECES[p] if isinstance(p, int) else (pl.multiple_of(64 + 64 * p, 64), 64)
        block = gath.at[origin, pl.ds(first, count)]
        h = away + stride
        group = 3 if isinstance(p, int) and p in EDGES else p
        recv = last_r.at[0] if h == 4 else ring_r.at[h - 1, group, 0 if to_down else 1]
        send = edge_s if isinstance(p, int) and p in EDGES else ring_s
        remote(block, block, send.at[0], recv, rows=target).start()

    def came(h, group, to_down):
        wait_bytes(gath.at[0, pl.ds(0, 64)], ring_r.at[h - 1, group, 0 if to_down else 1])

    def start_own(p):
        send_piece(p, 0, 1, True)
        send_piece(p, 0, 1, False)

    def forward(h, p):
        for to_down in (True, False):
            came(h, p, to_down)
            if h < 3 or p in (LAST_DOWN if to_down else LAST_UP):
                send_piece(p, h, 1, to_down)

    def edges_from_home():
        for stride in (1, 2):
            for p in EDGES:
                send_piece(p, 0, stride, True)
                send_piece(p, 0, stride, False)

    def edges_on():
        for to_down in (True, False):
            came(2, 3, to_down)
            for p in EDGES:
                send_piece(p, 2, 1, to_down)
                if p in (LAST_DOWN if to_down else LAST_UP):
                    send_piece(p, 2, 2, to_down)

    def conv(rows):
        total = None
        for a in range(3):
            value = rows(64 * (2 - a))
            for b in range(3):
                term_ab = nt(value[:, CH * b : CH * b + CH], sw_v[3 * a + b])
                total = term_ab if total is None else total + term_ab
        return total

    def pool(total, put):
        for j in range(2):
            half = total[:, 128 * j : 128 * j + 128]
            for i in range(2):
                lvl[j, 64 * i : 64 * i + 64, :] = (
                    half[128 * i : 128 * i + 64] + half[128 * i + 64 : 128 * i + 128]
                )
            put(
                j,
                (lvl[j, pl.ds(0, 64, stride=2), :] + lvl[j, pl.ds(1, 64, stride=2), :]).astype(BF16),
            )

    def conv_inner(t):
        first = pl.multiple_of(128 + 256 * t, 128)
        out = pl.multiple_of(64 + 64 * t, 64)
        total = conv(lambda shift: big[pl.ds(first + shift, 256), :])
        fg[pl.ds(first, 256), :] = total.astype(BF16)

        def put(j, pooled):
            gath[y, pl.ds(out, 64), 128 * j : 128 * j + 128] = pooled

        pool(total, put)

    def conv_edges():
        low = CELLS - 128
        total = conv(
            lambda shift: jnp.concatenate(
                [big[shift : shift + 128, :], big[low + shift : low + shift + 128, :]]
            )
        )
        fg[0:128, :] = total[0:128].astype(BF16)
        fg[low:CELLS, :] = total[128:256].astype(BF16)

        def put(j, pooled):
            gath[y, 0:64, 128 * j : 128 * j + 128] = pooled

        pool(total, put)

    for load in loads[3:]:
        load.start()

    loads[1].wait()
    conv_inner(0)

    pl.semaphore_wait(barrier, 7)

    halo_down = remote(
        g_v.at[pl.ds(CELLS, 64)], g_v.at[pl.ds(0, 64)], halo_s.at[0], halo_r.at[0], rows=down
    )
    halo_up = remote(
        g_v.at[pl.ds(64, 64)], g_v.at[pl.ds(CELLS + 64, 64)], halo_s.at[0], halo_r.at[0], rows=up
    )
    halo_down.start()
    halo_up.start()

    tell_y()
    tell_z()
    tell(seen_x, dict(dp_1=x_next), dict(dp_1=x_last))

    start_own(0)

    @pl.loop(1, 3)
    def _(t):
        conv_inner(t)
        start_own(t)

    def swap_core(k):
        rows = pl.ds(pl.multiple_of(k * CH, CH), CH)
        return remote(
            term.at[1 - c, rows], crecv.at[rows], core_s.at[0], core_r.at[k // 5], dp_2=1 - c
        )

    def put_term(k, value):
        rows = pl.ds(pl.multiple_of(k * CH, CH), CH)
        value = value.astype(BF16)
        term[0, rows, :] = value[:, 0:128]
        term[1, rows, :] = value[:, 128:256]
        swap_core(k).start()

    def tap(k):
        row = pl.multiple_of((2 - k // 3) * 64, 64)
        col = pl.multiple_of(lax.rem(k, 3) * CH, CH)
        put_term(k, nn(flt[...], big[pl.ds(row, CELLS), pl.ds(col, CH)]))

    loads[2].wait()

    @pl.loop(0, 4)
    def _(t):
        rows = pl.ds(pl.multiple_of(t * 256, 256), 256)
        flt[:, rows] = fl_v[rows, :].T

    @pl.loop(3, 6)
    def _(k):
        tap(k)

    forward(1, 0)

    wait_bytes(g_v.at[pl.ds(0, 128)], halo_r.at[0])

    @pl.when(y == 0)
    def _():
        g_v[0:64, :] = jnp.zeros((64, CH), BF16)

    @pl.when(y == NY - 1)
    def _():
        g_v[CELLS + 64 : CELLS + 128, :] = jnp.zeros((64, CH), BF16)

    widen(0, 64)
    widen(CELLS + 64, 64)

    conv_edges()
    forward(1, 1)
    forward(1, 2)
    hear(seen_y)
    edges_from_home()
    tell_y()

    @pl.loop(0, 3)
    def _(k):
        tap(k)

    @pl.loop(6, 9)
    def _(k):
        tap(k)

    def coarse(s):
        mid = jnp.concatenate([gath[s, 0:32], gath[s, 64:256], gath[s, 32:64]])
        cells = pl.ds(pl.multiple_of(s * CH, CH), CH)
        gm_o[cells, :] = nt(mid, mw_v[...]).astype(BF16)
        macc[0:64, :] += tn(mi_v[cells, :], mid)
        wide = mid.astype(F32)
        for j in range(2):
            half = wide[:, 128 * j : 128 * j + 128]
            for i in range(4):
                tmp[j, 32 * i : 32 * i + 32, :] = (
                    half[64 * i : 64 * i + 32] + half[64 * i + 32 : 64 * i + 64]
                )
            top[:, 128 * j : 128 * j + 128] = (
                tmp[j, pl.ds(0, 64, stride=2), :] + tmp[j, pl.ds(1, 64, stride=2), :]
            ).astype(BF16)
        small = top[...]
        cells = pl.ds(pl.multiple_of(s * 64, 64), 64)
        gt_o[cells, :] = nt(small, tw_v[...]).astype(BF16)
        macc[64:192, :] += tn(ti_v[cells, :], small)

    def core_sum(k):
        rows = pl.ds(pl.multiple_of(k * CH, CH), CH)
        csum[rows, :] = (term[c, rows, :].astype(F32) + crecv[rows, :].astype(F32)).astype(BF16)

    def owner(s):
        return 4 * (s // 4) + lax.rem(z + s + 1, 4)

    def x_copy(s, d):
        x_to = lax.rem(x + d, NX)
        rows = pl.ds(pl.multiple_of((owner(s) * NX + x_to) * 80, 80), 80)
        return remote(
            csum.at[rows], xrecv.at[s, d - 1], x_s.at[0], x_r.at[s], dp_1=x_to
        )

    def x_send(batch):
        wait_bytes(crecv.at[pl.ds(1280 * batch, 1280)], core_r.at[batch])

        @pl.loop(5 * batch, 5 * batch + 5)
        def _(k):
            core_sum(k)

        @pl.loop(4 * batch, 4 * batch + 4)
        def _(s):
            for d in X_FAR:
                x_copy(s, d).start()

    def z_copy(z_to):
        slot = lax.rem(z_to - z + NZ, NZ) - 1
        return remote(zsend.at[z_to], zrecv.at[slot], z_s.at[0], z_r.at[0], dp_0=z_to)

    def x_reduce(batch):
        @pl.loop(4 * batch, 4 * batch + 4)
        def _(s):
            wait_bytes(xrecv.at[s], x_r.at[s])
            z_to = owner(s)
            rows = pl.ds(pl.multiple_of((z_to * NX + x) * 80, 80), 80)
            total = csum[rows, :].astype(F32)
            for d in range(1, NX):
                total = total + xrecv[s, d - 1].astype(F32)
            zsend[z_to] = total.astype(BF16)

            @pl.when(z_to != z)
            def _():
                z_copy(z_to).start()

    hear(seen_x)
    hear(seen_z)
    tell_z()
    x_send(0)

    forward(2, 0)

    loads[3].wait()
    put_term(9, tn(fi_v[...], fg[...]))

    forward(2, 1)
    forward(2, 2)

    for load in loads[4:]:
        load.wait()
    macc[...] = jnp.zeros_like(macc)
    coarse(y)

    hear(seen_z)
    tell_z()

    x_send(1)

    hear(seen_y)
    edges_on()
    tell_y()

    came(1, 3, True)
    came(1, 3, False)
    coarse(lax.rem(y + 1, NY))
    coarse(lax.rem(y + NY - 1, NY))

    forward(3, 0)
    forward(3, 1)
    forward(3, 2)

    coarse(lax.rem(y + 2, NY))
    coarse(lax.rem(y + NY - 2, NY))

    for k in range(4):
        rows = slice(256 * k, 256 * k + 256)
        gf_o[rows, :] = nt(fg[rows, :], fw_v[...]).astype(BF16)

    hear(seen_y)
    tell(seen_c, dict(dp_2=1 - c))

    came(3, 3, True)
    came(3, 3, False)

    coarse(lax.rem(y + 3, NY))
    coarse(lax.rem(y + NY - 3, NY))

    hear(seen_z)

    x_reduce(0)

    wait_bytes(gath.at[0], last_r.at[0])

    coarse(lax.rem(y + 4, NY))
    hear(seen_c, 1)

    others = [(d, e) for d in X_FAR for e in (1, 0)] + [(0, 1)]
    for i in range(NX):
        for j in range(NC):
            bterm[NC * i + j] = macc[48 * i : 48 * i + 48, 128 * j : 128 * j + 128].astype(BF16)

    def bx_copy(d, e):
        x_to, c_to = lax.rem(x + d, NX), lax.rem(c + e, NC)
        return remote(
            bterm.at[NC * x_to + c_to], bxrecv.at[NC * d + e - 1], bx_s.at[0], bx_r.at[0],
            dp_1=x_to, dp_2=c_to,
        )

    for d, e in others:
        bx_copy(d, e).start()

    x_reduce(1)

    wait_bytes(bxrecv, bx_r.at[0])
    total = bterm[NC * x + c].astype(F32)
    for i in range(NX * NC - 1):
        total = total + bxrecv[i].astype(F32)
    bz[z] = total.astype(BF16)

    def bz_copy(d):
        return remote(bz.at[z], bz.at[z], bz_s.at[0], bz_r.at[0], dp_0=lax.rem(z + d, NZ))

    for d in FAR:
        bz_copy(d).start()

    wait_bytes(zrecv, z_r.at[0])
    total = zsend[z].astype(F32)
    for i in range(NZ - 1):
        total = total + zrecv[i].astype(F32)
    for i in range(NC):
        yown[i] = total[40 * i : 40 * i + 40].astype(BF16)
    yex[NY * c + y] = yown[c]

    def y_copy(d, e):
        c_to = lax.rem(c + e, NC)
        return remote(
            yown.at[c_to], yex.at[NY * c + y], y_s.at[0], y_r.at[0],
            rows=lax.rem(y + d, NY), dp_2=c_to,
        )

    for d in FAR:
        for e in (1, 0):
            y_copy(d, e).start()
    y_copy(0, 1).start()

    wait_bytes(bz.at[pl.ds(0, NZ - 1)], bz_r.at[0])
    total = bz[0].astype(F32)
    for i in range(1, NZ):
        total = total + bz[i].astype(F32)
    bfin[NC * x + c] = total.astype(BF16)

    def bf_copy(d, e):
        return remote(
            bfin.at[NC * x + c], bfin.at[NC * x + c], bf_s.at[0], bf_r.at[0],
            dp_1=lax.rem(x + d, NX), dp_2=lax.rem(c + e, NC),
        )

    for d, e in others:
        bf_copy(d, e).start()

    wait_bytes(yex.at[pl.ds(0, NC * NY - 1)], y_r.at[0])
    for i in range(NC):
        total = yex[NY * i].astype(F32)
        for j in range(1, NY):
            total = total + yex[NY * i + j].astype(F32)
        kg_o[:, 128 * i : 128 * i + 128] = total

    for ref, sem in (
        (g_v.at[pl.ds(0, 128)], halo_s), (gath.at[pl.ds(0, 7), pl.ds(0, 192)], ring_s),
        (gath.at[pl.ds(0, 7), pl.ds(0, 64)], edge_s), (crecv, core_s),
        (csum.at[pl.ds(0, NZ * (NX - 1) * 80)], x_s), (zrecv, z_s), (yex.at[pl.ds(0, NC * NY - 1)], y_s),
        (bxrecv, bx_s), (bz.at[pl.ds(0, NZ - 1)], bz_s),
    ):
        wait_bytes(ref, sem.at[0])

    wait_bytes(bfin.at[pl.ds(0, NX * NC - 1)], bf_r.at[0])
    for i in range(NX):
        for j in range(NC):
            block = bfin[NC * i + j].astype(F32)
            cols = slice(128 * j, 128 * j + 128)
            if i == 0:
                ml_o[0:48, cols] = block
            elif i == 1:
                ml_o[48:64, cols] = block[0:16]
                tl_o[0:32, cols] = block[16:48]
            else:
                tl_o[48 * i - 64 : 48 * i - 16, cols] = block
    wait_bytes(bfin.at[pl.ds(0, NX * NC - 1)], bf_s.at[0])


def store(*refs):
    copies = [pltpu.make_async_copy(refs[i], refs[6 + i], refs[12].at[i]) for i in range(6)]
    for copy in copies:
        copy.start()
    for copy in copies:
        copy.wait()


def body(
    fine_level, out_grad, fine_input, mid_input, top_input,
    smooth_weight, fine_lateral, mid_lateral, top_lateral,
):
    sem = pltpu.SemaphoreType.DMA
    sizes = [
        ((CELLS, CH), BF16), ((CELLS + 128, CH), BF16), ((CELLS, CH), BF16), ((2048, 64), BF16),
        ((512, 128), BF16), ((9, CH, CH), BF16), ((CH, CH), BF16), ((64, CH), BF16), ((128, CH), BF16),
        ((CELLS + 128, 3 * CH), BF16), ((CH, CELLS), BF16),
        ((2, 128, 128), F32), ((2, 128, 128), F32), ((CELLS, CH), BF16),
        ((NY, CH, CH), BF16), ((64, CH), BF16), ((192, CH), F32),
        ((2, 2560, 128), BF16), ((2560, 128), BF16), ((2560, 128), BF16), ((NZ, NX - 1, 80, 128), BF16),
        ((NZ, 80, 128), BF16), ((NZ - 1, 80, 128), BF16), ((NC, 40, 128), BF16), ((NC * NY, 40, 128), BF16),
        ((NX * NC, 48, 128), BF16), ((NX * NC - 1, 48, 128), BF16),
        ((NZ, 48, 128), BF16), ((NX * NC, 48, 128), BF16),
    ]
    sems = [
        (9,), (1,), (1,), (1,), (1,), (3, 4, 2), (1,),
        (1,), (2,), (1,), (NZ,), (1,), (1,), (1,), (1,),
        (1,), (1,), (1,), (1,), (1,), (1,),
    ]
    shapes = [
        ((CELLS, CH), BF16), ((2048, 64), BF16), ((512, 128), BF16),
        ((40, CH), F32), ((64, CH), F32), ((128, CH), F32),
    ]
    hbm = pl.BlockSpec(memory_space=pltpu.HBM)
    anywhere = pl.BlockSpec(memory_space=pl.ANY)
    grads = pl.pallas_call(
        kernel,
        out_shape=[pltpu.VMEM(*shape) for shape in shapes],
        in_specs=[hbm] * 9,
        out_specs=[pl.BlockSpec(memory_space=pltpu.VMEM)] * 6,
        scratch_shapes=[pltpu.VMEM(*size) for size in sizes] + [sem(size) for size in sems]
        + [pltpu.SemaphoreType.REGULAR((count,)) for count in (2, 2, 2, 1)],
        compiler_params=pltpu.CompilerParams(
            collective_id=0, has_side_effects=True, vmem_limit_bytes=48 * 1024 * 1024
        ),
    )(*(pltpu.with_memory_space_constraint(value, pltpu.HBM) for value in (
        fine_level.reshape(CELLS, CH), out_grad.reshape(CELLS, CH), fine_input.reshape(CELLS, CH),
        mid_input.reshape(2048, 64), top_input.reshape(512, 128), smooth_weight.reshape(9, CH, CH),
        fine_lateral, mid_lateral, top_lateral,
    )))
    grads = pl.pallas_call(
        store,
        out_shape=[pltpu.HBM(*shape) for shape in shapes],
        in_specs=[anywhere] * 6,
        out_specs=[hbm] * 6,
        scratch_shapes=[sem((6,))],
    )(*(pltpu.with_memory_space_constraint(grad, pltpu.VMEM) for grad in grads))
    return (
        grads[0].reshape(out_grad.shape), grads[1].reshape(mid_input.shape),
        grads[2].reshape(top_input.shape), grads[3], grads[4], grads[5],
    )


def solution(mesh):
    torus = Mesh(
        mesh.devices.reshape(NZ, NX, NC, NY), ("dp_0", "dp_1", "dp_2", "rows")
    )
    return jax.shard_map(
        body,
        mesh=torus,
        in_specs=(
            P(DP, "rows", None, None), P(DP, "rows", None, None), P(DP, "rows", None, None),
            P(DP, None, None, "rows"), P(DP, None, None, "rows"),
            P(), P(), P("rows", None), P("rows", None),
        ),
        out_specs=(
            P(DP, "rows", None, None), P(DP, None, None, "rows"), P(DP, None, None, "rows"),
            P(DP, None), P("rows", None), P("rows", None),
        ),
        check_vma=False,
    )
```

```python
import jax
import jax.numpy as jnp
from jax import lax
from jax.experimental import pallas as pl
from jax.experimental.pallas import tpu as pltpu
from jax.sharding import Mesh
from jax.sharding import PartitionSpec as P

DP = ("dp_0", "dp_1", "dp_2")
MESH = pl.DeviceIdType.MESH
F32 = jnp.float32
BF16 = jnp.bfloat16
NZ, NX, NC, NY = 8, 4, 2, 8
STRIP, WIDTH, CH = 16, 64, 256
CELLS = STRIP * WIDTH
PIECES = ((64, 64), (128, 64), (192, 64), (0, 64))
INNER, EDGES = (0, 1, 2), (3,)
X_FAR, FAR = (2, 1, 3), (4, 3, 5, 2, 6, 1, 7)
LAST_DOWN, LAST_UP = (0, 2), (1, 3)


def nt(left, right):
    return lax.dot_general(left, right, (((1,), (1,)), ((), ())), preferred_element_type=F32)


def tn(left, right):
    return lax.dot_general(left, right, (((0,), (0,)), ((), ())), preferred_element_type=F32)


def nn(left, right):
    return lax.dot_general(left, right, (((1,), (0,)), ((), ())), preferred_element_type=F32)


def kernel(
    fl, og, fi, mi, ti, sw, fw, mw, tw,
    gf_o, gm_o, gt_o, kg_o, ml_o, tl_o,
    fl_v, g_v, fi_v, mi_v, ti_v, sw_v, fw_v, mw_v, tw_v,
    big, flt, lvl, tmp, fg, gath, top, macc,
    term, crecv, csum, xrecv, zsend, zrecv, yown, yex,
    bterm, bxrecv, bz, bfin,
    in_sem, halo_s, halo_r, ring_s, edge_s, ring_r, last_r,
    core_s, core_r, x_s, x_r, z_s, z_r, y_s, y_r,
    bx_s, bx_r, bz_s, bz_r, bf_s, bf_r,
    seen_y, seen_z, seen_x, seen_c,
):
    z = lax.axis_index("dp_0")
    x = lax.axis_index("dp_1")
    c = lax.axis_index("dp_2")
    y = lax.axis_index("rows")

    def remote(src, dst, send, recv, **where):
        return pltpu.make_async_remote_copy(
            src_ref=src, dst_ref=dst, send_sem=send, recv_sem=recv,
            device_id=where, device_id_type=MESH,
        )

    def wait_bytes(ref, sem):
        remote(ref, ref, sem, sem, dp_2=1 - c).wait_recv()

    loads = [
        pltpu.make_async_copy(og, g_v.at[pl.ds(64, CELLS)], in_sem.at[0]),
        pltpu.make_async_copy(sw, sw_v, in_sem.at[1]),
        pltpu.make_async_copy(fl, fl_v, in_sem.at[2]),
        pltpu.make_async_copy(fi, fi_v, in_sem.at[3]),
        pltpu.make_async_copy(fw, fw_v, in_sem.at[4]),
        pltpu.make_async_copy(mi, mi_v, in_sem.at[5]),
        pltpu.make_async_copy(ti, ti_v, in_sem.at[6]),
        pltpu.make_async_copy(mw, mw_v, in_sem.at[7]),
        pltpu.make_async_copy(tw, tw_v, in_sem.at[8]),
    ]
    for load in loads[:3]:
        load.start()

    barrier = pltpu.get_barrier_semaphore()

    def greet(**where):
        pl.semaphore_signal(barrier, inc=1, device_id=where, device_id_type=MESH)

    down, up = lax.rem(y + 1, NY), lax.rem(y + NY - 1, NY)
    x_next, x_last = lax.rem(x + 1, NX), lax.rem(x + NX - 1, NX)
    z_next, z_last = lax.rem(z + 1, NZ), lax.rem(z + NZ - 1, NZ)
    for where in (
        dict(rows=down), dict(rows=up), dict(dp_1=x_next), dict(dp_1=x_last),
        dict(dp_0=z_next), dict(dp_0=z_last), dict(dp_2=1 - c),
    ):
        greet(**where)

    def tell(sem, *others):
        for i, where in enumerate(others):
            pl.semaphore_signal(sem.at[i], inc=1, device_id=where, device_id_type=MESH)

    def hear(sem, count=2):
        for i in range(count):
            pl.semaphore_wait(sem.at[i], 1)

    def tell_y():
        tell(seen_y, dict(rows=down), dict(rows=up))

    def tell_z():
        tell(seen_z, dict(dp_0=z_next), dict(dp_0=z_last))

    def widen(first, rows):
        value = g_v[pl.ds(first, rows), :].astype(F32)
        column = lax.rem(lax.broadcasted_iota(jnp.int32, (rows, CH), 0), WIDTH)
        after = jnp.where(column == WIDTH - 1, 0.0, pltpu.roll(value, rows - 1, 0))
        before = jnp.where(column == 0, 0.0, pltpu.roll(value, 1, 0))
        big[pl.ds(first, rows), 0:CH] = after.astype(BF16)
        big[pl.ds(first, rows), CH : 2 * CH] = value.astype(BF16)
        big[pl.ds(first, rows), 2 * CH : 3 * CH] = before.astype(BF16)

    loads[0].wait()

    @pl.loop(0, 4)
    def _(t):
        widen(pl.multiple_of(64 + t * 256, 64), 256)

    def send_piece(p, away, stride, to_down):
        origin = lax.rem(y + NY - away, NY) if to_down else lax.rem(y + away, NY)
        target = lax.rem(y + stride, NY) if to_down else lax.rem(y + NY - stride, NY)
        first, count = PIECES[p] if isinstance(p, int) else (pl.multiple_of(64 + 64 * p, 64), 64)
        block = gath.at[origin, pl.ds(first, count)]
        h = away + stride
        group = 3 if isinstance(p, int) and p in EDGES else p
        recv = last_r.at[0] if h == 4 else ring_r.at[h - 1, group, 0 if to_down else 1]
        send = edge_s if isinstance(p, int) and p in EDGES else ring_s
        remote(block, block, send.at[0], recv, rows=target).start()

    def came(h, group, to_down):
        wait_bytes(gath.at[0, pl.ds(0, 64)], ring_r.at[h - 1, group, 0 if to_down else 1])

    def start_own(p):
        send_piece(p, 0, 1, True)
        send_piece(p, 0, 1, False)

    def forward(h, p):
        for to_down in (True, False):
            came(h, p, to_down)
            if h < 3 or p in (LAST_DOWN if to_down else LAST_UP):
                send_piece(p, h, 1, to_down)

    def edges_from_home():
        for stride in (2, 1):
            for p in EDGES:
                send_piece(p, 0, stride, True)
                send_piece(p, 0, stride, False)

    def edges_on():
        for to_down in (True, False):
            came(2, 3, to_down)
            for p in EDGES:
                if p in (LAST_DOWN if to_down else LAST_UP):
                    send_piece(p, 2, 2, to_down)
                send_piece(p, 2, 1, to_down)

    def conv(rows):
        total = None
        for a in range(3):
            value = rows(64 * (2 - a))
            for b in range(3):
                term_ab = nt(value[:, CH * b : CH * b + CH], sw_v[3 * a + b])
                total = term_ab if total is None else total + term_ab
        return total

    def pool(total, put):
        for j in range(2):
            half = total[:, 128 * j : 128 * j + 128]
            for i in range(2):
                lvl[j, 64 * i : 64 * i + 64, :] = (
                    half[128 * i : 128 * i + 64] + half[128 * i + 64 : 128 * i + 128]
                )
            put(
                j,
                (lvl[j, pl.ds(0, 64, stride=2), :] + lvl[j, pl.ds(1, 64, stride=2), :]).astype(BF16),
            )

    def conv_inner(t):
        first = pl.multiple_of(128 + 256 * t, 128)
        out = pl.multiple_of(64 + 64 * t, 64)
        total = conv(lambda shift: big[pl.ds(first + shift, 256), :])
        fg[pl.ds(first, 256), :] = total.astype(BF16)

        def put(j, pooled):
            gath[y, pl.ds(out, 64), 128 * j : 128 * j + 128] = pooled

        pool(total, put)

    def conv_edges():
        low = CELLS - 128
        total = conv(
            lambda shift: jnp.concatenate(
                [big[shift : shift + 128, :], big[low + shift : low + shift + 128, :]]
            )
        )
        fg[0:128, :] = total[0:128].astype(BF16)
        fg[low:CELLS, :] = total[128:256].astype(BF16)

        def put(j, pooled):
            gath[y, 0:64, 128 * j : 128 * j + 128] = pooled

        pool(total, put)

    for load in loads[3:]:
        load.start()

    loads[1].wait()
    conv_inner(0)

    pl.semaphore_wait(barrier, 7)

    halo_down = remote(
        g_v.at[pl.ds(CELLS, 64)], g_v.at[pl.ds(0, 64)], halo_s.at[0], halo_r.at[0], rows=down
    )
    halo_up = remote(
        g_v.at[pl.ds(64, 64)], g_v.at[pl.ds(CELLS + 64, 64)], halo_s.at[0], halo_r.at[0], rows=up
    )
    start_own(0)
    halo_down.start()
    halo_up.start()

    tell_y()
    tell_z()
    tell(seen_x, dict(dp_1=x_next), dict(dp_1=x_last))

    @pl.loop(1, 3)
    def _(t):
        conv_inner(t)
        start_own(t)

    def swap_core(k):
        rows = pl.ds(pl.multiple_of(k * CH, CH), CH)
        return remote(
            term.at[1 - c, rows], crecv.at[rows], core_s.at[0], core_r.at[k // 5], dp_2=1 - c
        )

    def put_term(k, value):
        rows = pl.ds(pl.multiple_of(k * CH, CH), CH)
        value = value.astype(BF16)
        term[0, rows, :] = value[:, 0:128]
        term[1, rows, :] = value[:, 128:256]
        swap_core(k).start()

    def tap(k):
        row = pl.multiple_of((2 - k // 3) * 64, 64)
        col = pl.multiple_of(lax.rem(k, 3) * CH, CH)
        put_term(k, nn(flt[...], big[pl.ds(row, CELLS), pl.ds(col, CH)]))

    loads[2].wait()

    @pl.loop(0, 4)
    def _(t):
        rows = pl.ds(pl.multiple_of(t * 256, 256), 256)
        flt[:, rows] = fl_v[rows, :].T

    @pl.loop(3, 6)
    def _(k):
        tap(k)

    forward(1, 0)

    wait_bytes(g_v.at[pl.ds(0, 128)], halo_r.at[0])

    @pl.when(y == 0)
    def _():
        g_v[0:64, :] = jnp.zeros((64, CH), BF16)

    @pl.when(y == NY - 1)
    def _():
        g_v[CELLS + 64 : CELLS + 128, :] = jnp.zeros((64, CH), BF16)

    widen(0, 64)
    widen(CELLS + 64, 64)

    conv_edges()
    forward(1, 1)
    forward(1, 2)
    hear(seen_y)
    edges_from_home()
    tell_y()

    @pl.loop(0, 3)
    def _(k):
        tap(k)

    @pl.loop(6, 9)
    def _(k):
        tap(k)

    def coarse(s):
        mid = jnp.concatenate([gath[s, 0:32], gath[s, 64:256], gath[s, 32:64]])
        cells = pl.ds(pl.multiple_of(s * CH, CH), CH)
        gm_o[cells, :] = nt(mid, mw_v[...]).astype(BF16)
        macc[0:64, :] += tn(mi_v[cells, :], mid)
        wide = mid.astype(F32)
        for j in range(2):
            half = wide[:, 128 * j : 128 * j + 128]
            for i in range(4):
                tmp[j, 32 * i : 32 * i + 32, :] = (
                    half[64 * i : 64 * i + 32] + half[64 * i + 32 : 64 * i + 64]
                )
            top[:, 128 * j : 128 * j + 128] = (
                tmp[j, pl.ds(0, 64, stride=2), :] + tmp[j, pl.ds(1, 64, stride=2), :]
            ).astype(BF16)
        small = top[...]
        cells = pl.ds(pl.multiple_of(s * 64, 64), 64)
        gt_o[cells, :] = nt(small, tw_v[...]).astype(BF16)
        macc[64:192, :] += tn(ti_v[cells, :], small)

    def core_sum(k):
        rows = pl.ds(pl.multiple_of(k * CH, CH), CH)
        csum[rows, :] = (term[c, rows, :].astype(F32) + crecv[rows, :].astype(F32)).astype(BF16)

    def owner(s):
        return 4 * (s // 4) + lax.rem(z + s + 1, 4)

    def x_copy(s, d):
        x_to = lax.rem(x + d, NX)
        rows = pl.ds(pl.multiple_of((owner(s) * NX + x_to) * 80, 80), 80)
        return remote(
            csum.at[rows], xrecv.at[s, d - 1], x_s.at[0], x_r.at[s], dp_1=x_to
        )

    def x_send(batch):
        wait_bytes(crecv.at[pl.ds(1280 * batch, 1280)], core_r.at[batch])

        @pl.loop(5 * batch, 5 * batch + 5)
        def _(k):
            core_sum(k)

        @pl.loop(4 * batch, 4 * batch + 4)
        def _(s):
            for d in X_FAR:
                x_copy(s, d).start()

    def z_copy(z_to):
        slot = lax.rem(z_to - z + NZ, NZ) - 1
        return remote(zsend.at[z_to], zrecv.at[slot], z_s.at[0], z_r.at[0], dp_0=z_to)

    def x_reduce(batch):
        @pl.loop(4 * batch, 4 * batch + 4)
        def _(s):
            wait_bytes(xrecv.at[s], x_r.at[s])
            z_to = owner(s)
            rows = pl.ds(pl.multiple_of((z_to * NX + x) * 80, 80), 80)
            total = csum[rows, :].astype(F32)
            for d in range(1, NX):
                total = total + xrecv[s, d - 1].astype(F32)
            zsend[z_to] = total.astype(BF16)

            @pl.when(z_to != z)
            def _():
                z_copy(z_to).start()

    hear(seen_x)
    hear(seen_z)
    tell_z()
    loads[3].wait()
    put_term(9, tn(fi_v[...], fg[...]))

    forward(2, 0)

    x_send(0)

    forward(2, 1)
    forward(2, 2)

    for load in loads[4:]:
        load.wait()
    macc[...] = jnp.zeros_like(macc)
    coarse(y)

    hear(seen_z)
    tell_z()

    hear(seen_y)
    edges_on()
    tell_y()

    x_send(1)

    came(1, 3, True)
    came(1, 3, False)
    coarse(lax.rem(y + 1, NY))
    coarse(lax.rem(y + NY - 1, NY))

    forward(3, 0)
    forward(3, 1)
    forward(3, 2)

    coarse(lax.rem(y + 2, NY))
    coarse(lax.rem(y + NY - 2, NY))

    for k in range(4):
        rows = slice(256 * k, 256 * k + 256)
        gf_o[rows, :] = nt(fg[rows, :], fw_v[...]).astype(BF16)

    hear(seen_y)
    tell(seen_c, dict(dp_2=1 - c))

    came(3, 3, True)
    came(3, 3, False)

    coarse(lax.rem(y + 3, NY))
    coarse(lax.rem(y + NY - 3, NY))

    hear(seen_z)

    x_reduce(0)

    wait_bytes(gath.at[0], last_r.at[0])

    coarse(lax.rem(y + 4, NY))
    hear(seen_c, 1)

    others = [(d, e) for d in X_FAR for e in (1, 0)] + [(0, 1)]
    for i in range(NX):
        for j in range(NC):
            bterm[NC * i + j] = macc[48 * i : 48 * i + 48, 128 * j : 128 * j + 128].astype(BF16)

    def bx_copy(d, e):
        x_to, c_to = lax.rem(x + d, NX), lax.rem(c + e, NC)
        return remote(
            bterm.at[NC * x_to + c_to], bxrecv.at[NC * d + e - 1], bx_s.at[0], bx_r.at[0],
            dp_1=x_to, dp_2=c_to,
        )

    for d, e in others:
        bx_copy(d, e).start()

    x_reduce(1)

    wait_bytes(bxrecv, bx_r.at[0])
    total = bterm[NC * x + c].astype(F32)
    for i in range(NX * NC - 1):
        total = total + bxrecv[i].astype(F32)
    bz[z] = total.astype(BF16)

    def bz_copy(d):
        return remote(bz.at[z], bz.at[z], bz_s.at[0], bz_r.at[0], dp_0=lax.rem(z + d, NZ))

    for d in FAR:
        bz_copy(d).start()

    wait_bytes(zrecv, z_r.at[0])
    total = zsend[z].astype(F32)
    for i in range(NZ - 1):
        total = total + zrecv[i].astype(F32)
    for i in range(NC):
        yown[i] = total[40 * i : 40 * i + 40].astype(BF16)
    yex[NY * c + y] = yown[c]

    def y_copy(d, e):
        c_to = lax.rem(c + e, NC)
        return remote(
            yown.at[c_to], yex.at[NY * c + y], y_s.at[0], y_r.at[0],
            rows=lax.rem(y + d, NY), dp_2=c_to,
        )

    for d in FAR:
        for e in (1, 0):
            y_copy(d, e).start()
    y_copy(0, 1).start()

    wait_bytes(bz.at[pl.ds(0, NZ - 1)], bz_r.at[0])
    total = bz[0].astype(F32)
    for i in range(1, NZ):
        total = total + bz[i].astype(F32)
    bfin[NC * x + c] = total.astype(BF16)

    def bf_copy(d, e):
        return remote(
            bfin.at[NC * x + c], bfin.at[NC * x + c], bf_s.at[0], bf_r.at[0],
            dp_1=lax.rem(x + d, NX), dp_2=lax.rem(c + e, NC),
        )

    for d, e in others:
        bf_copy(d, e).start()

    wait_bytes(yex.at[pl.ds(0, NC * NY - 1)], y_r.at[0])
    for i in range(NC):
        total = yex[NY * i].astype(F32)
        for j in range(1, NY):
            total = total + yex[NY * i + j].astype(F32)
        kg_o[:, 128 * i : 128 * i + 128] = total

    for ref, sem in (
        (g_v.at[pl.ds(0, 128)], halo_s), (gath.at[pl.ds(0, 7), pl.ds(0, 192)], ring_s),
        (gath.at[pl.ds(0, 7), pl.ds(0, 64)], edge_s), (crecv, core_s),
        (csum.at[pl.ds(0, NZ * (NX - 1) * 80)], x_s), (zrecv, z_s), (yex.at[pl.ds(0, NC * NY - 1)], y_s),
        (bxrecv, bx_s), (bz.at[pl.ds(0, NZ - 1)], bz_s),
    ):
        wait_bytes(ref, sem.at[0])

    wait_bytes(bfin.at[pl.ds(0, NX * NC - 1)], bf_r.at[0])
    for i in range(NX):
        for j in range(NC):
            block = bfin[NC * i + j].astype(F32)
            cols = slice(128 * j, 128 * j + 128)
            if i == 0:
                ml_o[0:48, cols] = block
            elif i == 1:
                ml_o[48:64, cols] = block[0:16]
                tl_o[0:32, cols] = block[16:48]
            else:
                tl_o[48 * i - 64 : 48 * i - 16, cols] = block
    wait_bytes(bfin.at[pl.ds(0, NX * NC - 1)], bf_s.at[0])


def store(*refs):
    copies = [pltpu.make_async_copy(refs[i], refs[6 + i], refs[12].at[i]) for i in range(6)]
    for copy in copies:
        copy.start()
    for copy in copies:
        copy.wait()


def body(
    fine_level, out_grad, fine_input, mid_input, top_input,
    smooth_weight, fine_lateral, mid_lateral, top_lateral,
):
    sem = pltpu.SemaphoreType.DMA
    sizes = [
        ((CELLS, CH), BF16), ((CELLS + 128, CH), BF16), ((CELLS, CH), BF16), ((2048, 64), BF16),
        ((512, 128), BF16), ((9, CH, CH), BF16), ((CH, CH), BF16), ((64, CH), BF16), ((128, CH), BF16),
        ((CELLS + 128, 3 * CH), BF16), ((CH, CELLS), BF16),
        ((2, 128, 128), F32), ((2, 128, 128), F32), ((CELLS, CH), BF16),
        ((NY, CH, CH), BF16), ((64, CH), BF16), ((192, CH), F32),
        ((2, 2560, 128), BF16), ((2560, 128), BF16), ((2560, 128), BF16), ((NZ, NX - 1, 80, 128), BF16),
        ((NZ, 80, 128), BF16), ((NZ - 1, 80, 128), BF16), ((NC, 40, 128), BF16), ((NC * NY, 40, 128), BF16),
        ((NX * NC, 48, 128), BF16), ((NX * NC - 1, 48, 128), BF16),
        ((NZ, 48, 128), BF16), ((NX * NC, 48, 128), BF16),
    ]
    sems = [
        (9,), (1,), (1,), (1,), (1,), (3, 4, 2), (1,),
        (1,), (2,), (1,), (NZ,), (1,), (1,), (1,), (1,),
        (1,), (1,), (1,), (1,), (1,), (1,),
    ]
    shapes = [
        ((CELLS, CH), BF16), ((2048, 64), BF16), ((512, 128), BF16),
        ((40, CH), F32), ((64, CH), F32), ((128, CH), F32),
    ]
    hbm = pl.BlockSpec(memory_space=pltpu.HBM)
    anywhere = pl.BlockSpec(memory_space=pl.ANY)
    grads = pl.pallas_call(
        kernel,
        out_shape=[pltpu.VMEM(*shape) for shape in shapes],
        in_specs=[hbm] * 9,
        out_specs=[pl.BlockSpec(memory_space=pltpu.VMEM)] * 6,
        scratch_shapes=[pltpu.VMEM(*size) for size in sizes] + [sem(size) for size in sems]
        + [pltpu.SemaphoreType.REGULAR((count,)) for count in (2, 2, 2, 1)],
        compiler_params=pltpu.CompilerParams(
            collective_id=0, has_side_effects=True, vmem_limit_bytes=48 * 1024 * 1024
        ),
    )(*(pltpu.with_memory_space_constraint(value, pltpu.HBM) for value in (
        fine_level.reshape(CELLS, CH), out_grad.reshape(CELLS, CH), fine_input.reshape(CELLS, CH),
        mid_input.reshape(2048, 64), top_input.reshape(512, 128), smooth_weight.reshape(9, CH, CH),
        fine_lateral, mid_lateral, top_lateral,
    )))
    grads = pl.pallas_call(
        store,
        out_shape=[pltpu.HBM(*shape) for shape in shapes],
        in_specs=[anywhere] * 6,
        out_specs=[hbm] * 6,
        scratch_shapes=[sem((6,))],
    )(*(pltpu.with_memory_space_constraint(grad, pltpu.VMEM) for grad in grads))
    return (
        grads[0].reshape(out_grad.shape), grads[1].reshape(mid_input.shape),
        grads[2].reshape(top_input.shape), grads[3], grads[4], grads[5],
    )


def solution(mesh):
    torus = Mesh(
        mesh.devices.reshape(NZ, NX, NC, NY), ("dp_0", "dp_1", "dp_2", "rows")
    )
    return jax.shard_map(
        body,
        mesh=torus,
        in_specs=(
            P(DP, "rows", None, None), P(DP, "rows", None, None), P(DP, "rows", None, None),
            P(DP, None, None, "rows"), P(DP, None, None, "rows"),
            P(), P(), P("rows", None), P("rows", None),
        ),
        out_specs=(
            P(DP, "rows", None, None), P(DP, None, None, "rows"), P(DP, None, None, "rows"),
            P(DP, None), P("rows", None), P("rows", None),
        ),
        check_vma=False,
    )
```

```python
import jax
import jax.numpy as jnp
from jax import lax
from jax.experimental import pallas as pl
from jax.experimental.pallas import tpu as pltpu
from jax.sharding import Mesh
from jax.sharding import PartitionSpec as P

DP = ("dp_0", "dp_1", "dp_2")
MESH = pl.DeviceIdType.MESH
F32 = jnp.float32
BF16 = jnp.bfloat16
NZ, NX, NC, NY = 8, 4, 2, 8
STRIP, WIDTH, CH = 16, 64, 256
CELLS = STRIP * WIDTH
PIECES = ((64, 64), (128, 64), (192, 64), (0, 64))
INNER, EDGES = (0, 1, 2), (3,)
X_FAR, FAR = (2, 1, 3), (4, 3, 5, 2, 6, 1, 7)
LAST_DOWN, LAST_UP = (0, 2), (1, 3)


def nt(left, right):
    return lax.dot_general(left, right, (((1,), (1,)), ((), ())), preferred_element_type=F32)


def tn(left, right):
    return lax.dot_general(left, right, (((0,), (0,)), ((), ())), preferred_element_type=F32)


def nn(left, right):
    return lax.dot_general(left, right, (((1,), (0,)), ((), ())), preferred_element_type=F32)


def kernel(
    fl, og, fi, mi, ti, sw, fw, mw, tw,
    gf_o, gm_o, gt_o, kg_o, ml_o, tl_o,
    fl_v, g_v, fi_v, mi_v, ti_v, sw_v, fw_v, mw_v, tw_v,
    big, flt, lvl, tmp, fg, gath, top, macc,
    term, crecv, csum, xrecv, zsend, zrecv, yown, yex,
    bterm, bxrecv, bz, bfin,
    in_sem, halo_s, halo_r, ring_s, edge_s, ring_r, last_r,
    core_s, core_r, x_s, x_r, z_s, z_r, y_s, y_r,
    bx_s, bx_r, bz_s, bz_r, bf_s, bf_r,
    seen_y, seen_z, seen_x, seen_c,
):
    z = lax.axis_index("dp_0")
    x = lax.axis_index("dp_1")
    c = lax.axis_index("dp_2")
    y = lax.axis_index("rows")

    def remote(src, dst, send, recv, **where):
        return pltpu.make_async_remote_copy(
            src_ref=src, dst_ref=dst, send_sem=send, recv_sem=recv,
            device_id=where, device_id_type=MESH,
        )

    def wait_bytes(ref, sem):
        remote(ref, ref, sem, sem, dp_2=1 - c).wait_recv()

    loads = [
        pltpu.make_async_copy(og, g_v.at[pl.ds(64, CELLS)], in_sem.at[0]),
        pltpu.make_async_copy(sw, sw_v, in_sem.at[1]),
        pltpu.make_async_copy(fl, fl_v, in_sem.at[2]),
        pltpu.make_async_copy(fi, fi_v, in_sem.at[3]),
        pltpu.make_async_copy(fw, fw_v, in_sem.at[4]),
        pltpu.make_async_copy(mi, mi_v, in_sem.at[5]),
        pltpu.make_async_copy(ti, ti_v, in_sem.at[6]),
        pltpu.make_async_copy(mw, mw_v, in_sem.at[7]),
        pltpu.make_async_copy(tw, tw_v, in_sem.at[8]),
    ]
    for load in loads[:3]:
        load.start()

    barrier = pltpu.get_barrier_semaphore()

    def greet(**where):
        pl.semaphore_signal(barrier, inc=1, device_id=where, device_id_type=MESH)

    down, up = lax.rem(y + 1, NY), lax.rem(y + NY - 1, NY)
    x_next, x_last = lax.rem(x + 1, NX), lax.rem(x + NX - 1, NX)
    z_next, z_last = lax.rem(z + 1, NZ), lax.rem(z + NZ - 1, NZ)
    for where in (
        dict(rows=down), dict(rows=up), dict(dp_1=x_next), dict(dp_1=x_last),
        dict(dp_0=z_next), dict(dp_0=z_last), dict(dp_2=1 - c),
    ):
        greet(**where)

    def tell(sem, *others):
        for i, where in enumerate(others):
            pl.semaphore_signal(sem.at[i], inc=1, device_id=where, device_id_type=MESH)

    def hear(sem, count=2):
        for i in range(count):
            pl.semaphore_wait(sem.at[i], 1)

    def tell_y():
        tell(seen_y, dict(rows=down), dict(rows=up))

    def tell_z():
        tell(seen_z, dict(dp_0=z_next), dict(dp_0=z_last))

    def widen(first, rows):
        value = g_v[pl.ds(first, rows), :].astype(F32)
        column = lax.rem(lax.broadcasted_iota(jnp.int32, (rows, CH), 0), WIDTH)
        after = jnp.where(column == WIDTH - 1, 0.0, pltpu.roll(value, rows - 1, 0))
        before = jnp.where(column == 0, 0.0, pltpu.roll(value, 1, 0))
        big[pl.ds(first, rows), 0:CH] = after.astype(BF16)
        big[pl.ds(first, rows), CH : 2 * CH] = value.astype(BF16)
        big[pl.ds(first, rows), 2 * CH : 3 * CH] = before.astype(BF16)

    loads[0].wait()

    @pl.loop(0, 4)
    def _(t):
        widen(pl.multiple_of(64 + t * 256, 64), 256)

    def send_piece(p, away, stride, to_down):
        origin = lax.rem(y + NY - away, NY) if to_down else lax.rem(y + away, NY)
        target = lax.rem(y + stride, NY) if to_down else lax.rem(y + NY - stride, NY)
        first, count = PIECES[p] if isinstance(p, int) else (pl.multiple_of(64 + 64 * p, 64), 64)
        block = gath.at[origin, pl.ds(first, count)]
        h = away + stride
        group = 3 if isinstance(p, int) and p in EDGES else p
        recv = last_r.at[0] if h == 4 else ring_r.at[h - 1, group, 0 if to_down else 1]
        send = edge_s if isinstance(p, int) and p in EDGES else ring_s
        remote(block, block, send.at[0], recv, rows=target).start()

    def came(h, group, to_down):
        wait_bytes(gath.at[0, pl.ds(0, 64)], ring_r.at[h - 1, group, 0 if to_down else 1])

    def start_own(p):
        send_piece(p, 0, 1, True)
        send_piece(p, 0, 1, False)

    def forward(h, p):
        for to_down in (True, False):
            came(h, p, to_down)
            if h < 3 or p in (LAST_DOWN if to_down else LAST_UP):
                send_piece(p, h, 1, to_down)

    def edges_from_home():
        for stride in (1, 2):
            for p in EDGES:
                send_piece(p, 0, stride, True)
                send_piece(p, 0, stride, False)

    def edges_on():
        for to_down in (True, False):
            came(2, 3, to_down)
            for p in EDGES:
                send_piece(p, 2, 1, to_down)
                if p in (LAST_DOWN if to_down else LAST_UP):
                    send_piece(p, 2, 2, to_down)

    def conv(rows):
        total = None
        for a in range(3):
            value = rows(64 * (2 - a))
            for b in range(3):
                term_ab = nt(value[:, CH * b : CH * b + CH], sw_v[3 * a + b])
                total = term_ab if total is None else total + term_ab
        return total

    def pool(total, put):
        for j in range(2):
            half = total[:, 128 * j : 128 * j + 128]
            for i in range(2):
                lvl[j, 64 * i : 64 * i + 64, :] = (
                    half[128 * i : 128 * i + 64] + half[128 * i + 64 : 128 * i + 128]
                )
            put(
                j,
                (lvl[j, pl.ds(0, 64, stride=2), :] + lvl[j, pl.ds(1, 64, stride=2), :]).astype(BF16),
            )

    def conv_inner(t):
        first = pl.multiple_of(128 + 256 * t, 128)
        out = pl.multiple_of(64 + 64 * t, 64)
        total = conv(lambda shift: big[pl.ds(first + shift, 256), :])
        fg[pl.ds(first, 256), :] = total.astype(BF16)

        def put(j, pooled):
            gath[y, pl.ds(out, 64), 128 * j : 128 * j + 128] = pooled

        pool(total, put)

    def conv_edges():
        low = CELLS - 128
        total = conv(
            lambda shift: jnp.concatenate(
                [big[shift : shift + 128, :], big[low + shift : low + shift + 128, :]]
            )
        )
        fg[0:128, :] = total[0:128].astype(BF16)
        fg[low:CELLS, :] = total[128:256].astype(BF16)

        def put(j, pooled):
            gath[y, 0:64, 128 * j : 128 * j + 128] = pooled

        pool(total, put)

    for load in loads[3:]:
        load.start()

    loads[1].wait()
    conv_inner(0)

    pl.semaphore_wait(barrier, 7)

    halo_down = remote(
        g_v.at[pl.ds(CELLS, 64)], g_v.at[pl.ds(0, 64)], halo_s.at[0], halo_r.at[0], rows=down
    )
    halo_up = remote(
        g_v.at[pl.ds(64, 64)], g_v.at[pl.ds(CELLS + 64, 64)], halo_s.at[0], halo_r.at[0], rows=up
    )
    halo_down.start()
    halo_up.start()

    tell_y()
    tell_z()
    tell(seen_x, dict(dp_1=x_next), dict(dp_1=x_last))

    start_own(0)

    @pl.loop(1, 3)
    def _(t):
        conv_inner(t)
        start_own(t)

    def swap_core(k):
        rows = pl.ds(pl.multiple_of(k * CH, CH), CH)
        return remote(
            term.at[1 - c, rows], crecv.at[rows], core_s.at[0], core_r.at[k // 5], dp_2=1 - c
        )

    def put_term(k, value):
        rows = pl.ds(pl.multiple_of(k * CH, CH), CH)
        value = value.astype(BF16)
        term[0, rows, :] = value[:, 0:128]
        term[1, rows, :] = value[:, 128:256]
        swap_core(k).start()

    def tap(k):
        row = pl.multiple_of((2 - k // 3) * 64, 64)
        col = pl.multiple_of(lax.rem(k, 3) * CH, CH)
        put_term(k, nn(flt[...], big[pl.ds(row, CELLS), pl.ds(col, CH)]))

    loads[2].wait()

    @pl.loop(0, 4)
    def _(t):
        rows = pl.ds(pl.multiple_of(t * 256, 256), 256)
        flt[:, rows] = fl_v[rows, :].T

    @pl.loop(3, 6)
    def _(k):
        tap(k)

    forward(1, 0)

    wait_bytes(g_v.at[pl.ds(0, 128)], halo_r.at[0])

    @pl.when(y == 0)
    def _():
        g_v[0:64, :] = jnp.zeros((64, CH), BF16)

    @pl.when(y == NY - 1)
    def _():
        g_v[CELLS + 64 : CELLS + 128, :] = jnp.zeros((64, CH), BF16)

    widen(0, 64)
    widen(CELLS + 64, 64)

    conv_edges()
    forward(1, 1)
    forward(1, 2)
    hear(seen_y)
    edges_from_home()
    tell_y()

    @pl.loop(0, 3)
    def _(k):
        tap(k)

    @pl.loop(6, 9)
    def _(k):
        tap(k)

    def coarse_sums(s):
        mid = jnp.concatenate([gath[s, 0:32], gath[s, 64:256], gath[s, 32:64]])
        cells = pl.ds(pl.multiple_of(s * CH, CH), CH)
        macc[0:64, :] += tn(mi_v[cells, :], mid)
        wide = mid.astype(F32)
        for j in range(2):
            half = wide[:, 128 * j : 128 * j + 128]
            for i in range(4):
                tmp[j, 32 * i : 32 * i + 32, :] = (
                    half[64 * i : 64 * i + 32] + half[64 * i + 32 : 64 * i + 64]
                )
            top[:, 128 * j : 128 * j + 128] = (
                tmp[j, pl.ds(0, 64, stride=2), :] + tmp[j, pl.ds(1, 64, stride=2), :]
            ).astype(BF16)
        small = top[...]
        cells = pl.ds(pl.multiple_of(s * 64, 64), 64)
        macc[64:192, :] += tn(ti_v[cells, :], small)
        return mid, small

    def coarse_maps(s, mid, small):
        gm_o[pl.ds(pl.multiple_of(s * CH, CH), CH), :] = nt(mid, mw_v[...]).astype(BF16)
        gt_o[pl.ds(pl.multiple_of(s * 64, 64), 64), :] = nt(small, tw_v[...]).astype(BF16)

    def coarse(s):
        coarse_maps(s, *coarse_sums(s))

    def core_sum(k):
        rows = pl.ds(pl.multiple_of(k * CH, CH), CH)
        csum[rows, :] = (term[c, rows, :].astype(F32) + crecv[rows, :].astype(F32)).astype(BF16)

    def owner(s):
        return 4 * (s // 4) + lax.rem(z + s + 1, 4)

    def x_copy(s, d):
        x_to = lax.rem(x + d, NX)
        rows = pl.ds(pl.multiple_of((owner(s) * NX + x_to) * 80, 80), 80)
        return remote(
            csum.at[rows], xrecv.at[s, d - 1], x_s.at[0], x_r.at[s], dp_1=x_to
        )

    def x_send(batch):
        wait_bytes(crecv.at[pl.ds(1280 * batch, 1280)], core_r.at[batch])

        @pl.loop(5 * batch, 5 * batch + 5)
        def _(k):
            core_sum(k)

        @pl.loop(4 * batch, 4 * batch + 4)
        def _(s):
            for d in X_FAR:
                x_copy(s, d).start()

    def z_copy(z_to):
        slot = lax.rem(z_to - z + NZ, NZ) - 1
        return remote(zsend.at[z_to], zrecv.at[slot], z_s.at[0], z_r.at[0], dp_0=z_to)

    def x_reduce(batch):
        @pl.loop(4 * batch, 4 * batch + 4)
        def _(s):
            wait_bytes(xrecv.at[s], x_r.at[s])
            z_to = owner(s)
            rows = pl.ds(pl.multiple_of((z_to * NX + x) * 80, 80), 80)
            total = csum[rows, :].astype(F32)
            for d in range(1, NX):
                total = total + xrecv[s, d - 1].astype(F32)
            zsend[z_to] = total.astype(BF16)

            @pl.when(z_to != z)
            def _():
                z_copy(z_to).start()

    hear(seen_x)
    hear(seen_z)
    tell_z()
    x_send(0)

    forward(2, 0)

    loads[3].wait()
    put_term(9, tn(fi_v[...], fg[...]))

    forward(2, 1)
    forward(2, 2)

    for load in loads[4:]:
        load.wait()
    macc[...] = jnp.zeros_like(macc)
    coarse(y)

    hear(seen_z)
    tell_z()

    x_send(1)

    hear(seen_y)
    edges_on()
    tell_y()

    came(1, 3, True)
    came(1, 3, False)
    coarse(lax.rem(y + 1, NY))
    coarse(lax.rem(y + NY - 1, NY))

    forward(3, 0)
    forward(3, 1)
    forward(3, 2)

    coarse(lax.rem(y + 2, NY))
    coarse(lax.rem(y + NY - 2, NY))

    for k in range(4):
        rows = slice(256 * k, 256 * k + 256)
        gf_o[rows, :] = nt(fg[rows, :], fw_v[...]).astype(BF16)

    hear(seen_y)
    tell(seen_c, dict(dp_2=1 - c))

    came(3, 3, True)
    came(3, 3, False)

    coarse(lax.rem(y + 3, NY))
    coarse(lax.rem(y + NY - 3, NY))

    hear(seen_z)

    x_reduce(0)

    wait_bytes(gath.at[0], last_r.at[0])

    far = lax.rem(y + 4, NY)
    far_maps = coarse_sums(far)
    hear(seen_c, 1)

    others = [(d, e) for d in X_FAR for e in (1, 0)] + [(0, 1)]
    for i in range(NX):
        for j in range(NC):
            bterm[NC * i + j] = macc[48 * i : 48 * i + 48, 128 * j : 128 * j + 128].astype(BF16)

    def bx_copy(d, e):
        x_to, c_to = lax.rem(x + d, NX), lax.rem(c + e, NC)
        return remote(
            bterm.at[NC * x_to + c_to], bxrecv.at[NC * d + e - 1], bx_s.at[0], bx_r.at[0],
            dp_1=x_to, dp_2=c_to,
        )

    for d, e in others:
        bx_copy(d, e).start()

    coarse_maps(far, *far_maps)

    x_reduce(1)

    wait_bytes(bxrecv, bx_r.at[0])
    total = bterm[NC * x + c].astype(F32)
    for i in range(NX * NC - 1):
        total = total + bxrecv[i].astype(F32)
    bz[z] = total.astype(BF16)

    def bz_copy(d):
        return remote(bz.at[z], bz.at[z], bz_s.at[0], bz_r.at[0], dp_0=lax.rem(z + d, NZ))

    for d in FAR:
        bz_copy(d).start()

    wait_bytes(zrecv, z_r.at[0])
    total = zsend[z].astype(F32)
    for i in range(NZ - 1):
        total = total + zrecv[i].astype(F32)
    for i in range(NC):
        yown[i] = total[40 * i : 40 * i + 40].astype(BF16)
    yex[NY * c + y] = yown[c]

    def y_copy(d, e):
        c_to = lax.rem(c + e, NC)
        return remote(
            yown.at[c_to], yex.at[NY * c + y], y_s.at[0], y_r.at[0],
            rows=lax.rem(y + d, NY), dp_2=c_to,
        )

    for d in FAR:
        for e in (1, 0):
            y_copy(d, e).start()
    y_copy(0, 1).start()

    wait_bytes(bz.at[pl.ds(0, NZ - 1)], bz_r.at[0])
    total = bz[0].astype(F32)
    for i in range(1, NZ):
        total = total + bz[i].astype(F32)
    bfin[NC * x + c] = total.astype(BF16)

    def bf_copy(d, e):
        return remote(
            bfin.at[NC * x + c], bfin.at[NC * x + c], bf_s.at[0], bf_r.at[0],
            dp_1=lax.rem(x + d, NX), dp_2=lax.rem(c + e, NC),
        )

    for d, e in others:
        bf_copy(d, e).start()

    wait_bytes(yex.at[pl.ds(0, NC * NY - 1)], y_r.at[0])
    for i in range(NC):
        total = yex[NY * i].astype(F32)
        for j in range(1, NY):
            total = total + yex[NY * i + j].astype(F32)
        kg_o[:, 128 * i : 128 * i + 128] = total

    for ref, sem in (
        (g_v.at[pl.ds(0, 128)], halo_s), (gath.at[pl.ds(0, 7), pl.ds(0, 192)], ring_s),
        (gath.at[pl.ds(0, 7), pl.ds(0, 64)], edge_s), (crecv, core_s),
        (csum.at[pl.ds(0, NZ * (NX - 1) * 80)], x_s), (zrecv, z_s), (yex.at[pl.ds(0, NC * NY - 1)], y_s),
        (bxrecv, bx_s), (bz.at[pl.ds(0, NZ - 1)], bz_s),
    ):
        wait_bytes(ref, sem.at[0])

    wait_bytes(bfin.at[pl.ds(0, NX * NC - 1)], bf_r.at[0])
    for i in range(NX):
        for j in range(NC):
            block = bfin[NC * i + j].astype(F32)
            cols = slice(128 * j, 128 * j + 128)
            if i == 0:
                ml_o[0:48, cols] = block
            elif i == 1:
                ml_o[48:64, cols] = block[0:16]
                tl_o[0:32, cols] = block[16:48]
            else:
                tl_o[48 * i - 64 : 48 * i - 16, cols] = block
    wait_bytes(bfin.at[pl.ds(0, NX * NC - 1)], bf_s.at[0])


def store(*refs):
    copies = [pltpu.make_async_copy(refs[i], refs[6 + i], refs[12].at[i]) for i in range(6)]
    for copy in copies:
        copy.start()
    for copy in copies:
        copy.wait()


def body(
    fine_level, out_grad, fine_input, mid_input, top_input,
    smooth_weight, fine_lateral, mid_lateral, top_lateral,
):
    sem = pltpu.SemaphoreType.DMA
    sizes = [
        ((CELLS, CH), BF16), ((CELLS + 128, CH), BF16), ((CELLS, CH), BF16), ((2048, 64), BF16),
        ((512, 128), BF16), ((9, CH, CH), BF16), ((CH, CH), BF16), ((64, CH), BF16), ((128, CH), BF16),
        ((CELLS + 128, 3 * CH), BF16), ((CH, CELLS), BF16),
        ((2, 128, 128), F32), ((2, 128, 128), F32), ((CELLS, CH), BF16),
        ((NY, CH, CH), BF16), ((64, CH), BF16), ((192, CH), F32),
        ((2, 2560, 128), BF16), ((2560, 128), BF16), ((2560, 128), BF16), ((NZ, NX - 1, 80, 128), BF16),
        ((NZ, 80, 128), BF16), ((NZ - 1, 80, 128), BF16), ((NC, 40, 128), BF16), ((NC * NY, 40, 128), BF16),
        ((NX * NC, 48, 128), BF16), ((NX * NC - 1, 48, 128), BF16),
        ((NZ, 48, 128), BF16), ((NX * NC, 48, 128), BF16),
    ]
    sems = [
        (9,), (1,), (1,), (1,), (1,), (3, 4, 2), (1,),
        (1,), (2,), (1,), (NZ,), (1,), (1,), (1,), (1,),
        (1,), (1,), (1,), (1,), (1,), (1,),
    ]
    shapes = [
        ((CELLS, CH), BF16), ((2048, 64), BF16), ((512, 128), BF16),
        ((40, CH), F32), ((64, CH), F32), ((128, CH), F32),
    ]
    hbm = pl.BlockSpec(memory_space=pltpu.HBM)
    anywhere = pl.BlockSpec(memory_space=pl.ANY)
    grads = pl.pallas_call(
        kernel,
        out_shape=[pltpu.VMEM(*shape) for shape in shapes],
        in_specs=[hbm] * 9,
        out_specs=[pl.BlockSpec(memory_space=pltpu.VMEM)] * 6,
        scratch_shapes=[pltpu.VMEM(*size) for size in sizes] + [sem(size) for size in sems]
        + [pltpu.SemaphoreType.REGULAR((count,)) for count in (2, 2, 2, 1)],
        compiler_params=pltpu.CompilerParams(
            collective_id=0, has_side_effects=True, vmem_limit_bytes=48 * 1024 * 1024
        ),
    )(*(pltpu.with_memory_space_constraint(value, pltpu.HBM) for value in (
        fine_level.reshape(CELLS, CH), out_grad.reshape(CELLS, CH), fine_input.reshape(CELLS, CH),
        mid_input.reshape(2048, 64), top_input.reshape(512, 128), smooth_weight.reshape(9, CH, CH),
        fine_lateral, mid_lateral, top_lateral,
    )))
    grads = pl.pallas_call(
        store,
        out_shape=[pltpu.HBM(*shape) for shape in shapes],
        in_specs=[anywhere] * 6,
        out_specs=[hbm] * 6,
        scratch_shapes=[sem((6,))],
    )(*(pltpu.with_memory_space_constraint(grad, pltpu.VMEM) for grad in grads))
    return (
        grads[0].reshape(out_grad.shape), grads[1].reshape(mid_input.shape),
        grads[2].reshape(top_input.shape), grads[3], grads[4], grads[5],
    )


def solution(mesh):
    torus = Mesh(
        mesh.devices.reshape(NZ, NX, NC, NY), ("dp_0", "dp_1", "dp_2", "rows")
    )
    return jax.shard_map(
        body,
        mesh=torus,
        in_specs=(
            P(DP, "rows", None, None), P(DP, "rows", None, None), P(DP, "rows", None, None),
            P(DP, None, None, "rows"), P(DP, None, None, "rows"),
            P(), P(), P("rows", None), P("rows", None),
        ),
        out_specs=(
            P(DP, "rows", None, None), P(DP, None, None, "rows"), P(DP, None, None, "rows"),
            P(DP, None), P("rows", None), P("rows", None),
        ),
        check_vma=False,
    )
```
